32 devices in a mesh: samples: 2 (over x), px: 8 (over z, y), py: 2 (over core).
Axes of the slice: x: 2, y: 2, z: 4, core: 2. Of those that a mesh axis runs over, the one named last changes fastest.
Arguments:
- source: float32 [2, 512, 256, 256], P(None, 'samples', 'px', 'py'), parts along dimension 1, may hold values from -6 to 6
- speed: float32 [512, 256, 256], P('samples', 'px', 'py'), parts along dimension 0, may hold values from 0.5 to 3
Outputs:
- solution: float32 [2, 512, 256, 256], P(None, 'samples', 'px', 'py'), parts along dimension 1
The draws below stay inside these ranges and needn't reach their ends.
There are 2 independent parts, one for each index of `samples`. The reference program is written for one: setup_inputs(seed, part) draws one part's arguments, and reference() takes and returns one part's arrays. A program takes and returns all parts, laid end to end along the dimension named above; each array names one. Nothing has to cross between parts.
All inputs are finite; a program needn't handle non-finite values.
Results may differ from the reference program's by a relative error of at most 0.00024.
Values sent between devices are 32-bit elements; how exact they have to be, the bound alone decides.
A program may use at most 192 MiB of HBM per device.

```python
import math
import jax
import jax.numpy as jnp
from jax import lax

NX = 256
NY = 256
NZ = 256


def draw_source(key, part):
    normal_part = jnp.clip(jax.random.normal(key, (2, NX, NY, NZ), jnp.float32), -6.0, 6.0)
    return normal_part


def level_of(own_key, extent, shards, low, largest):
    loudness, own = 1.0, jax.random.fold_in(own_key, 6)
    for position, parts in shards:
        heights = jnp.exp(jax.random.uniform(jax.random.fold_in(own, position), (parts,), jnp.float32, low / len(shards), largest / len(shards)))
        loudness = loudness * jnp.repeat(heights, extent[position] // parts).reshape([-1 if axis == position else 1 for axis in range(len(extent))])
    return loudness


def setup_inputs(seed: int = 0, part: int = 0) -> dict:
    key_list = jax.random.split(jax.random.key(seed), 3)
    part_splits = jax.random.split(jax.random.fold_in(key_list[2], part), 3)
    return {
        "source": draw_source(jax.random.fold_in(jax.random.fold_in(key_list[2], part), 71), part),
        "speed": jnp.clip(jnp.exp(math.log(3.0) - 1.7917595 * jax.random.uniform(part_splits[1], (NX, NY, NZ), jnp.float32) ** level_of(part_splits[1], (NX, NY, NZ), ((1, 8), (2, 2)), -0.2, 0.2)), 0.5, 3.0),
    }


wave_square = 0.25
damping = 0.5
epsilon = 1e-06
highest = lax.Precision.HIGHEST

def sine_table(length):
    positions = jnp.arange(length, dtype=jnp.float32) + 1.0
    phases = jnp.pi * positions[:, None] * positions[None, :] / (length + 1.0)
    return jnp.sqrt(2.0 / (length + 1.0)) * jnp.sin(phases)

def eigen_line(length, offset, number):
    positions = jnp.arange(number, dtype=jnp.float32) + jnp.asarray(offset).astype(jnp.float32) + 1.0
    sine_half = jnp.sin(jnp.pi * positions / (2.0 * (length + 1.0)))
    return 4.0 * sine_half * sine_half

def divide(values, eigen_x, eigen_y, eigen_z):
    shifted = eigen_x[:, None, None] + eigen_y[None, :, None] + eigen_z[None, None, :] - wave_square
    damped = damping * wave_square
    modulus = shifted * shifted + damped * damped
    real_part = (values[0] * shifted + values[1] * damped) / modulus
    imag_part = (values[1] * shifted - values[0] * damped) / modulus
    return jnp.stack([real_part, imag_part])

def transform(values, matrix_x, matrix_y, matrix_z):
    values = jnp.einsum('ak,ckyz->cayz', matrix_x, values, precision=highest)
    values = jnp.einsum('ak,cxkz->cxaz', matrix_y, values, precision=highest)
    return jnp.einsum('ak,cxyk->cxya', matrix_z, values, precision=highest)

def precondition(vector):
    matrix_x = sine_table(NX)
    matrix_y = sine_table(NY)
    matrix_z = sine_table(NZ)
    spectral = transform(vector, matrix_x, matrix_y, matrix_z)
    scaled = divide(spectral, eigen_line(NX, 0, NX), eigen_line(NY, 0, NY), eigen_line(NZ, 0, NZ))
    return transform(scaled, matrix_x, matrix_y, matrix_z)

def operate(vector, wave_field):
    padded = jnp.pad(vector, ((0, 0), (1, 1), (1, 1), (1, 1)))
    neighbours = padded[:, 2:, 1:-1, 1:-1] + padded[:, :-2, 1:-1, 1:-1]
    neighbours = neighbours + padded[:, 1:-1, 2:, 1:-1] + padded[:, 1:-1, :-2, 1:-1]
    neighbours = neighbours + padded[:, 1:-1, 1:-1, 2:] + padded[:, 1:-1, 1:-1, :-2]
    return (6.0 - wave_field) * vector - neighbours

def inner_sums(left, right):
    real_sum = jnp.sum(left[0] * right[0] + left[1] * right[1])
    imag_sum = jnp.sum(left[0] * right[1] - left[1] * right[0])
    return (real_sum, imag_sum)

def scaled_by(factor, vector):
    real_part = factor[0] * vector[0] - factor[1] * vector[1]
    imag_part = factor[0] * vector[1] + factor[1] * vector[0]
    return jnp.stack([real_part, imag_part])

def reference(source, speed):
    wave_field = wave_square / (speed * speed)
    source_size = jnp.sqrt(jnp.sum(source * source) + epsilon)
    basis_one = source / source_size
    solved_one = precondition(basis_one)
    applied = operate(solved_one, wave_field)
    one_re, one_im = inner_sums(basis_one, applied)
    remainder = applied - scaled_by((one_re, one_im), basis_one)
    two_one = jnp.sqrt(jnp.sum(remainder * remainder) + epsilon)
    denominator = one_re * one_re + one_im * one_im + two_one * two_one
    weight = (source_size * one_re / denominator, -source_size * one_im / denominator)
    return scaled_by(weight, solved_one)
```

```python
import functools

import jax
import jax.numpy as jnp
import numpy as np
from jax import lax
from jax.experimental import pallas as pl
from jax.experimental.pallas import tpu as pltpu
from jax.sharding import PartitionSpec as P

wave_square = 0.25
damped = 0.125
epsilon = 1e-06
rows = 8
lanes = 128
MESH = pl.DeviceIdType.MESH


def sine_table(length):
    index = np.arange(length, dtype=np.int64) + 1
    turns = (index[:, None] * index[None, :]) % (2 * (length + 1))
    table = np.sqrt(2.0 / (length + 1.0)) * np.sin(np.pi * turns / (length + 1.0))
    high = table.astype(np.float32).astype(jnp.bfloat16)
    low = (table - high.astype(np.float64)).astype(np.float32).astype(jnp.bfloat16)
    return jnp.asarray(high), jnp.asarray(low)


def eigen_line(length):
    sine_half = np.sin(np.pi * (np.arange(length) + 1.0) / (2.0 * (length + 1.0)))
    return 4.0 * sine_half * sine_half


def root_table(length_x, length_z):
    half = eigen_line(length_x)[:, None] + eigen_line(length_z)[None, :]
    half = (half + 2.0 - wave_square + 1j * damped) / 2.0
    root = 1.0 / (half + np.sqrt(half * half - 1.0))
    return jnp.asarray(np.stack([root.real, root.imag]).astype(np.float32))


def halves(values):
    high = values.astype(jnp.bfloat16)
    low = (values - high.astype(jnp.float32)).astype(jnp.bfloat16)
    return high, low


def dot_three(left, right):
    dot = functools.partial(jnp.dot, preferred_element_type=jnp.float32)
    return dot(left[0], right[0]) + (dot(left[0], right[1]) + dot(left[1], right[0]))


def times(a, b):
    return a[0] * b[0] - a[1] * b[1], a[0] * b[1] + a[1] * b[0]


def plus(a, b):
    return a[0] + b[0], a[1] + b[1]


def inverse(a):
    scale = 1.0 / (a[0] * a[0] + a[1] * a[1])
    return a[0] * scale, -a[1] * scale


def minus(a, b):
    return a[0] - b[0], a[1] - b[1]


def power(a, number):
    result = None
    while number:
        if number & 1:
            result = a if result is None else times(result, a)
        number >>= 1
        if number:
            a = times(a, a)
    return result


def pair_of(ref, plane=0):
    return ref[plane], ref[plane + 1]


def greet(peers):
    barrier = pltpu.get_barrier_semaphore()
    for peer in peers:
        pl.semaphore_signal(barrier, inc=1, device_id=peer, device_id_type=MESH)
    pl.semaphore_wait(barrier, len(peers))


def around(axis, size):
    me = lax.axis_index(axis)
    return me, [lax.rem(me + k, size) for k in range(1, size)]


def exchange(axis, peers, source, target, sends, receives):
    return [
        pltpu.make_async_remote_copy(
            src_ref=source(peer),
            dst_ref=target,
            send_sem=sends.at[k],
            recv_sem=receives.at[k],
            device_id={axis: peer},
            device_id_type=MESH,
        )
        for k, peer in enumerate(peers)
    ]


def hand_over(step, last, parts, slots, target_of, local_sem, sends, receives):
    me, peers = around("py", parts)

    def copies(i):
        mine = pltpu.make_async_copy(slots.at[i, me], target_of(me, i), local_sem.at[i])
        others = exchange(
            "py", peers, lambda peer: slots.at[i, peer], target_of(me, i), sends.at[i], receives.at[i]
        )
        return [mine] + others

    for copy in copies(step):
        copy.start()

    @pl.when(step == last)
    def _():
        @pl.loop(0, last + 1)
        def _(i):
            for copy in copies(i):
                copy.wait()


def forward_x(x_ref, high_ref, low_ref, out_ref, slots, local_sem, sends, receives):
    _, length, _, _ = x_ref.shape
    flat = x_ref.at[0].reshape(length * rows, lanes)
    table = (high_ref[...], low_ref[...])
    parts, part = out_ref.shape[0], out_ref.shape[3]
    steps = out_ref.shape[2] // rows
    now = pl.program_id(0) * steps + pl.program_id(1)

    @pl.when(now == 0)
    def _():
        greet([{"py": peer} for peer in around("py", parts)[1]])

    for j in range(0, rows, 2):
        pair = [flat[pl.ds(j + k, length, stride=rows), :] for k in range(2)]
        result = dot_three(table, halves(jnp.concatenate(pair, axis=1)))
        for k in range(2):
            for h in range(parts):
                slots[now, h, j + k] = result[h * part : (h + 1) * part, k * lanes : (k + 1) * lanes]

    def target_of(me, i):
        return out_ref.at[me, i // steps, pl.ds(lax.rem(i, steps) * rows, rows)]

    hand_over(now, 2 * steps - 1, parts, slots, target_of, local_sem, sends, receives)


def remote(source, target, sends, receives, place, device):
    return pltpu.make_async_remote_copy(
        src_ref=source,
        dst_ref=target,
        send_sem=sends.at[place],
        recv_sem=receives.at[place],
        device_id=device,
        device_id_type=MESH,
    )


def middle(
    blocks,
    t_ref,
    roots_ref,
    high_ref,
    low_ref,
    out_ref,
    roots,
    jumps,
    tiles,
    modes,
    ends,
    pair,
    pairs,
    answer,
    carry,
    inner,
    edges,
    slots,
    root_sem,
    load_sem,
    ends_send,
    ends_recv,
    pair_send,
    pair_recv,
    carry_send,
    carry_recv,
    edge_send,
    edge_recv,
    own_sem,
    out_send,
    out_recv,
):
    steps, parts, _, number, tile, _ = tiles.shape
    length_z = modes.shape[-1]
    groups, _, _, span, _ = ends.shape
    per, places = span // tile, blocks // 2
    me = lax.axis_index("px")
    side, place = lax.rem(me, 2), lax.div(me, 2)
    other = me + 1 - 2 * side
    mine, across = around("py", parts)
    others = [lax.rem(place + k, places) for k in range(1, places)]
    root_load = pltpu.make_async_copy(
        roots_ref.at[:, pl.ds(pl.multiple_of(mine * roots.shape[1], 8), roots.shape[1])],
        roots,
        root_sem.at[0],
    )
    root_load.start()

    def load(i):
        return pltpu.make_async_copy(
            t_ref.at[:, :, :, pl.ds(pl.multiple_of(i * tile, tile), tile)], tiles.at[i], load_sem.at[i]
        )

    @pl.loop(0, steps)
    def _(i):
        load(i).start()

    greet(
        [{"py": peer} for peer in across]
        + [{"px": other}]
        + [{"px": 2 * peer + side} for peer in others]
    )
    table = (high_ref[...], low_ref[...])
    zero = jnp.zeros((tile, length_z), jnp.float32)
    own_lanes = pl.ds(pl.multiple_of(side * lanes, lanes), lanes)
    root_load.wait()
    jump = power((roots[0, :, own_lanes], roots[1, :, own_lanes]), number)
    jumps[0] = jump[0]
    jumps[1] = jump[1]

    def send_ends(k):
        return remote(ends.at[k, 2], ends.at[k, side], ends_send, ends_recv, k, {"px": other})

    def send_pair(k):
        return [
            remote(
                pair.at[k, :, pl.ds(pl.multiple_of(peer * rows, rows), rows)],
                pairs.at[k, place],
                pair_send.at[k],
                pair_recv.at[k],
                i,
                {"px": 2 * peer + side},
            )
            for i, peer in enumerate(others)
        ]

    def send_carry(k):
        return [
            remote(
                answer.at[k, peer],
                carry.at[k, :, pl.ds(pl.multiple_of(place * rows, rows), rows)],
                carry_send.at[k],
                carry_recv.at[k],
                i,
                {"px": 2 * peer + side},
            )
            for i, peer in enumerate(others)
        ]

    def send_edges(k):
        return remote(inner.at[k, 1 - side], edges.at[k, side], edge_send, edge_recv, k, {"px": other})

    def group_jump(k):
        part = pl.ds(k * span, span) if isinstance(k, int) else pl.ds(pl.multiple_of(k * span, span), span)
        return jumps[0, part], jumps[1, part]

    def tile_root(i):
        part = pl.ds(pl.multiple_of(i * tile, tile), tile)
        return roots[0, part], roots[1, part]

    def forward(k, i):
        s = k * per + i
        load(s).wait()
        for c in range(2):
            pieces = [tiles[s, h, c].reshape(number * tile, lanes) for h in range(parts)]
            result = dot_three(halves(jnp.concatenate(pieces, axis=1)), table)
            modes[s, c] = result.reshape(number, tile, length_z)
        root = tile_root(s)

        def step(j, state):
            first, last = state
            back = number - 1 - j
            last = plus(times(root, last), (modes[s, 0, j], modes[s, 1, j]))
            first = plus(times(root, first), (modes[s, 0, back], modes[s, 1, back]))
            return first, last

        first, last = lax.fori_loop(0, number, step, ((zero, zero), (zero, zero)), unroll=4)
        part = pl.ds(pl.multiple_of(i * tile, tile), tile)
        for h in range(2):
            slot = side + lax.rem(h + side, 2) * (2 - side)
            for plane, value in enumerate(first + last):
                ends[k, slot, plane, part] = value[:, h * lanes : (h + 1) * lanes]

    def merge(k):
        send_ends(k).wait_recv()
        rate = group_jump(k)
        first = plus(pair_of(ends.at[k, 0]), times(rate, pair_of(ends.at[k, 1])))
        last = plus(pair_of(ends.at[k, 1], 2), times(rate, pair_of(ends.at[k, 0], 2)))
        for plane, value in enumerate(first + last):
            pair[k, plane] = value
        own = pl.ds(pl.multiple_of(place * rows, rows), rows)
        pairs[k, place] = pair[k, :, own]
        for copy in send_pair(k):
            copy.start()

    def solve(k):
        for copy in send_pair(k):
            copy.wait_recv()
        own = pl.ds(pl.multiple_of(k * span + place * rows, rows), rows)
        root = (roots[0, own, own_lanes], roots[1, own, own_lanes])
        rate = (jumps[0, own], jumps[1, own])
        rate = times(rate, rate)
        whole = power(root, blocks * number + 1)
        square = times(whole, whole)
        spread = inverse((1.0 - square[0], -square[1]))
        spread = times((-root[0], -root[1]), spread)
        none = jnp.zeros((rows, lanes), jnp.float32)
        from_left, from_right = (none, none), (none, none)
        for q in range(places):
            from_left = plus(pair_of(pairs.at[k, q], 2), times(rate, from_left))
            from_right = plus(pair_of(pairs.at[k, places - 1 - q]), times(rate, from_right))
        before = times(spread, minus(from_right, times(whole, from_left)))
        after = times(spread, minus(from_left, times(whole, from_right)))
        for q in range(places):
            p = places - 1 - q
            for c in range(2):
                answer[k, q, c] = before[c]
                answer[k, p, 2 + c] = after[c]
            before = plus(pair_of(pairs.at[k, q], 2), times(rate, before))
            after = plus(pair_of(pairs.at[k, p]), times(rate, after))
        mine_rows = pl.ds(pl.multiple_of(place * rows, rows), rows)
        carry[k, :, mine_rows] = answer[k, place]
        for copy in send_carry(k):
            copy.start()

    def expand(k):
        for copy in send_carry(k):
            copy.wait_recv()
        rate = group_jump(k)
        before, after = pair_of(carry.at[k]), pair_of(carry.at[k], 2)
        left = before + plus(pair_of(ends.at[k, 1]), times(rate, after))
        right = plus(pair_of(ends.at[k, 0], 2), times(rate, before)) + after
        for q, values in enumerate((left, right)):
            for plane, value in enumerate(values):
                inner[k, q, plane] = value
        send_edges(k).start()
        edges[k, side] = inner[k, side]

    def out_copies(i):
        def target(me):
            return out_ref.at[me, :, :, pl.ds(pl.multiple_of(i * tile, tile), tile)]

        own = pltpu.make_async_copy(slots.at[i, mine], target(mine), own_sem.at[i])
        return [own] + exchange(
            "py", across, lambda peer: slots.at[i, peer], target(mine), out_send.at[i], out_recv.at[i]
        )

    def backward(k, i):
        s = k * per + i
        root = tile_root(s)
        part = pl.ds(pl.multiple_of(i * tile, tile), tile)

        def side_of(plane):
            return tuple(
                jnp.concatenate([edges[k, h, plane + c, part] for h in range(2)], axis=1) for c in range(2)
            )

        before, after = side_of(0), side_of(2)

        def ahead(j, state):
            state = plus(times(root, state), (modes[s, 0, j], modes[s, 1, j]))
            modes[s, 0, j] = state[0]
            modes[s, 1, j] = state[1]
            return state

        last = lax.fori_loop(0, number, ahead, before, unroll=4)
        square = times(root, root)
        scaled = times(root, inverse((1.0 - square[0], -square[1])))
        value = times(scaled, plus(times(root, last), after))

        def back(j, value):
            j = number - 1 - j
            value = times(root, plus(value, (modes[s, 0, j], modes[s, 1, j])))
            modes[s, 0, j] = value[0]
            modes[s, 1, j] = value[1]
            return value

        lax.fori_loop(0, number, back, value, unroll=4)
        for c in range(2):
            result = dot_three(halves(modes[s, c].reshape(number * tile, length_z)), table)
            for h in range(parts):
                slots[s, h, c] = result[:, h * lanes : (h + 1) * lanes].reshape(number, tile, lanes)
        for copy in out_copies(s):
            copy.start()

    lag = 2

    @pl.loop(0, groups)
    def _(k):
        @pl.loop(0, per)
        def _(i):
            forward(k, i)

        send_ends(k).start()

        @pl.when(k >= lag)
        def _():
            merge(k - lag)

    for k in range(max(groups - lag, 0), groups):
        merge(k)
    for k in range(groups):
        solve(k)
    for k in range(groups):
        expand(k)

    @pl.loop(0, groups)
    def _(k):
        send_edges(k).wait_recv()

        @pl.loop(0, per)
        def _(i):
            backward(k, i)

    @pl.loop(0, groups)
    def _(k):
        send_ends(k).wait_send()
        send_edges(k).wait_send()
        for copy in send_pair(k) + send_carry(k):
            copy.wait_send()

    @pl.loop(0, steps)
    def _(i):
        for copy in out_copies(i):
            copy.wait()


def backward_x(t_ref, high_ref, low_ref, source_ref, speed_ref, w_ref, out_ref, sums_ref):
    parts, _, _, _, _ = t_ref.shape
    length = speed_ref.shape[0]
    table = (high_ref[...], low_ref[...])
    flat = w_ref.reshape(2 * length * rows, lanes)
    for c in range(2):
        for j in range(0, rows, 2):
            pair = [
                jnp.concatenate([t_ref[h, c, j + k] for h in range(parts)], axis=0) for k in range(2)
            ]
            result = dot_three(table, halves(jnp.concatenate(pair, axis=1)))
            for k in range(2):
                flat[pl.ds(c * length * rows + j + k, length, stride=rows), :] = result[
                    :, k * lanes : (k + 1) * lanes
                ]

    @pl.when(pl.program_id(0) == 0)
    def _():
        sums_ref[...] = jnp.zeros_like(sums_ref)

    group = 8
    zero = jnp.zeros((rows, lanes), jnp.float32)

    def step(i, sums):
        part = pl.ds(i * group, group)
        speed = speed_ref[part]
        shift = wave_square - wave_square / (speed * speed)
        s_re, s_im, w_re, w_im = source_ref[0, part], source_ref[1, part], w_ref[0, part], w_ref[1, part]
        u_re = s_re + shift * w_re + damped * w_im
        u_im = s_im + shift * w_im - damped * w_re
        terms = (
            s_re * s_re + s_im * s_im,
            s_re * u_re + s_im * u_im,
            s_re * u_im - s_im * u_re,
            u_re * u_re + u_im * u_im,
        )
        return tuple(a + jnp.sum(b, axis=0) for a, b in zip(sums, terms))

    sums = lax.fori_loop(0, length // group, step, (zero,) * 4)
    for k in range(4):
        sums_ref[k] += sums[k]

    @pl.when(pl.program_id(0) == pl.num_programs(0) - 1)
    def _():
        out_ref[...] = jnp.zeros_like(out_ref)
        for k in range(4):
            out_ref[pl.ds(k, 1)] = jnp.sum(sums_ref[k], axis=0, keepdims=True)


def total(blocks, parts, sums_ref, out_ref, slots, sends, receives):
    me = lax.axis_index("px") * parts + lax.axis_index("py")
    peers = []
    for k in range(1, blocks * parts):
        peer = lax.rem(me + k, blocks * parts)
        peers.append({"px": peer // parts, "py": lax.rem(peer, parts)})
    greet(peers)
    copies = [
        pltpu.make_async_remote_copy(
            src_ref=sums_ref,
            dst_ref=slots.at[k],
            send_sem=sends.at[k],
            recv_sem=receives.at[k],
            device_id=peer,
            device_id_type=MESH,
        )
        for k, peer in enumerate(peers)
    ]
    for copy in copies:
        copy.start()
    for copy in copies:
        copy.wait()
    out_ref[...] = sums_ref[...] + jnp.sum(slots[...], axis=0)


def scale(total_ref, w_ref, out_ref):
    sums = jnp.sum(total_ref[...], axis=1, keepdims=True)
    size = sums[0:1] + epsilon
    one_re, one_im, squares = sums[1:2] / size, sums[2:3] / size, sums[3:4] / size
    one = one_re * one_re + one_im * one_im
    denominator = squares - one * (epsilon / size) + epsilon
    spread = (w_ref.shape[2], lanes)
    re = jnp.broadcast_to(one_re / denominator, spread)
    im = jnp.broadcast_to(-one_im / denominator, spread)
    out_ref[0] = re * w_ref[0] - im * w_ref[1]
    out_ref[1] = re * w_ref[1] + im * w_ref[0]


def on_device(blocks, parts, source, speed):
    _, length_x, number, width = source.shape
    length_z = width * parts
    part = length_x // parts
    tile = 2 * rows
    steps = number // rows
    f32 = jnp.float32
    shape = jax.ShapeDtypeStruct
    whole = pl.BlockSpec((length_x, length_x), lambda *_: (0, 0))
    def sequential(n, number=None):
        remote = {} if number is None else {"collective_id": number, "has_side_effects": True}
        return pltpu.CompilerParams(
            dimension_semantics=("arbitrary",) * n, vmem_limit_bytes=60000 * 1024, **remote
        )

    def semaphores(steps):
        dma = pltpu.SemaphoreType.DMA
        return [dma((steps,)), dma((steps, parts - 1)), dma((steps, parts - 1))]

    anywhere = pl.BlockSpec(memory_space=pl.ANY)
    x_high, x_low = sine_table(length_x)
    z_high, z_low = sine_table(length_z)

    held = pl.pallas_call(
        forward_x,
        grid=(2, steps),
        in_specs=[pl.BlockSpec((1, length_x, rows, width), lambda c, y: (c, 0, y, 0)), whole, whole],
        out_specs=anywhere,
        out_shape=shape((parts, 2, number, part, width), f32),
        scratch_shapes=[pltpu.VMEM((2 * steps, parts, rows, part, width), f32)] + semaphores(2 * steps),
        compiler_params=sequential(2, 0),
        name="forward_x",
    )(source, x_high, x_low)
    dma = pltpu.SemaphoreType.DMA
    tiles = part // tile
    span = rows * blocks // 2
    groups, places = part // span, blocks // 2
    back = pl.pallas_call(
        functools.partial(middle, blocks),
        in_specs=[anywhere, anywhere] + [pl.BlockSpec(memory_space=pltpu.VMEM)] * 2,
        out_specs=anywhere,
        out_shape=shape((parts, 2, number, part, width), f32),
        scratch_shapes=[
            pltpu.VMEM((2, part, length_z), f32),
            pltpu.VMEM((2, part, lanes), f32),
            pltpu.VMEM((tiles, parts, 2, number, tile, width), f32),
            pltpu.VMEM((tiles, 2, number, tile, length_z), f32),
            pltpu.VMEM((groups, 3, 4, span, lanes), f32),
            pltpu.VMEM((groups, 4, span, lanes), f32),
            pltpu.VMEM((groups, places, 4, rows, lanes), f32),
            pltpu.VMEM((groups, places, 4, rows, lanes), f32),
            pltpu.VMEM((groups, 4, span, lanes), f32),
            pltpu.VMEM((groups, 2, 4, span, lanes), f32),
            pltpu.VMEM((groups, 2, 4, span, lanes), f32),
            pltpu.VMEM((tiles, parts, 2, number, tile, width), f32),
            dma((1,)),
            dma((tiles,)),
            dma((groups,)),
            dma((groups,)),
        ]
        + [dma((groups, places - 1))] * 4
        + [dma((groups,))] * 2
        + semaphores(tiles),
        compiler_params=sequential(0, 1),
        name="middle",
    )(held, root_table(length_x, length_z), z_high, z_low)
    block = pl.BlockSpec((2, length_x, rows, width), lambda y: (0, 0, y, 0))
    image, sums = pl.pallas_call(
        backward_x,
        grid=(steps,),
        in_specs=[
            pl.BlockSpec((parts, 2, rows, part, width), lambda y: (0, 0, y, 0, 0)),
            whole,
            whole,
            block,
            pl.BlockSpec((length_x, rows, width), lambda y: (0, y, 0)),
        ],
        out_specs=[block, pl.BlockSpec((rows, width), lambda y: (0, 0))],
        out_shape=[shape(source.shape, f32), shape((rows, width), f32)],
        scratch_shapes=[pltpu.VMEM((4, rows, width), f32)],
        compiler_params=sequential(1),
        name="backward_x",
    )(back, x_high, x_low, source, speed)
    peers = blocks * parts - 1
    sums = pl.pallas_call(
        functools.partial(total, blocks, parts),
        in_specs=[pl.BlockSpec(memory_space=pltpu.VMEM)],
        out_specs=pl.BlockSpec(memory_space=pltpu.VMEM),
        out_shape=shape((rows, width), f32),
        scratch_shapes=[
            pltpu.VMEM((peers, rows, width), f32),
            pltpu.SemaphoreType.DMA((peers,)),
            pltpu.SemaphoreType.DMA((peers,)),
        ],
        compiler_params=sequential(0, 3),
        name="total",
    )(sums)
    cut = pl.BlockSpec((2, length_x // 8, number, width), lambda i: (0, i, 0, 0))
    return pl.pallas_call(
        scale,
        grid=(8,),
        in_specs=[pl.BlockSpec((rows, width), lambda i: (0, 0)), cut],
        out_specs=cut,
        out_shape=shape(source.shape, f32),
        compiler_params=sequential(1),
        name="scale",
    )(sums, image)


def solution(mesh):
    return jax.shard_map(
        functools.partial(on_device, mesh.shape["px"], mesh.shape["py"]),
        mesh=mesh,
        in_specs=(P(None, "samples", "px", "py"), P("samples", "px", "py")),
        out_specs=P(None, "samples", "px", "py"),
        check_vma=False,
    )
```

```python
import functools

import jax
import jax.numpy as jnp
import numpy as np
from jax import lax
from jax.experimental import pallas as pl
from jax.experimental.pallas import tpu as pltpu
from jax.sharding import PartitionSpec as P

wave_square = 0.25
damped = 0.125
epsilon = 1e-06
rows = 8
lanes = 128
MESH = pl.DeviceIdType.MESH


def sine_table(length):
    index = np.arange(length, dtype=np.int64) + 1
    turns = (index[:, None] * index[None, :]) % (2 * (length + 1))
    table = np.sqrt(2.0 / (length + 1.0)) * np.sin(np.pi * turns / (length + 1.0))
    high = table.astype(np.float32).astype(jnp.bfloat16)
    low = (table - high.astype(np.float64)).astype(np.float32).astype(jnp.bfloat16)
    return jnp.asarray(high), jnp.asarray(low)


def eigen_line(length):
    sine_half = np.sin(np.pi * (np.arange(length) + 1.0) / (2.0 * (length + 1.0)))
    return 4.0 * sine_half * sine_half


def root_table(length_x, length_z):
    half = eigen_line(length_x)[:, None] + eigen_line(length_z)[None, :]
    half = (half + 2.0 - wave_square + 1j * damped) / 2.0
    root = 1.0 / (half + np.sqrt(half * half - 1.0))
    return jnp.asarray(np.stack([root.real, root.imag]).astype(np.float32))


def halves(values):
    high = values.astype(jnp.bfloat16)
    low = (values - high.astype(jnp.float32)).astype(jnp.bfloat16)
    return high, low


def dot_three(left, right):
    dot = functools.partial(jnp.dot, preferred_element_type=jnp.float32)
    return dot(left[0], right[0]) + (dot(left[0], right[1]) + dot(left[1], right[0]))


def times(a, b):
    return a[0] * b[0] - a[1] * b[1], a[0] * b[1] + a[1] * b[0]


def plus(a, b):
    return a[0] + b[0], a[1] + b[1]


def inverse(a):
    scale = 1.0 / (a[0] * a[0] + a[1] * a[1])
    return a[0] * scale, -a[1] * scale


def minus(a, b):
    return a[0] - b[0], a[1] - b[1]


def power(a, number):
    result = None
    while number:
        if number & 1:
            result = a if result is None else times(result, a)
        number >>= 1
        if number:
            a = times(a, a)
    return result


def pair_of(ref, plane=0):
    return ref[plane], ref[plane + 1]


def greet(peers):
    barrier = pltpu.get_barrier_semaphore()
    for peer in peers:
        pl.semaphore_signal(barrier, inc=1, device_id=peer, device_id_type=MESH)
    pl.semaphore_wait(barrier, len(peers))


def remote(source, target, sends, receives, place, device):
    return pltpu.make_async_remote_copy(
        src_ref=source,
        dst_ref=target,
        send_sem=sends.at[place],
        recv_sem=receives.at[place],
        device_id=device,
        device_id_type=MESH,
    )


def solve_all(
    blocks,
    parts,
    source_ref,
    speed_ref,
    roots_ref,
    x_high_ref,
    x_low_ref,
    high_ref,
    low_ref,
    image_ref,
    total_ref,
    source,
    speed,
    roots,
    jumps,
    tiles,
    modes,
    ends,
    pair,
    pairs,
    answer,
    carry,
    inner,
    edges,
    slots,
    image,
    sums_ref,
    heard,
    source_sem,
    speed_sem,
    root_sem,
    image_sem,
    in_send,
    in_recv,
    ends_send,
    ends_recv,
    pair_send,
    pair_recv,
    carry_send,
    carry_recv,
    edge_send,
    edge_recv,
    out_send,
    out_recv,
    sum_send,
    sum_recv,
):
    steps, _, _, number, tile, _ = tiles.shape
    _, length, _, _ = source.shape
    bands = number // rows
    part = length // parts
    length_z = modes.shape[-1]
    groups, _, _, span, _ = ends.shape
    per, places = span // tile, blocks // 2
    me = lax.axis_index("px")
    side, place = lax.rem(me, 2), lax.div(me, 2)
    other = me + 1 - 2 * side
    mine = lax.axis_index("py")
    beside = {"py": 1 - mine}
    others = [lax.rem(place + k, places) for k in range(1, places)]
    everyone = []
    for k in range(1, blocks * parts):
        peer = lax.rem(me * parts + mine + k, blocks * parts)
        everyone.append({"px": lax.div(peer, parts), "py": lax.rem(peer, parts)})

    def band(y):
        return pl.ds(pl.multiple_of(y * rows, rows), rows)

    def load_source(i):
        return pltpu.make_async_copy(
            source_ref.at[lax.div(i, bands), :, band(lax.rem(i, bands))], source.at[i], source_sem.at[i]
        )

    def load_speed(y):
        return pltpu.make_async_copy(speed_ref.at[:, band(y)], speed.at[y], speed_sem.at[y])

    root_load = pltpu.make_async_copy(
        roots_ref.at[:, pl.ds(pl.multiple_of(mine * part, 8), part)], roots, root_sem.at[0]
    )

    @pl.loop(0, 2 * bands)
    def _(i):
        load_source(i).start()

    root_load.start()

    @pl.loop(0, bands)
    def _(y):
        load_speed(y).start()

    greet(everyone)
    x_table = (x_high_ref[...], x_low_ref[...])

    def slot_of(h, own):
        return own + lax.rem(h + own, 2) * (2 - own)

    def send_in(i):
        c, y = lax.div(i, bands), lax.rem(i, bands)
        return remote(
            tiles.at[:, 2, c, band(y)], tiles.at[:, mine, c, band(y)], in_send, in_recv, i, beside
        )

    @pl.loop(0, 2 * bands)
    def _(i):
        load_source(i).wait()
        c, y = lax.div(i, bands), lax.rem(i, bands)
        flat = source.at[i].reshape(length * rows, lanes)
        for j in range(0, rows, 2):
            pieces = [flat[pl.ds(j + k, length, stride=rows), :] for k in range(2)]
            result = dot_three(x_table, halves(jnp.concatenate(pieces, axis=1)))
            for k in range(2):
                for h in range(parts):
                    block = result[h * part : (h + 1) * part, k * lanes : (k + 1) * lanes]
                    tiles[:, slot_of(h, mine), c, y * rows + j + k] = block.reshape(steps, tile, lanes)
        send_in(i).start()

    table = (high_ref[...], low_ref[...])
    zero = jnp.zeros((tile, length_z), jnp.float32)
    own_lanes = pl.ds(pl.multiple_of(side * lanes, lanes), lanes)
    root_load.wait()
    jump = power((roots[0, :, own_lanes], roots[1, :, own_lanes]), number)
    jumps[0] = jump[0]
    jumps[1] = jump[1]

    def send_ends(k):
        return remote(ends.at[k, 2], ends.at[k, side], ends_send, ends_recv, k, {"px": other})

    def send_pair(k):
        return [
            remote(
                pair.at[k, :, pl.ds(pl.multiple_of(peer * rows, rows), rows)],
                pairs.at[k, place],
                pair_send.at[k],
                pair_recv.at[k],
                i,
                {"px": 2 * peer + side},
            )
            for i, peer in enumerate(others)
        ]

    def send_carry(k):
        return [
            remote(
                answer.at[k, peer],
                carry.at[k, :, pl.ds(pl.multiple_of(place * rows, rows), rows)],
                carry_send.at[k],
                carry_recv.at[k],
                i,
                {"px": 2 * peer + side},
            )
            for i, peer in enumerate(others)
        ]

    def send_edges(k):
        return remote(inner.at[k, 1 - side], edges.at[k, side], edge_send, edge_recv, k, {"px": other})

    def group_jump(k):
        part = pl.ds(k * span, span) if isinstance(k, int) else pl.ds(pl.multiple_of(k * span, span), span)
        return jumps[0, part], jumps[1, part]

    def tile_root(i):
        part = pl.ds(pl.multiple_of(i * tile, tile), tile)
        return roots[0, part], roots[1, part]

    def forward(k, i):
        s = k * per + i
        for c in range(2):
            pieces = [tiles[s, h, c].reshape(number * tile, lanes) for h in range(parts)]
            result = dot_three(halves(jnp.concatenate(pieces, axis=1)), table)
            modes[s, c] = result.reshape(number, tile, length_z)
        root = tile_root(s)

        def step(j, state):
            first, last = state
            back = number - 1 - j
            last = plus(times(root, last), (modes[s, 0, j], modes[s, 1, j]))
            first = plus(times(root, first), (modes[s, 0, back], modes[s, 1, back]))
            return first, last

        first, last = lax.fori_loop(0, number, step, ((zero, zero), (zero, zero)), unroll=4)
        part = pl.ds(pl.multiple_of(i * tile, tile), tile)
        for h in range(2):
            slot = slot_of(h, side)
            for plane, value in enumerate(first + last):
                ends[k, slot, plane, part] = value[:, h * lanes : (h + 1) * lanes]

    def merge(k):
        send_ends(k).wait_recv()
        rate = group_jump(k)
        first = plus(pair_of(ends.at[k, 0]), times(rate, pair_of(ends.at[k, 1])))
        last = plus(pair_of(ends.at[k, 1], 2), times(rate, pair_of(ends.at[k, 0], 2)))
        for plane, value in enumerate(first + last):
            pair[k, plane] = value
        own = pl.ds(pl.multiple_of(place * rows, rows), rows)
        pairs[k, place] = pair[k, :, own]
        for copy in send_pair(k):
            copy.start()

    def solve(k):
        for copy in send_pair(k):
            copy.wait_recv()
        own = pl.ds(pl.multiple_of(k * span + place * rows, rows), rows)
        root = (roots[0, own, own_lanes], roots[1, own, own_lanes])
        rate = (jumps[0, own], jumps[1, own])
        rate = times(rate, rate)
        whole = power(root, blocks * number + 1)
        square = times(whole, whole)
        spread = inverse((1.0 - square[0], -square[1]))
        spread = times((-root[0], -root[1]), spread)
        none = jnp.zeros((rows, lanes), jnp.float32)
        from_left, from_right = (none, none), (none, none)
        for q in range(places):
            from_left = plus(pair_of(pairs.at[k, q], 2), times(rate, from_left))
            from_right = plus(pair_of(pairs.at[k, places - 1 - q]), times(rate, from_right))
        before = times(spread, minus(from_right, times(whole, from_left)))
        after = times(spread, minus(from_left, times(whole, from_right)))
        for q in range(places):
            p = places - 1 - q
            for c in range(2):
                answer[k, q, c] = before[c]
                answer[k, p, 2 + c] = after[c]
            before = plus(pair_of(pairs.at[k, q], 2), times(rate, before))
            after = plus(pair_of(pairs.at[k, p]), times(rate, after))
        mine_rows = pl.ds(pl.multiple_of(place * rows, rows), rows)
        carry[k, :, mine_rows] = answer[k, place]
        for copy in send_carry(k):
            copy.start()

    def expand(k):
        for copy in send_carry(k):
            copy.wait_recv()
        rate = group_jump(k)
        before, after = pair_of(carry.at[k]), pair_of(carry.at[k], 2)
        left = before + plus(pair_of(ends.at[k, 1]), times(rate, after))
        right = plus(pair_of(ends.at[k, 0], 2), times(rate, before)) + after
        for q, values in enumerate((left, right)):
            for plane, value in enumerate(values):
                inner[k, q, plane] = value
        send_edges(k).start()
        edges[k, side] = inner[k, side]

    def send_out(i):
        spot = pl.ds(pl.multiple_of(i * tile, tile), tile)
        return remote(slots.at[2, :, :, spot], slots.at[mine, :, :, spot], out_send, out_recv, i, beside)

    def backward(k, i):
        s = k * per + i
        root = tile_root(s)
        part = pl.ds(pl.multiple_of(i * tile, tile), tile)

        def side_of(plane):
            return tuple(
                jnp.concatenate([edges[k, h, plane + c, part] for h in range(2)], axis=1) for c in range(2)
            )

        before, after = side_of(0), side_of(2)

        def ahead(j, state):
            state = plus(times(root, state), (modes[s, 0, j], modes[s, 1, j]))
            modes[s, 0, j] = state[0]
            modes[s, 1, j] = state[1]
            return state

        last = lax.fori_loop(0, number, ahead, before, unroll=4)
        square = times(root, root)
        scaled = times(root, inverse((1.0 - square[0], -square[1])))
        value = times(scaled, plus(times(root, last), after))

        def back(j, value):
            j = number - 1 - j
            value = times(root, plus(value, (modes[s, 0, j], modes[s, 1, j])))
            modes[s, 0, j] = value[0]
            modes[s, 1, j] = value[1]
            return value

        lax.fori_loop(0, number, back, value, unroll=4)
        for c in range(2):
            result = dot_three(halves(modes[s, c].reshape(number * tile, length_z)), table)
            spot = pl.ds(pl.multiple_of(s * tile, tile), tile)
            for h in range(parts):
                block = result[:, h * lanes : (h + 1) * lanes]
                slots[slot_of(h, mine), c, :, spot] = block.reshape(number, tile, lanes)
        send_out(s).start()

    @pl.loop(0, 2 * bands)
    def _(i):
        send_in(i).wait_recv()

    lag = 2

    @pl.loop(0, groups)
    def _(k):
        @pl.loop(0, per)
        def _(i):
            forward(k, i)

        send_ends(k).start()

        @pl.when(k >= lag)
        def _():
            merge(k - lag)

    for k in range(max(groups - lag, 0), groups):
        merge(k)
    for k in range(groups):
        solve(k)
    for k in range(groups):
        expand(k)

    @pl.loop(0, groups)
    def _(k):
        send_edges(k).wait_recv()

        @pl.loop(0, per)
        def _(i):
            backward(k, i)

    @pl.loop(0, groups)
    def _(k):
        send_ends(k).wait_send()
        send_edges(k).wait_send()
        for copy in send_pair(k) + send_carry(k):
            copy.wait_send()

    @pl.loop(0, 2 * bands)
    def _(i):
        send_in(i).wait_send()

    @pl.loop(0, steps)
    def _(i):
        send_out(i).wait_recv()

    sums_ref[...] = jnp.zeros_like(sums_ref)
    group = 8

    def save(y):
        return pltpu.make_async_copy(image.at[y], image_ref.at[:, :, band(y)], image_sem.at[y])

    @pl.loop(0, bands)
    def _(y):
        load_speed(y).wait()
        flat = image.at[y].reshape(2 * length * rows, lanes)
        for c in range(2):
            for j in range(0, rows, 2):
                pieces = [
                    jnp.concatenate([slots[h, c, y * rows + j + k] for h in range(parts)], axis=0)
                    for k in range(2)
                ]
                result = dot_three(x_table, halves(jnp.concatenate(pieces, axis=1)))
                for k in range(2):
                    flat[pl.ds(c * length * rows + j + k, length, stride=rows), :] = result[
                        :, k * lanes : (k + 1) * lanes
                    ]
        save(y).start()

        def step(i, sums):
            some = pl.ds(i * group, group)
            v = speed[y, some]
            shift = wave_square - wave_square / (v * v)
            s_re, s_im = source[y, some], source[bands + y, some]
            w_re, w_im = image[y, 0, some], image[y, 1, some]
            u_re = s_re + shift * w_re + damped * w_im
            u_im = s_im + shift * w_im - damped * w_re
            terms = (
                s_re * s_re + s_im * s_im,
                s_re * u_re + s_im * u_im,
                s_re * u_im - s_im * u_re,
                u_re * u_re + u_im * u_im,
            )
            return tuple(a + jnp.sum(b, axis=0) for a, b in zip(sums, terms))

        none = jnp.zeros((rows, lanes), jnp.float32)
        sums = lax.fori_loop(0, length // group, step, (none,) * 4)
        for k in range(4):
            sums_ref[pl.ds(k, 1)] += jnp.sum(sums[k], axis=0, keepdims=True)

    copies = [
        remote(sums_ref, heard.at[k], sum_send, sum_recv, k, peer) for k, peer in enumerate(everyone)
    ]
    for copy in copies:
        copy.start()
    for copy in copies:
        copy.wait()
    total_ref[...] = sums_ref[...] + jnp.sum(heard[...], axis=0)

    @pl.loop(0, steps)
    def _(i):
        send_out(i).wait_send()

    @pl.loop(0, bands)
    def _(y):
        save(y).wait()


def scale(total_ref, w_ref, out_ref):
    sums = jnp.sum(total_ref[...], axis=1, keepdims=True)
    size = sums[0:1] + epsilon
    one_re, one_im, squares = sums[1:2] / size, sums[2:3] / size, sums[3:4] / size
    one = one_re * one_re + one_im * one_im
    denominator = squares - one * (epsilon / size) + epsilon
    spread = (w_ref.shape[2], lanes)
    re = jnp.broadcast_to(one_re / denominator, spread)
    im = jnp.broadcast_to(-one_im / denominator, spread)
    out_ref[0] = re * w_ref[0] - im * w_ref[1]
    out_ref[1] = re * w_ref[1] + im * w_ref[0]


def on_device(blocks, parts, source, speed):
    _, length_x, number, width = source.shape
    length_z = width * parts
    part = length_x // parts
    tile = 2 * rows
    bands, tiles = number // rows, part // tile
    span = rows * blocks // 2
    groups, places, peers = part // span, blocks // 2, blocks * parts - 1
    f32 = jnp.float32
    shape, dma = jax.ShapeDtypeStruct, pltpu.SemaphoreType.DMA

    def vmem(*size):
        return pltpu.VMEM(size, f32)

    anywhere, inside = pl.BlockSpec(memory_space=pl.ANY), pl.BlockSpec(memory_space=pltpu.VMEM)
    image, sums = pl.pallas_call(
        functools.partial(solve_all, blocks, parts),
        in_specs=[anywhere] * 3 + [inside] * 4,
        out_specs=[anywhere, inside],
        out_shape=[shape(source.shape, f32), shape((rows, width), f32)],
        scratch_shapes=[
            vmem(2 * bands, length_x, rows, width),
            vmem(bands, length_x, rows, width),
            vmem(2, part, length_z),
            vmem(2, part, lanes),
            vmem(tiles, 3, 2, number, tile, width),
            vmem(tiles, 2, number, tile, length_z),
            vmem(groups, 3, 4, span, lanes),
            vmem(groups, 4, span, lanes),
            vmem(groups, places, 4, rows, lanes),
            vmem(groups, places, 4, rows, lanes),
            vmem(groups, 4, span, lanes),
            vmem(groups, 2, 4, span, lanes),
            vmem(groups, 2, 4, span, lanes),
            vmem(3, 2, number, part, width),
            vmem(bands, 2, length_x, rows, width),
            vmem(rows, width),
            vmem(peers, rows, width),
            dma((2 * bands,)),
            dma((bands,)),
            dma((1,)),
            dma((bands,)),
            dma((2 * bands,)),
            dma((2 * bands,)),
            dma((groups,)),
            dma((groups,)),
        ]
        + [dma((groups, places - 1))] * 4
        + [dma((groups,))] * 2
        + [dma((tiles,))] * 2
        + [dma((peers,))] * 2,
        compiler_params=pltpu.CompilerParams(
            vmem_limit_bytes=65472 * 1024, collective_id=0, has_side_effects=True
        ),
        name="solve_all",
    )(source, speed, root_table(length_x, length_z), *sine_table(length_x), *sine_table(length_z))
    cut = pl.BlockSpec((2, length_x // 8, number, width), lambda i: (0, i, 0, 0))
    return pl.pallas_call(
        scale,
        grid=(8,),
        in_specs=[pl.BlockSpec((rows, width), lambda i: (0, 0)), cut],
        out_specs=cut,
        out_shape=shape(source.shape, f32),
        compiler_params=pltpu.CompilerParams(
            dimension_semantics=("arbitrary",), vmem_limit_bytes=60000 * 1024
        ),
        name="scale",
    )(sums, image)


def solution(mesh):
    return jax.shard_map(
        functools.partial(on_device, mesh.shape["px"], mesh.shape["py"]),
        mesh=mesh,
        in_specs=(P(None, "samples", "px", "py"), P("samples", "px", "py")),
        out_specs=P(None, "samples", "px", "py"),
        check_vma=False,
    )
```

```python
import functools

import jax
import jax.numpy as jnp
import numpy as np
from jax import lax
from jax.experimental import pallas as pl
from jax.experimental.pallas import tpu as pltpu
from jax.sharding import PartitionSpec as P

wave_square = 0.25
damped = 0.125
epsilon = 1e-06
rows = 8
lanes = 128
MESH = pl.DeviceIdType.MESH


def sine_table(length):
    index = np.arange(length, dtype=np.int64) + 1
    turns = (index[:, None] * index[None, :]) % (2 * (length + 1))
    table = np.sqrt(2.0 / (length + 1.0)) * np.sin(np.pi * turns / (length + 1.0))
    high = table.astype(np.float32).astype(jnp.bfloat16)
    low = (table - high.astype(np.float64)).astype(np.float32).astype(jnp.bfloat16)
    return jnp.asarray(high), jnp.asarray(low)


def eigen_line(length):
    sine_half = np.sin(np.pi * (np.arange(length) + 1.0) / (2.0 * (length + 1.0)))
    return 4.0 * sine_half * sine_half


def root_table(length_x, length_z):
    half = eigen_line(length_x)[:, None] + eigen_line(length_z)[None, :]
    half = (half + 2.0 - wave_square + 1j * damped) / 2.0
    root = 1.0 / (half + np.sqrt(half * half - 1.0))
    return jnp.asarray(np.stack([root.real, root.imag]).astype(np.float32))


def halves(values):
    high = values.astype(jnp.bfloat16)
    low = (values - high.astype(jnp.float32)).astype(jnp.bfloat16)
    return high, low


def dot_three(left, right):
    dot = functools.partial(jnp.dot, preferred_element_type=jnp.float32)
    return dot(left[0], right[0]) + (dot(left[0], right[1]) + dot(left[1], right[0]))


def times(a, b):
    return a[0] * b[0] - a[1] * b[1], a[0] * b[1] + a[1] * b[0]


def plus(a, b):
    return a[0] + b[0], a[1] + b[1]


def inverse(a):
    scale = 1.0 / (a[0] * a[0] + a[1] * a[1])
    return a[0] * scale, -a[1] * scale


def minus(a, b):
    return a[0] - b[0], a[1] - b[1]


def power(a, number):
    result = None
    while number:
        if number & 1:
            result = a if result is None else times(result, a)
        number >>= 1
        if number:
            a = times(a, a)
    return result


def pair_of(ref, plane=0):
    return ref[plane], ref[plane + 1]


def greet(peers):
    barrier = pltpu.get_barrier_semaphore()
    for peer in peers:
        pl.semaphore_signal(barrier, inc=1, device_id=peer, device_id_type=MESH)
    pl.semaphore_wait(barrier, len(peers))


def remote(source, target, sends, receives, place, device):
    return pltpu.make_async_remote_copy(
        src_ref=source,
        dst_ref=target,
        send_sem=sends.at[place],
        recv_sem=receives.at[place],
        device_id=device,
        device_id_type=MESH,
    )


def solve_all(
    blocks,
    parts,
    source_ref,
    speed_ref,
    roots_ref,
    x_high_ref,
    x_low_ref,
    z_high_ref,
    z_low_ref,
    image,
    total_ref,
    source,
    speed,
    roots,
    jumps,
    tiles,
    modes,
    ends,
    pair,
    pairs,
    answer,
    carry,
    inner,
    edges,
    slots,
    x_halves,
    z_halves,
    sums_ref,
    heard,
    source_sem,
    speed_sem,
    table_sem,
    in_send,
    in_recv,
    ends_send,
    ends_recv,
    pair_send,
    pair_recv,
    carry_send,
    carry_recv,
    edge_send,
    edge_recv,
    out_send,
    out_recv,
    sum_send,
    sum_recv,
):
    steps, _, _, number, tile, _ = tiles.shape
    _, length, _, _ = source.shape
    bands = number // rows
    part = length // parts
    length_z = modes.shape[-1]
    groups, _, _, span, _ = ends.shape
    per, places = span // tile, blocks // 2
    me = lax.axis_index("px")
    side, place = lax.rem(me, 2), lax.div(me, 2)
    other = me + 1 - 2 * side
    mine = lax.axis_index("py")
    beside = {"py": 1 - mine}
    others = [lax.rem(place + k, places) for k in range(1, places)]
    everyone = []
    for k in range(1, blocks * parts):
        peer = lax.rem(me * parts + mine + k, blocks * parts)
        everyone.append({"px": lax.div(peer, parts), "py": lax.rem(peer, parts)})

    def band(y):
        return pl.ds(pl.multiple_of(y * rows, rows), rows)

    def load_source(i):
        return pltpu.make_async_copy(
            source_ref.at[lax.div(i, bands), :, band(lax.rem(i, bands))], source.at[i], source_sem.at[i]
        )

    def load_speed(y):
        return pltpu.make_async_copy(speed_ref.at[:, band(y)], speed.at[y], speed_sem.at[y])

    root_rows = pl.ds(pl.multiple_of(mine * part, 8), part)
    tables = [
        (x_high_ref, x_halves.at[0]),
        (x_low_ref, x_halves.at[1]),
        (z_high_ref, z_halves.at[0]),
        (z_low_ref, z_halves.at[1]),
        (roots_ref.at[:, root_rows], roots),
    ]
    tables = [pltpu.make_async_copy(a, b, table_sem.at[k]) for k, (a, b) in enumerate(tables)]
    load_source(0).start()
    for copy in tables:
        copy.start()

    @pl.loop(1, 2 * bands)
    def _(i):
        load_source(i).start()

    @pl.loop(0, bands)
    def _(y):
        load_speed(y).start()

    greet(everyone)
    for copy in tables[:2]:
        copy.wait()
    x_table = (x_halves[0], x_halves[1])

    def slot_of(h, own):
        return own + lax.rem(h + own, 2) * (2 - own)

    def send_in(i):
        c, y = lax.div(i, bands), lax.rem(i, bands)
        return remote(
            tiles.at[:, 2, c, band(y)], tiles.at[:, mine, c, band(y)], in_send, in_recv, i, beside
        )

    @pl.loop(0, 2 * bands)
    def _(i):
        load_source(i).wait()
        c, y = lax.div(i, bands), lax.rem(i, bands)
        flat = source.at[i].reshape(length * rows, lanes)
        for j in range(0, rows, 2):
            pieces = [flat[pl.ds(j + k, length, stride=rows), :] for k in range(2)]
            result = dot_three(x_table, halves(jnp.concatenate(pieces, axis=1)))
            for k in range(2):
                for h in range(parts):
                    block = result[h * part : (h + 1) * part, k * lanes : (k + 1) * lanes]
                    tiles[:, slot_of(h, mine), c, y * rows + j + k] = block.reshape(steps, tile, lanes)
        send_in(i).start()

    for copy in tables[2:]:
        copy.wait()
    table = (z_halves[0], z_halves[1])
    zero = jnp.zeros((tile, length_z), jnp.float32)
    own_lanes = pl.ds(pl.multiple_of(side * lanes, lanes), lanes)
    jump = power((roots[0, :, own_lanes], roots[1, :, own_lanes]), number)
    jumps[0] = jump[0]
    jumps[1] = jump[1]

    def send_ends(k, i):
        spot = pl.ds(pl.multiple_of(i * tile, tile), tile)
        return remote(
            ends.at[k, 2, :, spot],
            ends.at[k, side, :, spot],
            ends_send,
            ends_recv,
            k * per + i,
            {"px": other},
        )

    def send_pair(k):
        return [
            remote(
                pair.at[k, :, pl.ds(pl.multiple_of(peer * rows, rows), rows)],
                pairs.at[k, place],
                pair_send.at[k],
                pair_recv.at[k],
                i,
                {"px": 2 * peer + side},
            )
            for i, peer in enumerate(others)
        ]

    def send_carry(k):
        return [
            remote(
                answer.at[k, peer],
                carry.at[k, :, pl.ds(pl.multiple_of(place * rows, rows), rows)],
                carry_send.at[k],
                carry_recv.at[k],
                i,
                {"px": 2 * peer + side},
            )
            for i, peer in enumerate(others)
        ]

    def send_edges(k):
        return remote(inner.at[k, 1 - side], edges.at[k, side], edge_send, edge_recv, k, {"px": other})

    def group_jump(k):
        part = pl.ds(k * span, span) if isinstance(k, int) else pl.ds(pl.multiple_of(k * span, span), span)
        return jumps[0, part], jumps[1, part]

    def tile_root(i):
        part = pl.ds(pl.multiple_of(i * tile, tile), tile)
        return roots[0, part], roots[1, part]

    def forward(k, i):
        s = k * per + i
        for c in range(2):
            pieces = [tiles[s, h, c].reshape(number * tile, lanes) for h in range(parts)]
            result = dot_three(halves(jnp.concatenate(pieces, axis=1)), table)
            modes[s, c] = result.reshape(number, tile, length_z)
        root = tile_root(s)

        def step(j, state):
            first, last = state
            back = number - 1 - j
            last = plus(times(root, last), (modes[s, 0, j], modes[s, 1, j]))
            first = plus(times(root, first), (modes[s, 0, back], modes[s, 1, back]))
            return first, last

        first, last = lax.fori_loop(0, number, step, ((zero, zero), (zero, zero)), unroll=4)
        part = pl.ds(pl.multiple_of(i * tile, tile), tile)
        for h in range(2):
            slot = slot_of(h, side)
            for plane, value in enumerate(first + last):
                ends[k, slot, plane, part] = value[:, h * lanes : (h + 1) * lanes]
        send_ends(k, i).start()

    def merge(k):
        for i in range(per):
            send_ends(k, i).wait_recv()
        rate = group_jump(k)
        first = plus(pair_of(ends.at[k, 0]), times(rate, pair_of(ends.at[k, 1])))
        last = plus(pair_of(ends.at[k, 1], 2), times(rate, pair_of(ends.at[k, 0], 2)))
        for plane, value in enumerate(first + last):
            pair[k, plane] = value
        own = pl.ds(pl.multiple_of(place * rows, rows), rows)
        pairs[k, place] = pair[k, :, own]
        for copy in send_pair(k):
            copy.start()

    def solve(k):
        for copy in send_pair(k):
            copy.wait_recv()
        own = pl.ds(pl.multiple_of(k * span + place * rows, rows), rows)
        root = (roots[0, own, own_lanes], roots[1, own, own_lanes])
        rate = (jumps[0, own], jumps[1, own])
        rate = times(rate, rate)
        whole = power(root, blocks * number + 1)
        square = times(whole, whole)
        spread = inverse((1.0 - square[0], -square[1]))
        spread = times((-root[0], -root[1]), spread)
        none = jnp.zeros((rows, lanes), jnp.float32)
        from_left, from_right = (none, none), (none, none)
        for q in range(places):
            from_left = plus(pair_of(pairs.at[k, q], 2), times(rate, from_left))
            from_right = plus(pair_of(pairs.at[k, places - 1 - q]), times(rate, from_right))
        before = times(spread, minus(from_right, times(whole, from_left)))
        after = times(spread, minus(from_left, times(whole, from_right)))
        for q in range(places):
            p = places - 1 - q
            for c in range(2):
                answer[k, q, c] = before[c]
                answer[k, p, 2 + c] = after[c]
            before = plus(pair_of(pairs.at[k, q], 2), times(rate, before))
            after = plus(pair_of(pairs.at[k, p]), times(rate, after))
        mine_rows = pl.ds(pl.multiple_of(place * rows, rows), rows)
        carry[k, :, mine_rows] = answer[k, place]
        for copy in send_carry(k):
            copy.start()

    def expand(k):
        for copy in send_carry(k):
            copy.wait_recv()
        rate = group_jump(k)
        before, after = pair_of(carry.at[k]), pair_of(carry.at[k], 2)
        left = before + plus(pair_of(ends.at[k, 1]), times(rate, after))
        right = plus(pair_of(ends.at[k, 0], 2), times(rate, before)) + after
        for q, values in enumerate((left, right)):
            for plane, value in enumerate(values):
                inner[k, q, plane] = value
        send_edges(k).start()
        edges[k, side] = inner[k, side]

    def send_out(i):
        spot = pl.ds(pl.multiple_of(i * tile, tile), tile)
        return remote(slots.at[2, :, :, spot], slots.at[mine, :, :, spot], out_send, out_recv, i, beside)

    wide = 2 if per % 2 == 0 else 1

    def backward(k, i):
        spots = [i * wide + n for n in range(wide)]
        tiles_here = [k * per + spot for spot in spots]
        own = [tile_root(s) for s in tiles_here]

        def side_of(plane):
            return [
                tuple(
                    jnp.concatenate(
                        [
                            edges[k, h, plane + c, pl.ds(pl.multiple_of(spot * tile, tile), tile)]
                            for h in range(2)
                        ],
                        axis=1,
                    )
                    for c in range(2)
                )
                for spot in spots
            ]

        before, after = side_of(0), side_of(2)

        def mode(s, j):
            return modes[s, 0, j], modes[s, 1, j]

        def keep(s, j, value):
            modes[s, 0, j] = value[0]
            modes[s, 1, j] = value[1]

        def ahead(j, states):
            states = [plus(times(r, v), mode(s, j)) for s, r, v in zip(tiles_here, own, states)]
            for s, value in zip(tiles_here, states):
                keep(s, j, value)
            return states

        lasts = lax.fori_loop(0, number, ahead, before, unroll=2)
        values = []
        for root, last, far in zip(own, lasts, after):
            square = times(root, root)
            scaled = times(root, inverse((1.0 - square[0], -square[1])))
            values.append(times(scaled, plus(times(root, last), far)))

        def back(j, values):
            j = number - 1 - j
            values = [times(r, plus(v, mode(s, j))) for s, r, v in zip(tiles_here, own, values)]
            for s, value in zip(tiles_here, values):
                keep(s, j, value)
            return values

        lax.fori_loop(0, number, back, values, unroll=2)

        @pl.loop(0, wide)
        def _(n):
            s = k * per + i * wide + n
            for c in range(2):
                result = dot_three(halves(modes[s, c].reshape(number * tile, length_z)), table)
                spot = pl.ds(pl.multiple_of(s * tile, tile), tile)
                for h in range(parts):
                    block = result[:, h * lanes : (h + 1) * lanes]
                    slots[slot_of(h, mine), c, :, spot] = block.reshape(number, tile, lanes)
            send_out(s).start()

    @pl.loop(0, 2 * bands)
    def _(i):
        send_in(i).wait_recv()

    lag = 2

    @pl.loop(0, groups)
    def _(k):
        @pl.loop(0, per)
        def _(i):
            forward(k, i)

        @pl.when(k >= lag)
        def _():
            merge(k - lag)

    early = 3
    stages = [(k, 3.4, merge, k) for k in range(max(groups - lag, 0), groups)]
    stages += [(k, 6.7, solve, k) for k in range(groups)]
    stages += [(k, 10.0, expand, k) for k in range(min(early, groups))]
    for _, _, stage, k in sorted(stages, key=lambda item: 1.8 * item[0] + item[1]):
        stage(k)

    @pl.loop(0, groups)
    def _(k):
        send_edges(k).wait_recv()

        @pl.loop(0, per // wide)
        def _(i):
            backward(k, i)

        @pl.when(k + early < groups)
        def _():
            expand(k + early)

    @pl.loop(0, groups)
    def _(k):
        send_edges(k).wait_send()
        for copy in [send_ends(k, i) for i in range(per)] + send_pair(k) + send_carry(k):
            copy.wait_send()

    @pl.loop(0, 2 * bands)
    def _(i):
        send_in(i).wait_send()

    @pl.loop(0, steps)
    def _(i):
        send_out(i).wait_recv()

    sums_ref[...] = jnp.zeros_like(sums_ref)
    group = 8

    @pl.loop(0, bands)
    def _(y):
        load_speed(y).wait()
        flat = image.at[y].reshape(2 * length * rows, lanes)
        for c in range(2):
            for j in range(0, rows, 2):
                pieces = [
                    jnp.concatenate([slots[h, c, y * rows + j + k] for h in range(parts)], axis=0)
                    for k in range(2)
                ]
                result = dot_three(x_table, halves(jnp.concatenate(pieces, axis=1)))
                for k in range(2):
                    flat[pl.ds(c * length * rows + j + k, length, stride=rows), :] = result[
                        :, k * lanes : (k + 1) * lanes
                    ]

        def step(i, sums):
            some = pl.ds(i * group, group)
            v = speed[y, some]
            shift = wave_square - wave_square / (v * v)
            s_re, s_im = source[y, some], source[bands + y, some]
            w_re, w_im = image[y, 0, some], image[y, 1, some]
            u_re = s_re + shift * w_re + damped * w_im
            u_im = s_im + shift * w_im - damped * w_re
            terms = (
                s_re * s_re + s_im * s_im,
                s_re * u_re + s_im * u_im,
                s_re * u_im - s_im * u_re,
                u_re * u_re + u_im * u_im,
            )
            return tuple(a + jnp.sum(b, axis=0) for a, b in zip(sums, terms))

        none = jnp.zeros((rows, lanes), jnp.float32)
        sums = lax.fori_loop(0, length // group, step, (none,) * 4)
        for k in range(4):
            sums_ref[pl.ds(k, 1)] += jnp.sum(sums[k], axis=0, keepdims=True)

    copies = [
        remote(sums_ref, heard.at[k], sum_send, sum_recv, k, peer) for k, peer in enumerate(everyone)
    ]
    for copy in copies:
        copy.start()
    for copy in copies:
        copy.wait()
    total_ref[...] = sums_ref[...] + jnp.sum(heard[...], axis=0)

    @pl.loop(0, steps)
    def _(i):
        send_out(i).wait_send()


def scale(total_ref, w_ref, out_ref):
    sums = jnp.sum(total_ref[...], axis=1, keepdims=True)
    size = sums[0:1] + epsilon
    one_re, one_im, squares = sums[1:2] / size, sums[2:3] / size, sums[3:4] / size
    one = one_re * one_re + one_im * one_im
    denominator = squares - one * (epsilon / size) + epsilon
    re = jnp.broadcast_to(one_re / denominator, (rows, lanes))
    im = jnp.broadcast_to(-one_im / denominator, (rows, lanes))
    bands, depth = w_ref.shape[0], out_ref.shape[1]
    base = pl.program_id(0) * depth

    @pl.loop(0, depth, unroll=4)
    def _(x):
        for y in range(bands):
            w_re, w_im = w_ref[y, 0, base + x], w_ref[y, 1, base + x]
            out_ref[0, x, y * rows : (y + 1) * rows] = re * w_re - im * w_im
            out_ref[1, x, y * rows : (y + 1) * rows] = re * w_im + im * w_re


def on_device(blocks, parts, source, speed):
    _, length_x, number, width = source.shape
    length_z = width * parts
    part = length_x // parts
    tile = 2 * rows
    bands, tiles = number // rows, part // tile
    span = rows * blocks // 2
    groups, places, peers = part // span, blocks // 2, blocks * parts - 1
    f32 = jnp.float32
    shape, dma = jax.ShapeDtypeStruct, pltpu.SemaphoreType.DMA

    def vmem(*size):
        return pltpu.VMEM(size, f32)

    anywhere, inside = pl.BlockSpec(memory_space=pl.ANY), pl.BlockSpec(memory_space=pltpu.VMEM)
    image, sums = pl.pallas_call(
        functools.partial(solve_all, blocks, parts),
        in_specs=[anywhere] * 7,
        out_specs=[inside, inside],
        out_shape=[vmem(bands, 2, length_x, rows, width), vmem(rows, width)],
        scratch_shapes=[
            vmem(2 * bands, length_x, rows, width),
            vmem(bands, length_x, rows, width),
            vmem(2, part, length_z),
            vmem(2, part, lanes),
            vmem(tiles, 3, 2, number, tile, width),
            vmem(tiles, 2, number, tile, length_z),
            vmem(groups, 3, 4, span, lanes),
            vmem(groups, 4, span, lanes),
            vmem(groups, places, 4, rows, lanes),
            vmem(groups, places, 4, rows, lanes),
            vmem(groups, 4, span, lanes),
            vmem(groups, 2, 4, span, lanes),
            vmem(groups, 2, 4, span, lanes),
            vmem(3, 2, number, part, width),
            pltpu.VMEM((2, length_x, length_x), jnp.bfloat16),
            pltpu.VMEM((2, length_z, length_z), jnp.bfloat16),
            vmem(rows, width),
            vmem(peers, rows, width),
            dma((2 * bands,)),
            dma((bands,)),
            dma((5,)),
            dma((2 * bands,)),
            dma((2 * bands,)),
        ]
        + [dma((tiles,))] * 2
        + [dma((groups, places - 1))] * 4
        + [dma((groups,))] * 2
        + [dma((tiles,))] * 2
        + [dma((peers,))] * 2,
        compiler_params=pltpu.CompilerParams(
            vmem_limit_bytes=55 * 1024 * 1024, collective_id=0, has_side_effects=True
        ),
        name="solve_all",
    )(source, speed, root_table(length_x, length_z), *sine_table(length_x), *sine_table(length_z))
    pieces = 8
    return pl.pallas_call(
        scale,
        grid=(pieces,),
        in_specs=[inside, inside],
        out_specs=pl.BlockSpec((2, length_x // pieces, number, width), lambda i: (0, i, 0, 0)),
        out_shape=shape(source.shape, f32),
        compiler_params=pltpu.CompilerParams(
            dimension_semantics=("arbitrary",), vmem_limit_bytes=16 * 1024 * 1024
        ),
        name="scale",
    )(sums, image)


def solution(mesh):
    return jax.shard_map(
        functools.partial(on_device, mesh.shape["px"], mesh.shape["py"]),
        mesh=mesh,
        in_specs=(P(None, "samples", "px", "py"), P("samples", "px", "py")),
        out_specs=P(None, "samples", "px", "py"),
        check_vma=False,
    )
```

```python
import functools

import jax
import jax.numpy as jnp
import numpy as np
from jax import lax
from jax.experimental import pallas as pl
from jax.experimental.pallas import tpu as pltpu
from jax.sharding import PartitionSpec as P

wave_square = 0.25
damped = 0.125
epsilon = 1e-06
rows = 8
lanes = 128
MESH = pl.DeviceIdType.MESH


def sine_table(length):
    index = np.arange(length, dtype=np.int64) + 1
    turns = (index[:, None] * index[None, :]) % (2 * (length + 1))
    table = np.sqrt(2.0 / (length + 1.0)) * np.sin(np.pi * turns / (length + 1.0))
    high = table.astype(np.float32).astype(jnp.bfloat16)
    low = (table - high.astype(np.float64)).astype(np.float32).astype(jnp.bfloat16)
    return jnp.asarray(high), jnp.asarray(low)


def eigen_line(length):
    sine_half = np.sin(np.pi * (np.arange(length) + 1.0) / (2.0 * (length + 1.0)))
    return 4.0 * sine_half * sine_half


def root_table(length_x, length_z):
    half = eigen_line(length_x)[:, None] + eigen_line(length_z)[None, :]
    half = (half + 2.0 - wave_square + 1j * damped) / 2.0
    root = 1.0 / (half + np.sqrt(half * half - 1.0))
    return jnp.asarray(np.stack([root.real, root.imag]).astype(np.float32))


def halves(values):
    high = values.astype(jnp.bfloat16)
    low = (values - high.astype(jnp.float32)).astype(jnp.bfloat16)
    return high, low


def dot_three(left, right):
    dot = functools.partial(jnp.dot, preferred_element_type=jnp.float32)
    return dot(left[0], right[0]) + (dot(left[0], right[1]) + dot(left[1], right[0]))


def times(a, b):
    return a[0] * b[0] - a[1] * b[1], a[0] * b[1] + a[1] * b[0]


def plus(a, b):
    return a[0] + b[0], a[1] + b[1]


def inverse(a):
    scale = 1.0 / (a[0] * a[0] + a[1] * a[1])
    return a[0] * scale, -a[1] * scale


def minus(a, b):
    return a[0] - b[0], a[1] - b[1]


def power(a, number):
    result = None
    while number:
        if number & 1:
            result = a if result is None else times(result, a)
        number >>= 1
        if number:
            a = times(a, a)
    return result


def pair_of(ref, plane=0):
    return ref[plane], ref[plane + 1]


def greet(peers):
    barrier = pltpu.get_barrier_semaphore()
    for peer in peers:
        pl.semaphore_signal(barrier, inc=1, device_id=peer, device_id_type=MESH)
    pl.semaphore_wait(barrier, len(peers))


def remote(source, target, sends, receives, place, device):
    return pltpu.make_async_remote_copy(
        src_ref=source,
        dst_ref=target,
        send_sem=sends.at[place],
        recv_sem=receives.at[place],
        device_id=device,
        device_id_type=MESH,
    )


def solve_all(
    blocks,
    parts,
    source_ref,
    speed_ref,
    roots_ref,
    x_high_ref,
    x_low_ref,
    z_high_ref,
    z_low_ref,
    image,
    total_ref,
    source,
    speed,
    roots,
    rates,
    tiles,
    modes,
    ends,
    pair,
    waves_out,
    waves,
    inner,
    edges,
    slots,
    x_halves,
    z_halves,
    sums_ref,
    heard,
    source_sem,
    speed_sem,
    table_sem,
    in_send,
    in_recv,
    ends_send,
    ends_recv,
    wave_send,
    wave_recv,
    edge_send,
    edge_recv,
    out_send,
    out_recv,
    sum_send,
    sum_recv,
):
    steps, _, _, number, tile, _ = tiles.shape
    _, length, _, _ = source.shape
    bands = number // rows
    part = length // parts
    length_z = modes.shape[-1]
    groups, _, _, span, _ = ends.shape
    per, places = span // tile, blocks // 2
    me = lax.axis_index("px")
    side, place = lax.rem(me, 2), lax.div(me, 2)
    other = me + 1 - 2 * side
    mine = lax.axis_index("py")
    beside = {"py": 1 - mine}
    depths = places // 2
    behind = lax.div(place, depths)
    depth = place + behind * (places - 1 - 2 * place)
    inmost = lax.div(depth + 1, depths)
    toward = 1 - 2 * behind
    everyone = []
    for k in range(1, blocks * parts):
        peer = lax.rem(me * parts + mine + k, blocks * parts)
        everyone.append({"px": lax.div(peer, parts), "py": lax.rem(peer, parts)})

    def band(y):
        return pl.ds(pl.multiple_of(y * rows, rows), rows)

    def load_source(i):
        return pltpu.make_async_copy(
            source_ref.at[lax.div(i, bands), :, band(lax.rem(i, bands))], source.at[i], source_sem.at[i]
        )

    def load_speed(y):
        return pltpu.make_async_copy(speed_ref.at[:, band(y)], speed.at[y], speed_sem.at[y])

    root_rows = pl.ds(pl.multiple_of(mine * part, 8), part)
    tables = [
        (x_high_ref, x_halves.at[0]),
        (x_low_ref, x_halves.at[1]),
        (z_high_ref, z_halves.at[0]),
        (z_low_ref, z_halves.at[1]),
        (roots_ref.at[:, root_rows], roots),
    ]
    tables = [pltpu.make_async_copy(a, b, table_sem.at[k]) for k, (a, b) in enumerate(tables)]
    load_source(0).start()
    for copy in tables:
        copy.start()

    @pl.loop(1, 2 * bands)
    def _(i):
        load_source(i).start()

    @pl.loop(0, bands)
    def _(y):
        load_speed(y).start()

    greet(everyone)
    for copy in tables[:2]:
        copy.wait()
    x_table = (x_halves[0], x_halves[1])

    def slot_of(h, own):
        return own + lax.rem(h + own, 2) * (2 - own)

    def send_in(i):
        c, y = lax.div(i, bands), lax.rem(i, bands)
        return remote(
            tiles.at[:, 2, c, band(y)], tiles.at[:, mine, c, band(y)], in_send, in_recv, i, beside
        )

    @pl.loop(0, 2 * bands)
    def _(i):
        load_source(i).wait()
        c, y = lax.div(i, bands), lax.rem(i, bands)
        flat = source.at[i].reshape(length * rows, lanes)
        for j in range(0, rows, 2):
            pieces = [flat[pl.ds(j + k, length, stride=rows), :] for k in range(2)]
            result = dot_three(x_table, halves(jnp.concatenate(pieces, axis=1)))
            for k in range(2):
                for h in range(parts):
                    block = result[h * part : (h + 1) * part, k * lanes : (k + 1) * lanes]
                    tiles[:, slot_of(h, mine), c, y * rows + j + k] = block.reshape(steps, tile, lanes)
        send_in(i).start()

    for copy in tables[2:]:
        copy.wait()
    table = (z_halves[0], z_halves[1])
    zero = jnp.zeros((tile, length_z), jnp.float32)
    own_lanes = pl.ds(pl.multiple_of(side * lanes, lanes), lanes)
    root = (roots[0, :, own_lanes], roots[1, :, own_lanes])
    jump = power(root, number)
    rate = times(jump, jump)
    double = times(rate, rate)
    echo = (-root[0], -root[1])
    for n in range(1, depths):
        deeper = times(echo, double)
        echo = tuple(jnp.where(depth >= n, a, b) for a, b in zip(deeper, echo))
    whole = power(root, blocks * number + 1)
    square = times(whole, whole)
    spread = inverse((1.0 - square[0], -square[1]))
    for n, values in enumerate((jump, rate, echo, whole, spread)):
        rates[2 * n] = values[0]
        rates[2 * n + 1] = values[1]

    def send_ends(k, i):
        spot = pl.ds(pl.multiple_of(i * tile, tile), tile)
        return remote(
            ends.at[k, 2, :, spot],
            ends.at[k, side, :, spot],
            ends_send,
            ends_recv,
            k * per + i,
            {"px": other},
        )

    def wave(k, way, slot, place):
        return pltpu.make_async_remote_copy(
            src_ref=waves_out.at[k, way],
            dst_ref=waves.at[k, slot],
            send_sem=wave_send.at[2 * k + way],
            recv_sem=wave_recv.at[2 * k + slot],
            device_id={"px": 2 * place + side},
            device_id_type=MESH,
        )

    def send_inward(k):
        return wave(k, 0, inmost, place + toward)

    def send_outward(k):
        return wave(k, 1, 1, place - toward)

    def send_edges(k):
        return remote(inner.at[k, 1 - side], edges.at[k, side], edge_send, edge_recv, k, {"px": other})

    def group_rates(k, *which):
        part = pl.ds(k * span, span) if isinstance(k, int) else pl.ds(pl.multiple_of(k * span, span), span)
        return [(rates[2 * n, part], rates[2 * n + 1, part]) for n in which]

    def tile_root(i):
        part = pl.ds(pl.multiple_of(i * tile, tile), tile)
        return roots[0, part], roots[1, part]

    def forward(k, i):
        s = k * per + i
        for c in range(2):
            pieces = [tiles[s, h, c].reshape(number * tile, lanes) for h in range(parts)]
            result = dot_three(halves(jnp.concatenate(pieces, axis=1)), table)
            modes[s, c] = result.reshape(number, tile, length_z)
        root = tile_root(s)

        def step(j, state):
            first, last = state
            back = number - 1 - j
            last = plus(times(root, last), (modes[s, 0, j], modes[s, 1, j]))
            first = plus(times(root, first), (modes[s, 0, back], modes[s, 1, back]))
            return first, last

        first, last = lax.fori_loop(0, number, step, ((zero, zero), (zero, zero)), unroll=4)
        part = pl.ds(pl.multiple_of(i * tile, tile), tile)
        for h in range(2):
            slot = slot_of(h, side)
            for plane, value in enumerate(first + last):
                ends[k, slot, plane, part] = value[:, h * lanes : (h + 1) * lanes]
        send_ends(k, i).start()

    def either(a, b):
        return tuple(jnp.where(behind == 0, x, y) for x, y in zip(a, b))

    def pass_inward(k, rate, echo, came):
        bounced = times(echo, pair_of(pair.at[k], 2))
        value = plus(pair_of(pair.at[k]), times(rate, plus(came, bounced)))
        for c in range(2):
            waves_out[k, 0, c] = value[c]
        send_inward(k).start()

    def merge(k):
        for i in range(per):
            send_ends(k, i).wait_recv()
        jump, rate, echo = group_rates(k, 0, 1, 2)
        first = plus(pair_of(ends.at[k, 0]), times(jump, pair_of(ends.at[k, 1])))
        last = plus(pair_of(ends.at[k, 1], 2), times(jump, pair_of(ends.at[k, 0], 2)))
        for plane, value in enumerate(either(last, first) + either(first, last)):
            pair[k, plane] = value

        @pl.when(depth == 0)
        def _():
            none = jnp.zeros((span, lanes), jnp.float32)
            for c in range(2):
                waves[k, 0, c] = none
            pass_inward(k, rate, echo, (none, none))

    def relay(k):
        @pl.when(depth > 0)
        def _():
            wave(k, 0, 0, place - toward).wait_recv()
            rate, echo = group_rates(k, 1, 2)
            pass_inward(k, rate, echo, pair_of(waves.at[k, 0]))

    def expand(k):
        wave(k, 1, 1, place + toward).wait_recv()
        jump, rate, echo, whole, spread = group_rates(k, 0, 1, 2, 3, 4)
        came = pair_of(waves.at[k, 1])
        met = times(spread, minus(came, times(whole, pair_of(waves_out.at[k, 0]))))
        came = tuple(jnp.where(inmost == 1, a, b) for a, b in zip(met, came))
        out = plus(pair_of(pair.at[k], 2), times(rate, came))
        back = plus(pair_of(waves.at[k, 0]), times(echo, out))

        @pl.when(depth > 0)
        def _():
            for c in range(2):
                waves_out[k, 1, c] = out[c]
            send_outward(k).start()

        before, after = either(back, came), either(came, back)
        left = before + plus(pair_of(ends.at[k, 1]), times(jump, after))
        right = plus(pair_of(ends.at[k, 0], 2), times(jump, before)) + after
        for q, values in enumerate((left, right)):
            for plane, value in enumerate(values):
                inner[k, q, plane] = value
        send_edges(k).start()
        edges[k, side] = inner[k, side]

    def send_out(i):
        spot = pl.ds(pl.multiple_of(i * tile, tile), tile)
        return remote(slots.at[2, :, :, spot], slots.at[mine, :, :, spot], out_send, out_recv, i, beside)

    wide = 2 if per % 2 == 0 else 1

    def backward(k, i):
        spots = [i * wide + n for n in range(wide)]
        tiles_here = [k * per + spot for spot in spots]
        own = [tile_root(s) for s in tiles_here]

        def side_of(plane):
            return [
                tuple(
                    jnp.concatenate(
                        [
                            edges[k, h, plane + c, pl.ds(pl.multiple_of(spot * tile, tile), tile)]
                            for h in range(2)
                        ],
                        axis=1,
                    )
                    for c in range(2)
                )
                for spot in spots
            ]

        before, after = side_of(0), side_of(2)

        def mode(s, j):
            return modes[s, 0, j], modes[s, 1, j]

        def keep(s, j, value):
            modes[s, 0, j] = value[0]
            modes[s, 1, j] = value[1]

        def ahead(j, states):
            states = [plus(times(r, v), mode(s, j)) for s, r, v in zip(tiles_here, own, states)]
            for s, value in zip(tiles_here, states):
                keep(s, j, value)
            return states

        lasts = lax.fori_loop(0, number, ahead, before, unroll=2)
        values = []
        for root, last, far in zip(own, lasts, after):
            square = times(root, root)
            scaled = times(root, inverse((1.0 - square[0], -square[1])))
            values.append(times(scaled, plus(times(root, last), far)))

        def back(j, values):
            j = number - 1 - j
            values = [times(r, plus(v, mode(s, j))) for s, r, v in zip(tiles_here, own, values)]
            for s, value in zip(tiles_here, values):
                keep(s, j, value)
            return values

        lax.fori_loop(0, number, back, values, unroll=2)

        @pl.loop(0, wide)
        def _(n):
            s = k * per + i * wide + n
            for c in range(2):
                result = dot_three(halves(modes[s, c].reshape(number * tile, length_z)), table)
                spot = pl.ds(pl.multiple_of(s * tile, tile), tile)
                for h in range(parts):
                    block = result[:, h * lanes : (h + 1) * lanes]
                    slots[slot_of(h, mine), c, :, spot] = block.reshape(number, tile, lanes)
            send_out(s).start()

    @pl.loop(0, 2 * bands)
    def _(i):
        send_in(i).wait_recv()

    lag = 2

    @pl.loop(0, groups)
    def _(k):
        @pl.loop(0, per)
        def _(i):
            forward(k, i)

        @pl.when(k >= lag)
        def _():
            merge(k - lag)

    early = 3
    stages = [(2.9, merge, k) for k in range(max(groups - lag, 0), groups)]
    stages += [(5.2, relay, k) for k in range(groups)]
    stages += [(8.7, expand, k) for k in range(min(early, groups))]
    for _, stage, k in sorted(stages, key=lambda item: 1.8 * item[2] + item[0]):
        stage(k)

    @pl.loop(0, groups)
    def _(k):
        send_edges(k).wait_recv()

        @pl.loop(0, per // wide)
        def _(i):
            backward(k, i)

        @pl.when(k + early < groups)
        def _():
            expand(k + early)

    @pl.loop(0, groups)
    def _(k):
        send_edges(k).wait_send()
        send_inward(k).wait_send()
        for i in range(per):
            send_ends(k, i).wait_send()

        @pl.when(depth > 0)
        def _():
            send_outward(k).wait_send()

    @pl.loop(0, 2 * bands)
    def _(i):
        send_in(i).wait_send()

    @pl.loop(0, steps)
    def _(i):
        send_out(i).wait_recv()

    sums_ref[...] = jnp.zeros_like(sums_ref)
    group = 8

    @pl.loop(0, bands)
    def _(y):
        load_speed(y).wait()
        flat = image.at[y].reshape(2 * length * rows, lanes)
        for c in range(2):
            for j in range(0, rows, 2):
                pieces = [
                    jnp.concatenate([slots[h, c, y * rows + j + k] for h in range(parts)], axis=0)
                    for k in range(2)
                ]
                result = dot_three(x_table, halves(jnp.concatenate(pieces, axis=1)))
                for k in range(2):
                    flat[pl.ds(c * length * rows + j + k, length, stride=rows), :] = result[
                        :, k * lanes : (k + 1) * lanes
                    ]

        def step(i, sums):
            some = pl.ds(i * group, group)
            v = speed[y, some]
            shift = wave_square - wave_square / (v * v)
            s_re, s_im = source[y, some], source[bands + y, some]
            w_re, w_im = image[y, 0, some], image[y, 1, some]
            u_re = s_re + shift * w_re + damped * w_im
            u_im = s_im + shift * w_im - damped * w_re
            terms = (
                s_re * s_re + s_im * s_im,
                s_re * u_re + s_im * u_im,
                s_re * u_im - s_im * u_re,
                u_re * u_re + u_im * u_im,
            )
            return tuple(a + jnp.sum(b, axis=0) for a, b in zip(sums, terms))

        none = jnp.zeros((rows, lanes), jnp.float32)
        sums = lax.fori_loop(0, length // group, step, (none,) * 4)
        for k in range(4):
            sums_ref[pl.ds(k, 1)] += jnp.sum(sums[k], axis=0, keepdims=True)

    copies = [
        remote(sums_ref, heard.at[k], sum_send, sum_recv, k, peer) for k, peer in enumerate(everyone)
    ]
    for copy in copies:
        copy.start()
    for copy in copies:
        copy.wait()
    total_ref[...] = sums_ref[...] + jnp.sum(heard[...], axis=0)

    @pl.loop(0, steps)
    def _(i):
        send_out(i).wait_send()


def scale(total_ref, w_ref, out_ref):
    sums = jnp.sum(total_ref[...], axis=1, keepdims=True)
    size = sums[0:1] + epsilon
    one_re, one_im, squares = sums[1:2] / size, sums[2:3] / size, sums[3:4] / size
    one = one_re * one_re + one_im * one_im
    denominator = squares - one * (epsilon / size) + epsilon
    re = jnp.broadcast_to(one_re / denominator, (rows, lanes))
    im = jnp.broadcast_to(-one_im / denominator, (rows, lanes))
    bands, depth = w_ref.shape[0], out_ref.shape[1]
    base = pl.program_id(0) * depth

    @pl.loop(0, depth, unroll=4)
    def _(x):
        for y in range(bands):
            w_re, w_im = w_ref[y, 0, base + x], w_ref[y, 1, base + x]
            out_ref[0, x, y * rows : (y + 1) * rows] = re * w_re - im * w_im
            out_ref[1, x, y * rows : (y + 1) * rows] = re * w_im + im * w_re


def on_device(blocks, parts, source, speed):
    _, length_x, number, width = source.shape
    length_z = width * parts
    part = length_x // parts
    tile = 2 * rows
    bands, tiles = number // rows, part // tile
    span = rows * blocks // 2
    groups, peers = part // span, blocks * parts - 1
    f32 = jnp.float32
    shape, dma = jax.ShapeDtypeStruct, pltpu.SemaphoreType.DMA

    def vmem(*size):
        return pltpu.VMEM(size, f32)

    anywhere, inside = pl.BlockSpec(memory_space=pl.ANY), pl.BlockSpec(memory_space=pltpu.VMEM)
    image, sums = pl.pallas_call(
        functools.partial(solve_all, blocks, parts),
        in_specs=[anywhere] * 7,
        out_specs=[inside, inside],
        out_shape=[vmem(bands, 2, length_x, rows, width), vmem(rows, width)],
        scratch_shapes=[
            vmem(2 * bands, length_x, rows, width),
            vmem(bands, length_x, rows, width),
            vmem(2, part, length_z),
            vmem(10, part, lanes),
            vmem(tiles, 3, 2, number, tile, width),
            vmem(tiles, 2, number, tile, length_z),
            vmem(groups, 3, 4, span, lanes),
            vmem(groups, 4, span, lanes),
            vmem(groups, 2, 2, span, lanes),
            vmem(groups, 2, 2, span, lanes),
            vmem(groups, 2, 4, span, lanes),
            vmem(groups, 2, 4, span, lanes),
            vmem(3, 2, number, part, width),
            pltpu.VMEM((2, length_x, length_x), jnp.bfloat16),
            pltpu.VMEM((2, length_z, length_z), jnp.bfloat16),
            vmem(rows, width),
            vmem(peers, rows, width),
            dma((2 * bands,)),
            dma((bands,)),
            dma((5,)),
            dma((2 * bands,)),
            dma((2 * bands,)),
        ]
        + [dma((tiles,))] * 2
        + [dma((2 * groups,))] * 2
        + [dma((groups,))] * 2
        + [dma((tiles,))] * 2
        + [dma((peers,))] * 2,
        compiler_params=pltpu.CompilerParams(
            vmem_limit_bytes=55 * 1024 * 1024, collective_id=0, has_side_effects=True
        ),
        name="solve_all",
    )(source, speed, root_table(length_x, length_z), *sine_table(length_x), *sine_table(length_z))
    pieces = 8
    return pl.pallas_call(
        scale,
        grid=(pieces,),
        in_specs=[inside, inside],
        out_specs=pl.BlockSpec((2, length_x // pieces, number, width), lambda i: (0, i, 0, 0)),
        out_shape=shape(source.shape, f32),
        compiler_params=pltpu.CompilerParams(
            dimension_semantics=("arbitrary",), vmem_limit_bytes=16 * 1024 * 1024
        ),
        name="scale",
    )(sums, image)


def solution(mesh):
    return jax.shard_map(
        functools.partial(on_device, mesh.shape["px"], mesh.shape["py"]),
        mesh=mesh,
        in_specs=(P(None, "samples", "px", "py"), P("samples", "px", "py")),
        out_specs=P(None, "samples", "px", "py"),
        check_vma=False,
    )
```

```python
import functools

import jax
import jax.numpy as jnp
import numpy as np
from jax import lax
from jax.experimental import pallas as pl
from jax.experimental.pallas import tpu as pltpu
from jax.sharding import PartitionSpec as P

wave_square = 0.25
damped = 0.125
epsilon = 1e-06
rows = 8
lanes = 128
MESH = pl.DeviceIdType.MESH


def sine_table(length):
    index = np.arange(length, dtype=np.int64) + 1
    turns = (index[:, None] * index[None, :]) % (2 * (length + 1))
    table = np.sqrt(2.0 / (length + 1.0)) * np.sin(np.pi * turns / (length + 1.0))
    high = table.astype(np.float32).astype(jnp.bfloat16)
    low = (table - high.astype(np.float64)).astype(np.float32).astype(jnp.bfloat16)
    return jnp.asarray(high), jnp.asarray(low)


def eigen_line(length):
    sine_half = np.sin(np.pi * (np.arange(length) + 1.0) / (2.0 * (length + 1.0)))
    return 4.0 * sine_half * sine_half


def root_table(length_x, length_z):
    half = eigen_line(length_x)[:, None] + eigen_line(length_z)[None, :]
    half = (half + 2.0 - wave_square + 1j * damped) / 2.0
    root = 1.0 / (half + np.sqrt(half * half - 1.0))
    return jnp.asarray(np.stack([root.real, root.imag]).astype(np.float32))


def halves(values):
    high = values.astype(jnp.bfloat16)
    low = (values - high.astype(jnp.float32)).astype(jnp.bfloat16)
    return high, low


def dot_three(left, right):
    dot = functools.partial(jnp.dot, preferred_element_type=jnp.float32)
    return dot(left[0], right[0]) + (dot(left[0], right[1]) + dot(left[1], right[0]))


def times(a, b):
    return a[0] * b[0] - a[1] * b[1], a[0] * b[1] + a[1] * b[0]


def plus(a, b):
    return a[0] + b[0], a[1] + b[1]


def inverse(a):
    scale = 1.0 / (a[0] * a[0] + a[1] * a[1])
    return a[0] * scale, -a[1] * scale


def minus(a, b):
    return a[0] - b[0], a[1] - b[1]


def power(a, number):
    result = None
    while number:
        if number & 1:
            result = a if result is None else times(result, a)
        number >>= 1
        if number:
            a = times(a, a)
    return result


def pair_of(ref, plane=0):
    return ref[plane], ref[plane + 1]


def greet(peers):
    barrier = pltpu.get_barrier_semaphore()
    for peer in peers:
        pl.semaphore_signal(barrier, inc=1, device_id=peer, device_id_type=MESH)
    pl.semaphore_wait(barrier, len(peers))


def remote(source, target, sends, receives, place, device):
    return pltpu.make_async_remote_copy(
        src_ref=source,
        dst_ref=target,
        send_sem=sends.at[place],
        recv_sem=receives.at[place],
        device_id=device,
        device_id_type=MESH,
    )


def solve_all(
    blocks,
    parts,
    source_ref,
    speed_ref,
    roots_ref,
    x_high_ref,
    x_low_ref,
    z_high_ref,
    z_low_ref,
    image,
    total_ref,
    source,
    speed,
    roots,
    rates,
    tiles,
    modes,
    ends,
    pair,
    waves_out,
    waves,
    inner,
    edges,
    slots,
    x_halves,
    z_halves,
    squares_ref,
    heard,
    source_sem,
    speed_sem,
    table_sem,
    in_send,
    in_recv,
    ends_send,
    ends_recv,
    wave_send,
    wave_recv,
    edge_send,
    edge_recv,
    out_send,
    out_recv,
    sum_send,
    sum_recv,
):
    steps, _, _, number, tile, _ = tiles.shape
    _, length, _, _ = source.shape
    bands = number // rows
    part = length // parts
    length_z = modes.shape[-1]
    groups, _, _, span, _ = ends.shape
    per, places = span // tile, blocks // 2
    me = lax.axis_index("px")
    side, place = lax.rem(me, 2), lax.div(me, 2)
    other = me + 1 - 2 * side
    mine = lax.axis_index("py")
    beside = {"py": 1 - mine}
    depths = places // 2
    behind = lax.div(place, depths)
    depth = place + behind * (places - 1 - 2 * place)
    inmost = lax.div(depth + 1, depths)
    toward = 1 - 2 * behind
    everyone = []
    for k in range(1, blocks * parts):
        peer = lax.rem(me * parts + mine + k, blocks * parts)
        everyone.append({"px": lax.div(peer, parts), "py": lax.rem(peer, parts)})

    def band(y):
        return pl.ds(pl.multiple_of(y * rows, rows), rows)

    def load_source(i):
        return pltpu.make_async_copy(
            source_ref.at[lax.div(i, bands), :, band(lax.rem(i, bands))], source.at[i], source_sem.at[i]
        )

    def load_speed(y):
        return pltpu.make_async_copy(speed_ref.at[:, band(y)], speed.at[y], speed_sem.at[y])

    root_rows = pl.ds(pl.multiple_of(mine * part, 8), part)
    tables = [
        (x_high_ref, x_halves.at[0]),
        (x_low_ref, x_halves.at[1]),
        (z_high_ref, z_halves.at[0]),
        (z_low_ref, z_halves.at[1]),
        (roots_ref.at[:, root_rows], roots),
    ]
    tables = [pltpu.make_async_copy(a, b, table_sem.at[k]) for k, (a, b) in enumerate(tables)]
    load_source(0).start()
    for copy in tables:
        copy.start()

    @pl.loop(1, 2 * bands)
    def _(i):
        load_source(i).start()

    @pl.loop(0, bands)
    def _(y):
        load_speed(y).start()

    greet(everyone)
    for copy in tables[:2]:
        copy.wait()
    x_table = (x_halves[0], x_halves[1])

    def slot_of(h, own):
        return own + lax.rem(h + own, 2) * (2 - own)

    def send_in(i):
        c, y = lax.div(i, bands), lax.rem(i, bands)
        return remote(
            tiles.at[:, 2, c, band(y)], tiles.at[:, mine, c, band(y)], in_send, in_recv, i, beside
        )

    @pl.loop(0, 2 * bands)
    def _(i):
        load_source(i).wait()
        c, y = lax.div(i, bands), lax.rem(i, bands)
        flat = source.at[i].reshape(length * rows, lanes)
        for j in range(0, rows, 2):
            pieces = [flat[pl.ds(j + k, length, stride=rows), :] for k in range(2)]
            result = dot_three(x_table, halves(jnp.concatenate(pieces, axis=1)))
            for k in range(2):
                for h in range(parts):
                    block = result[h * part : (h + 1) * part, k * lanes : (k + 1) * lanes]
                    tiles[:, slot_of(h, mine), c, y * rows + j + k] = block.reshape(steps, tile, lanes)
        send_in(i).start()

    for copy in tables[2:]:
        copy.wait()
    table = (z_halves[0], z_halves[1])
    zero = jnp.zeros((tile, length_z), jnp.float32)
    own_lanes = pl.ds(pl.multiple_of(side * lanes, lanes), lanes)
    root = (roots[0, :, own_lanes], roots[1, :, own_lanes])
    jump = power(root, number)
    rate = times(jump, jump)
    double = times(rate, rate)
    echo = (-root[0], -root[1])
    for n in range(1, depths):
        deeper = times(echo, double)
        echo = tuple(jnp.where(depth >= n, a, b) for a, b in zip(deeper, echo))
    whole = power(root, blocks * number + 1)
    square = times(whole, whole)
    spread = inverse((1.0 - square[0], -square[1]))
    for n, values in enumerate((jump, rate, echo, whole, spread)):
        rates[2 * n] = values[0]
        rates[2 * n + 1] = values[1]

    def send_ends(k, i):
        spot = pl.ds(pl.multiple_of(i * tile, tile), tile)
        return remote(
            ends.at[k, 2, :, spot],
            ends.at[k, side, :, spot],
            ends_send,
            ends_recv,
            k * per + i,
            {"px": other},
        )

    def wave(k, way, slot, place):
        return pltpu.make_async_remote_copy(
            src_ref=waves_out.at[k, way],
            dst_ref=waves.at[k, slot],
            send_sem=wave_send.at[2 * k + way],
            recv_sem=wave_recv.at[2 * k + slot],
            device_id={"px": 2 * place + side},
            device_id_type=MESH,
        )

    def send_inward(k):
        return wave(k, 0, inmost, place + toward)

    def send_outward(k):
        return wave(k, 1, 1, place - toward)

    def send_edges(k):
        return remote(inner.at[k, 1 - side], edges.at[k, side], edge_send, edge_recv, k, {"px": other})

    def group_rates(k, *which):
        part = pl.ds(k * span, span) if isinstance(k, int) else pl.ds(pl.multiple_of(k * span, span), span)
        return [(rates[2 * n, part], rates[2 * n + 1, part]) for n in which]

    def tile_root(i):
        part = pl.ds(pl.multiple_of(i * tile, tile), tile)
        return roots[0, part], roots[1, part]

    def forward(k, i):
        s = k * per + i
        for c in range(2):
            pieces = [tiles[s, h, c].reshape(number * tile, lanes) for h in range(parts)]
            result = dot_three(halves(jnp.concatenate(pieces, axis=1)), table)
            modes[s, c] = result.reshape(number, tile, length_z)
        root = tile_root(s)

        def step(j, state):
            first, last = state
            back = number - 1 - j
            last = plus(times(root, last), (modes[s, 0, j], modes[s, 1, j]))
            first = plus(times(root, first), (modes[s, 0, back], modes[s, 1, back]))
            return first, last

        first, last = lax.fori_loop(0, number, step, ((zero, zero), (zero, zero)), unroll=4)
        part = pl.ds(pl.multiple_of(i * tile, tile), tile)
        for h in range(2):
            slot = slot_of(h, side)
            for plane, value in enumerate(first + last):
                ends[k, slot, plane, part] = value[:, h * lanes : (h + 1) * lanes]
        send_ends(k, i).start()

    def either(a, b):
        return tuple(jnp.where(behind == 0, x, y) for x, y in zip(a, b))

    def pass_inward(k, rate, echo, came):
        bounced = times(echo, pair_of(pair.at[k], 2))
        value = plus(pair_of(pair.at[k]), times(rate, plus(came, bounced)))
        for c in range(2):
            waves_out[k, 0, c] = value[c]
        send_inward(k).start()

    def merge(k):
        for i in range(per):
            send_ends(k, i).wait_recv()
        jump, rate, echo = group_rates(k, 0, 1, 2)
        first = plus(pair_of(ends.at[k, 0]), times(jump, pair_of(ends.at[k, 1])))
        last = plus(pair_of(ends.at[k, 1], 2), times(jump, pair_of(ends.at[k, 0], 2)))
        for plane, value in enumerate(either(last, first) + either(first, last)):
            pair[k, plane] = value

        @pl.when(depth == 0)
        def _():
            none = jnp.zeros((span, lanes), jnp.float32)
            for c in range(2):
                waves[k, 0, c] = none
            pass_inward(k, rate, echo, (none, none))

    def relay(k):
        @pl.when(depth > 0)
        def _():
            wave(k, 0, 0, place - toward).wait_recv()
            rate, echo = group_rates(k, 1, 2)
            pass_inward(k, rate, echo, pair_of(waves.at[k, 0]))

    def expand(k):
        wave(k, 1, 1, place + toward).wait_recv()
        jump, rate, echo, whole, spread = group_rates(k, 0, 1, 2, 3, 4)
        came = pair_of(waves.at[k, 1])
        met = times(spread, minus(came, times(whole, pair_of(waves_out.at[k, 0]))))
        came = tuple(jnp.where(inmost == 1, a, b) for a, b in zip(met, came))
        out = plus(pair_of(pair.at[k], 2), times(rate, came))
        back = plus(pair_of(waves.at[k, 0]), times(echo, out))

        @pl.when(depth > 0)
        def _():
            for c in range(2):
                waves_out[k, 1, c] = out[c]
            send_outward(k).start()

        before, after = either(back, came), either(came, back)
        left = before + plus(pair_of(ends.at[k, 1]), times(jump, after))
        right = plus(pair_of(ends.at[k, 0], 2), times(jump, before)) + after
        for q, values in enumerate((left, right)):
            for plane, value in enumerate(values):
                inner[k, q, plane] = value
        send_edges(k).start()
        edges[k, side] = inner[k, side]

    def send_out(i):
        spot = pl.ds(pl.multiple_of(i * tile, tile), tile)
        return remote(slots.at[2, :, :, spot], slots.at[mine, :, :, spot], out_send, out_recv, i, beside)

    wide = 2 if per % 2 == 0 else 1

    def backward(k, i):
        spots = [i * wide + n for n in range(wide)]
        tiles_here = [k * per + spot for spot in spots]
        own = [tile_root(s) for s in tiles_here]

        def side_of(plane):
            return [
                tuple(
                    jnp.concatenate(
                        [
                            edges[k, h, plane + c, pl.ds(pl.multiple_of(spot * tile, tile), tile)]
                            for h in range(2)
                        ],
                        axis=1,
                    )
                    for c in range(2)
                )
                for spot in spots
            ]

        before, after = side_of(0), side_of(2)

        def mode(s, j):
            return modes[s, 0, j], modes[s, 1, j]

        def keep(s, j, value):
            modes[s, 0, j] = value[0]
            modes[s, 1, j] = value[1]

        def ahead(j, states):
            states = [plus(times(r, v), mode(s, j)) for s, r, v in zip(tiles_here, own, states)]
            for s, value in zip(tiles_here, states):
                keep(s, j, value)
            return states

        lasts = lax.fori_loop(0, number, ahead, before, unroll=2)
        values = []
        for root, last, far in zip(own, lasts, after):
            square = times(root, root)
            scaled = times(root, inverse((1.0 - square[0], -square[1])))
            values.append(times(scaled, plus(times(root, last), far)))

        def back(j, values):
            j = number - 1 - j
            values = [times(r, plus(v, mode(s, j))) for s, r, v in zip(tiles_here, own, values)]
            for s, value in zip(tiles_here, values):
                keep(s, j, value)
            return values

        lax.fori_loop(0, number, back, values, unroll=2)

        @pl.loop(0, wide)
        def _(n):
            s = k * per + i * wide + n
            for c in range(2):
                result = dot_three(halves(modes[s, c].reshape(number * tile, length_z)), table)
                spot = pl.ds(pl.multiple_of(s * tile, tile), tile)
                for h in range(parts):
                    block = result[:, h * lanes : (h + 1) * lanes]
                    slots[slot_of(h, mine), c, :, spot] = block.reshape(number, tile, lanes)
            send_out(s).start()

    @pl.loop(0, 2 * bands)
    def _(i):
        send_in(i).wait_recv()

    group = 8
    squares_ref[...] = jnp.zeros_like(squares_ref)

    def prepare(y):
        load_speed(y).wait()

        def step(i, square):
            some = pl.ds(i * group, group)
            v = speed[y, some]
            speed[y, some] = wave_square - wave_square / (v * v)
            s_re, s_im = source[y, some], source[bands + y, some]
            return square + jnp.sum(s_re * s_re + s_im * s_im, axis=0)

        squares_ref[...] += lax.fori_loop(
            0, length // group, step, jnp.zeros((rows, lanes), jnp.float32), unroll=2
        )

    lag = 2

    @pl.loop(0, groups)
    def _(k):
        @pl.loop(0, per)
        def _(i):
            forward(k, i)

        @pl.when(k >= lag)
        def _():
            merge(k - lag)

    early = 3
    stages = [(2.9, merge, k) for k in range(max(groups - lag, 0), groups)]
    stages += [(5.2, relay, k) for k in range(groups)]
    stages += [(8.7, expand, k) for k in range(min(early, groups))]
    stages += [(5.1, prepare, k) for k in range(bands)]
    for _, stage, k in sorted(stages, key=lambda item: 1.8 * item[2] + item[0]):
        stage(k)

    @pl.loop(0, groups)
    def _(k):
        send_edges(k).wait_recv()

        @pl.loop(0, per // wide)
        def _(i):
            backward(k, i)

        @pl.when(k + early < groups)
        def _():
            expand(k + early)

    @pl.loop(0, groups)
    def _(k):
        send_edges(k).wait_send()
        send_inward(k).wait_send()
        for i in range(per):
            send_ends(k, i).wait_send()

        @pl.when(depth > 0)
        def _():
            send_outward(k).wait_send()

    @pl.loop(0, 2 * bands)
    def _(i):
        send_in(i).wait_send()

    @pl.loop(0, steps)
    def _(i):
        send_out(i).wait_recv()

    def transform(y, j):
        flat = image.at[y].reshape(2 * length * rows, lanes)
        for c in range(2):
            pieces = [
                jnp.concatenate([slots[h, c, y * rows + j + k] for h in range(parts)], axis=0)
                for k in range(2)
            ]
            result = dot_three(x_table, halves(jnp.concatenate(pieces, axis=1)))
            for k in range(2):
                flat[pl.ds(c * length * rows + j + k, length, stride=rows), :] = result[
                    :, k * lanes : (k + 1) * lanes
                ]

    def tally(y, i, sums):
        some = pl.ds(i * group, group)
        shift = speed[y, some]
        s_re, s_im = source[y, some], source[bands + y, some]
        w_re, w_im = image[y, 0, some], image[y, 1, some]
        u_re = s_re + shift * w_re + damped * w_im
        u_im = s_im + shift * w_im - damped * w_re
        terms = (
            s_re * u_re + s_im * u_im,
            s_re * u_im - s_im * u_re,
            u_re * u_re + u_im * u_im,
        )
        return tuple(a + jnp.sum(b, axis=0) for a, b in zip(sums, terms))

    pairs, runs = rows // 2, length // group

    def both(y, sums):
        for n in range(pairs):
            for i in range(n * runs // pairs, (n + 1) * runs // pairs):
                sums = tally(y - 1, i, sums)
            transform(y, 2 * n)
        return sums

    for n in range(pairs):
        transform(0, 2 * n)
    sums = lax.fori_loop(1, bands, both, (jnp.zeros((rows, lanes), jnp.float32),) * 3)
    sums = lax.fori_loop(0, runs, functools.partial(tally, bands - 1), sums, unroll=2)
    sums = [jnp.sum(a, axis=0, keepdims=True) for a in (squares_ref[...],) + sums]
    lane = lax.broadcasted_iota(jnp.int32, (1, lanes), 1)
    packed = jnp.zeros((1, lanes), jnp.float32)
    for k, row in enumerate(sums):
        for shift in (lanes // 2, lanes // 4):
            row = row + pltpu.roll(row, shift, 1)
        packed = jnp.where(lax.div(lane, lanes // 4) == k, row, packed)
    own = len(everyone)
    heard[own : own + 1] = packed
    copies = [
        remote(heard.at[own : own + 1], heard.at[k : k + 1], sum_send, sum_recv, k, peer)
        for k, peer in enumerate(everyone)
    ]
    for copy in copies:
        copy.start()
    for copy in copies:
        copy.wait()
    total_ref[...] = jnp.broadcast_to(jnp.sum(heard[...], axis=0, keepdims=True), total_ref.shape)

    @pl.loop(0, steps)
    def _(i):
        send_out(i).wait_send()


def scale(total_ref, w_ref, out_ref, scaled, sems):
    bands, _, length, _, _ = w_ref.shape
    pieces = sems.shape[0]
    depth = length // pieces
    row = total_ref[0:1]
    lane = lax.div(lax.broadcasted_iota(jnp.int32, row.shape, 1), lanes // 4)
    sums = [jnp.sum(jnp.where(lane == k, row, 0.0), axis=1, keepdims=True) for k in range(4)]
    size = sums[0] + epsilon
    one_re, one_im, squares = sums[1] / size, sums[2] / size, sums[3] / size
    one = one_re * one_re + one_im * one_im
    denominator = squares - one * (epsilon / size) + epsilon
    re = jnp.broadcast_to(one_re / denominator, (rows, lanes))
    im = jnp.broadcast_to(-one_im / denominator, (rows, lanes))

    def save(i):
        part = pl.ds(i * depth, depth)
        return pltpu.make_async_copy(scaled.at[:, part], out_ref.at[:, part], sems.at[i])

    @pl.loop(0, pieces)
    def _(i):
        @pl.loop(0, depth, unroll=4)
        def _(j):
            x = i * depth + j
            for y in range(bands):
                w_re, w_im = w_ref[y, 0, x], w_ref[y, 1, x]
                scaled[0, x, y * rows : (y + 1) * rows] = re * w_re - im * w_im
                scaled[1, x, y * rows : (y + 1) * rows] = re * w_im + im * w_re

        save(i).start()

    @pl.loop(0, pieces)
    def _(i):
        save(i).wait()


def on_device(blocks, parts, source, speed):
    _, length_x, number, width = source.shape
    length_z = width * parts
    part = length_x // parts
    tile = 2 * rows
    bands, tiles = number // rows, part // tile
    span = rows * blocks // 2
    groups, peers = part // span, blocks * parts - 1
    f32 = jnp.float32
    shape, dma = jax.ShapeDtypeStruct, pltpu.SemaphoreType.DMA

    def vmem(*size):
        return pltpu.VMEM(size, f32)

    anywhere, inside = pl.BlockSpec(memory_space=pl.ANY), pl.BlockSpec(memory_space=pltpu.VMEM)
    image, sums = pl.pallas_call(
        functools.partial(solve_all, blocks, parts),
        in_specs=[anywhere] * 7,
        out_specs=[inside, inside],
        out_shape=[vmem(bands, 2, length_x, rows, width), vmem(rows, width)],
        scratch_shapes=[
            vmem(2 * bands, length_x, rows, width),
            vmem(bands, length_x, rows, width),
            vmem(2, part, length_z),
            vmem(10, part, lanes),
            vmem(tiles, 3, 2, number, tile, width),
            vmem(tiles, 2, number, tile, length_z),
            vmem(groups, 3, 4, span, lanes),
            vmem(groups, 4, span, lanes),
            vmem(groups, 2, 2, span, lanes),
            vmem(groups, 2, 2, span, lanes),
            vmem(groups, 2, 4, span, lanes),
            vmem(groups, 2, 4, span, lanes),
            vmem(3, 2, number, part, width),
            pltpu.VMEM((2, length_x, length_x), jnp.bfloat16),
            pltpu.VMEM((2, length_z, length_z), jnp.bfloat16),
            vmem(rows, width),
            vmem(peers + 1, width),
            dma((2 * bands,)),
            dma((bands,)),
            dma((5,)),
            dma((2 * bands,)),
            dma((2 * bands,)),
        ]
        + [dma((tiles,))] * 2
        + [dma((2 * groups,))] * 2
        + [dma((groups,))] * 2
        + [dma((tiles,))] * 2
        + [dma((peers,))] * 2,
        compiler_params=pltpu.CompilerParams(
            vmem_limit_bytes=55 * 1024 * 1024, collective_id=0, has_side_effects=True
        ),
        name="solve_all",
    )(source, speed, root_table(length_x, length_z), *sine_table(length_x), *sine_table(length_z))
    pieces = 16
    return pl.pallas_call(
        scale,
        in_specs=[inside, inside],
        out_specs=anywhere,
        out_shape=shape(source.shape, f32),
        scratch_shapes=[vmem(*source.shape), dma((pieces,))],
        compiler_params=pltpu.CompilerParams(vmem_limit_bytes=20 * 1024 * 1024),
        name="scale",
    )(sums, image)


def solution(mesh):
    return jax.shard_map(
        functools.partial(on_device, mesh.shape["px"], mesh.shape["py"]),
        mesh=mesh,
        in_specs=(P(None, "samples", "px", "py"), P("samples", "px", "py")),
        out_specs=P(None, "samples", "px", "py"),
        check_vma=False,
    )
```

```python
import functools

import jax
import jax.numpy as jnp
import numpy as np
from jax import lax
from jax.experimental import pallas as pl
from jax.experimental.pallas import tpu as pltpu
from jax.sharding import PartitionSpec as P

wave_square = 0.25
damped = 0.125
epsilon = 1e-06
rows = 8
lanes = 128
MESH = pl.DeviceIdType.MESH


def sine_table(length):
    index = np.arange(length, dtype=np.int64) + 1
    turns = (index[:, None] * index[None, :]) % (2 * (length + 1))
    table = np.sqrt(2.0 / (length + 1.0)) * np.sin(np.pi * turns / (length + 1.0))
    high = table.astype(np.float32).astype(jnp.bfloat16)
    low = (table - high.astype(np.float64)).astype(np.float32).astype(jnp.bfloat16)
    return jnp.asarray(high), jnp.asarray(low)


def eigen_line(length):
    sine_half = np.sin(np.pi * (np.arange(length) + 1.0) / (2.0 * (length + 1.0)))
    return 4.0 * sine_half * sine_half


def root_table(length_x, length_z):
    half = eigen_line(length_x)[:, None] + eigen_line(length_z)[None, :]
    half = (half + 2.0 - wave_square + 1j * damped) / 2.0
    root = 1.0 / (half + np.sqrt(half * half - 1.0))
    return jnp.asarray(np.stack([root.real, root.imag]).astype(np.float32))


def halves(values):
    high = values.astype(jnp.bfloat16)
    low = (values - high.astype(jnp.float32)).astype(jnp.bfloat16)
    return high, low


def dot_three(left, right):
    dot = functools.partial(jnp.dot, preferred_element_type=jnp.float32)
    return dot(left[0], right[0]) + (dot(left[0], right[1]) + dot(left[1], right[0]))


def times(a, b):
    return a[0] * b[0] - a[1] * b[1], a[0] * b[1] + a[1] * b[0]


def plus(a, b):
    return a[0] + b[0], a[1] + b[1]


def inverse(a):
    scale = 1.0 / (a[0] * a[0] + a[1] * a[1])
    return a[0] * scale, -a[1] * scale


def minus(a, b):
    return a[0] - b[0], a[1] - b[1]


def power(a, number):
    result = None
    while number:
        if number & 1:
            result = a if result is None else times(result, a)
        number >>= 1
        if number:
            a = times(a, a)
    return result


def pair_of(ref, plane=0):
    return ref[plane], ref[plane + 1]


def greet(peers):
    barrier = pltpu.get_barrier_semaphore()
    for peer in peers:
        pl.semaphore_signal(barrier, inc=1, device_id=peer, device_id_type=MESH)
    pl.semaphore_wait(barrier, len(peers))


def remote(source, target, sends, receives, place, device):
    return pltpu.make_async_remote_copy(
        src_ref=source,
        dst_ref=target,
        send_sem=sends.at[place],
        recv_sem=receives.at[place],
        device_id=device,
        device_id_type=MESH,
    )


def solve_all(
    blocks,
    parts,
    source_ref,
    speed_ref,
    roots_ref,
    x_high_ref,
    x_low_ref,
    z_high_ref,
    z_low_ref,
    image,
    total_ref,
    source,
    speed,
    roots,
    rates,
    tiles,
    even_modes,
    odd_modes,
    even_work,
    odd_work,
    ends,
    pair,
    waves_out,
    waves,
    inner,
    edges,
    slots,
    x_halves,
    z_halves,
    squares_ref,
    heard,
    source_sem,
    speed_sem,
    table_sem,
    in_send,
    in_recv,
    ends_send,
    ends_recv,
    wave_send,
    wave_recv,
    edge_send,
    edge_recv,
    out_send,
    out_recv,
    sum_send,
    sum_recv,
):
    steps, _, _, number, tile, _ = tiles.shape
    _, length, _, _ = source.shape
    bands = number // rows
    part = length // parts
    length_z = even_modes.shape[-1]
    groups, _, _, span, _ = ends.shape
    per, places = span // tile, blocks // 2
    me = lax.axis_index("px")
    side, place = lax.rem(me, 2), lax.div(me, 2)
    other = me + 1 - 2 * side
    mine = lax.axis_index("py")
    beside = {"py": 1 - mine}
    depths = places // 2
    behind = lax.div(place, depths)
    depth = place + behind * (places - 1 - 2 * place)
    inmost = lax.div(depth + 1, depths)
    toward = 1 - 2 * behind
    everyone = []
    for k in range(1, blocks * parts):
        peer = lax.rem(me * parts + mine + k, blocks * parts)
        everyone.append({"px": lax.div(peer, parts), "py": lax.rem(peer, parts)})

    def band(y):
        return pl.ds(pl.multiple_of(y * rows, rows), rows)

    def load_source(i):
        return pltpu.make_async_copy(
            source_ref.at[lax.div(i, bands), :, band(lax.rem(i, bands))], source.at[i], source_sem.at[i]
        )

    def load_speed(y):
        return pltpu.make_async_copy(speed_ref.at[:, band(y)], speed.at[y], speed_sem.at[y])

    root_rows = pl.ds(pl.multiple_of(mine * part, 8), part)
    tables = [
        (x_high_ref, x_halves.at[0]),
        (x_low_ref, x_halves.at[1]),
        (z_high_ref, z_halves.at[0]),
        (z_low_ref, z_halves.at[1]),
        (roots_ref.at[:, root_rows], roots),
    ]
    tables = [pltpu.make_async_copy(a, b, table_sem.at[k]) for k, (a, b) in enumerate(tables)]
    load_source(0).start()
    for copy in tables:
        copy.start()

    @pl.loop(1, 2 * bands)
    def _(i):
        load_source(i).start()

    @pl.loop(0, bands)
    def _(y):
        load_speed(y).start()

    greet(everyone)
    for copy in tables[:2]:
        copy.wait()
    x_table = (x_halves[0], x_halves[1])

    def slot_of(h, own):
        return own + lax.rem(h + own, 2) * (2 - own)

    def send_in(i):
        c, y = lax.div(i, bands), lax.rem(i, bands)
        return remote(
            tiles.at[:, 2, c, band(y)], tiles.at[:, mine, c, band(y)], in_send, in_recv, i, beside
        )

    @pl.loop(0, 2 * bands)
    def _(i):
        load_source(i).wait()
        c, y = lax.div(i, bands), lax.rem(i, bands)
        flat = source.at[i].reshape(length * rows, lanes)
        for j in range(0, rows, 2):
            pieces = [flat[pl.ds(j + k, length, stride=rows), :] for k in range(2)]
            result = dot_three(x_table, halves(jnp.concatenate(pieces, axis=1)))
            for k in range(2):
                for h in range(parts):
                    block = result[h * part : (h + 1) * part, k * lanes : (k + 1) * lanes]
                    tiles[:, slot_of(h, mine), c, y * rows + j + k] = block.reshape(steps, tile, lanes)
        send_in(i).start()

    for copy in tables[2:]:
        copy.wait()
    table = (z_halves[0], z_halves[1])
    zero = jnp.zeros((tile, length_z), jnp.float32)
    own_lanes = pl.ds(pl.multiple_of(side * lanes, lanes), lanes)
    root = (roots[0, :, own_lanes], roots[1, :, own_lanes])
    jump = power(root, number)
    rate = times(jump, jump)
    double = times(rate, rate)
    echo = (-root[0], -root[1])
    for n in range(1, depths):
        deeper = times(echo, double)
        echo = tuple(jnp.where(depth >= n, a, b) for a, b in zip(deeper, echo))
    whole = power(root, blocks * number + 1)
    square = times(whole, whole)
    spread = inverse((1.0 - square[0], -square[1]))
    for n, values in enumerate((jump, rate, echo, whole, spread)):
        rates[2 * n] = values[0]
        rates[2 * n + 1] = values[1]

    def send_ends(k, i):
        spot = pl.ds(pl.multiple_of(i * tile, tile), tile)
        return remote(
            ends.at[k, 2, :, spot],
            ends.at[k, side, :, spot],
            ends_send,
            ends_recv,
            k * per + i,
            {"px": other},
        )

    def wave(k, way, slot, place):
        return pltpu.make_async_remote_copy(
            src_ref=waves_out.at[k, way],
            dst_ref=waves.at[k, slot],
            send_sem=wave_send.at[2 * k + way],
            recv_sem=wave_recv.at[2 * k + slot],
            device_id={"px": 2 * place + side},
            device_id_type=MESH,
        )

    def send_inward(k):
        return wave(k, 0, inmost, place + toward)

    def send_outward(k):
        return wave(k, 1, 1, place - toward)

    def send_edges(k):
        return remote(inner.at[k, 1 - side], edges.at[k, side], edge_send, edge_recv, k, {"px": other})

    def group_rates(k, *which):
        part = pl.ds(k * span, span) if isinstance(k, int) else pl.ds(pl.multiple_of(k * span, span), span)
        return [(rates[2 * n, part], rates[2 * n + 1, part]) for n in which]

    def tile_root(i):
        part = pl.ds(pl.multiple_of(i * tile, tile), tile)
        return roots[0, part], roots[1, part]

    modes, work = (even_modes, odd_modes), (even_work, odd_work)

    def transform_z(p, odd):
        for c in range(2):
            pieces = [tiles[2 * p + odd, h, c].reshape(number * tile, lanes) for h in range(parts)]
            result = dot_three(halves(jnp.concatenate(pieces, axis=1)), table)
            modes[odd][p, c] = result.reshape(number, tile, length_z)

    def sweep(p, odd):
        s = 2 * p + odd
        k, i = lax.div(s, per), lax.rem(s, per)
        root = tile_root(s)
        first, last = (zero, zero), (zero, zero)
        for j in range(number):
            back = number - 1 - j
            last = plus(times(root, last), (modes[odd][p, 0, j], modes[odd][p, 1, j]))
            first = plus(times(root, first), (modes[odd][p, 0, back], modes[odd][p, 1, back]))
        part = pl.ds(pl.multiple_of(i * tile, tile), tile)
        for h in range(2):
            slot = slot_of(h, side)
            for plane, value in enumerate(first + last):
                ends[k, slot, plane, part] = value[:, h * lanes : (h + 1) * lanes]
        return send_ends(k, i)

    def either(a, b):
        return tuple(jnp.where(behind == 0, x, y) for x, y in zip(a, b))

    def pass_inward(k, rate, echo, came):
        bounced = times(echo, pair_of(pair.at[k], 2))
        value = plus(pair_of(pair.at[k]), times(rate, plus(came, bounced)))
        for c in range(2):
            waves_out[k, 0, c] = value[c]
        send_inward(k).start()

    def merge(k):
        for i in range(per):
            send_ends(k, i).wait_recv()
        jump, rate, echo = group_rates(k, 0, 1, 2)
        first = plus(pair_of(ends.at[k, 0]), times(jump, pair_of(ends.at[k, 1])))
        last = plus(pair_of(ends.at[k, 1], 2), times(jump, pair_of(ends.at[k, 0], 2)))
        for plane, value in enumerate(either(last, first) + either(first, last)):
            pair[k, plane] = value

        @pl.when(depth == 0)
        def _():
            none = jnp.zeros((span, lanes), jnp.float32)
            for c in range(2):
                waves[k, 0, c] = none
            pass_inward(k, rate, echo, (none, none))

    def relay(k):
        @pl.when(depth > 0)
        def _():
            wave(k, 0, 0, place - toward).wait_recv()
            rate, echo = group_rates(k, 1, 2)
            pass_inward(k, rate, echo, pair_of(waves.at[k, 0]))

    def expand(k):
        wave(k, 1, 1, place + toward).wait_recv()
        jump, rate, echo, whole, spread = group_rates(k, 0, 1, 2, 3, 4)
        came = pair_of(waves.at[k, 1])
        met = times(spread, minus(came, times(whole, pair_of(waves_out.at[k, 0]))))
        came = tuple(jnp.where(inmost == 1, a, b) for a, b in zip(met, came))
        out = plus(pair_of(pair.at[k], 2), times(rate, came))
        back = plus(pair_of(waves.at[k, 0]), times(echo, out))

        @pl.when(depth > 0)
        def _():
            for c in range(2):
                waves_out[k, 1, c] = out[c]
            send_outward(k).start()

        before, after = either(back, came), either(came, back)
        left = before + plus(pair_of(ends.at[k, 1]), times(jump, after))
        right = plus(pair_of(ends.at[k, 0], 2), times(jump, before)) + after
        for q, values in enumerate((left, right)):
            for plane, value in enumerate(values):
                inner[k, q, plane] = value
        send_edges(k).start()
        edges[k, side] = inner[k, side]

    def send_out(i):
        spot = pl.ds(pl.multiple_of(i * tile, tile), tile)
        return remote(slots.at[2, :, :, spot], slots.at[mine, :, :, spot], out_send, out_recv, i, beside)

    def solve_y(p, odd):
        s = 2 * p + odd
        k, i = lax.div(s, per), lax.rem(s, per)
        root = tile_root(s)
        part = pl.ds(pl.multiple_of(i * tile, tile), tile)
        carried = [
            jnp.concatenate([edges[k, h, plane, part] for h in range(2)], axis=1) for plane in range(4)
        ]
        state, after = tuple(carried[:2]), tuple(carried[2:])
        for j in range(number):
            state = plus(times(root, state), (modes[odd][p, 0, j], modes[odd][p, 1, j]))
            work[odd][0, j] = state[0]
            work[odd][1, j] = state[1]
        square = times(root, root)
        scaled = times(root, inverse((1.0 - square[0], -square[1])))
        value = times(scaled, plus(times(root, state), after))
        for j in range(number - 1, -1, -1):
            value = times(root, plus(value, (work[odd][0, j], work[odd][1, j])))
            work[odd][0, j] = value[0]
            work[odd][1, j] = value[1]

    def emit(p, odd):
        s = 2 * p + odd
        spot = pl.ds(pl.multiple_of(s * tile, tile), tile)
        for c in range(2):
            result = dot_three(halves(work[odd][c].reshape(number * tile, length_z)), table)
            for h in range(parts):
                block = result[:, h * lanes : (h + 1) * lanes]
                slots[slot_of(h, mine), c, :, spot] = block.reshape(number, tile, lanes)
        return send_out(s)

    @pl.loop(0, 2 * bands)
    def _(i):
        send_in(i).wait_recv()

    group = 8
    squares_ref[...] = jnp.zeros_like(squares_ref)

    def prepare(y):
        load_speed(y).wait()

        def step(i, square):
            some = pl.ds(i * group, group)
            v = speed[y, some]
            speed[y, some] = wave_square - wave_square / (v * v)
            s_re, s_im = source[y, some], source[bands + y, some]
            return square + jnp.sum(s_re * s_re + s_im * s_im, axis=0)

        squares_ref[...] += lax.fori_loop(
            0, length // group, step, jnp.zeros((rows, lanes), jnp.float32), unroll=2
        )

    lag = 2

    duos = steps // 2
    duos_of = per // 2

    def ready(p):
        @pl.when(jnp.logical_and(lax.rem(p + 1, duos_of) == 0, lax.div(p, duos_of) >= lag))
        def _():
            merge(lax.div(p, duos_of) - lag)

    transform_z(0, 0)

    @pl.loop(0, duos - 1)
    def _(p):
        copy = sweep(p, 0)
        transform_z(p, 1)
        copy.start()
        copy = sweep(p, 1)
        transform_z(p + 1, 0)
        copy.start()
        ready(p)

    copy = sweep(duos - 1, 0)
    transform_z(duos - 1, 1)
    copy.start()
    sweep(duos - 1, 1).start()
    if groups > lag:
        merge(groups - 1 - lag)
    early = 3
    stages = [(2.9, merge, k) for k in range(max(groups - lag, 0), groups)]
    stages += [(5.2, relay, k) for k in range(groups)]
    stages += [(8.7, expand, k) for k in range(min(early, groups))]
    stages += [(5.1, prepare, k) for k in range(bands)]
    for _, stage, k in sorted(stages, key=lambda item: 1.8 * item[2] + item[0]):
        stage(k)

    send_edges(0).wait_recv()
    solve_y(0, 0)
    solve_y(0, 1)
    emit(0, 0).start()

    @pl.loop(1, duos)
    def _(p):
        k = lax.div(p, duos_of)

        @pl.when(lax.rem(p, duos_of) == 0)
        def _():
            @pl.when(k - 1 + early < groups)
            def _():
                expand(k - 1 + early)

            send_edges(k).wait_recv()

        copy = emit(p - 1, 1)
        solve_y(p, 0)
        copy.start()
        copy = emit(p, 0)
        solve_y(p, 1)
        copy.start()

    emit(duos - 1, 1).start()

    @pl.loop(0, steps)
    def _(i):
        send_out(i).wait_recv()

    def transform(y, j):
        flat = image.at[y].reshape(2 * length * rows, lanes)
        for c in range(2):
            pieces = [
                jnp.concatenate([slots[h, c, y * rows + j + k] for h in range(parts)], axis=0)
                for k in range(2)
            ]
            result = dot_three(x_table, halves(jnp.concatenate(pieces, axis=1)))
            for k in range(2):
                flat[pl.ds(c * length * rows + j + k, length, stride=rows), :] = result[
                    :, k * lanes : (k + 1) * lanes
                ]

    def tally(y, i, sums):
        some = pl.ds(i * group, group)
        shift = speed[y, some]
        s_re, s_im = source[y, some], source[bands + y, some]
        w_re, w_im = image[y, 0, some], image[y, 1, some]
        u_re = s_re + shift * w_re + damped * w_im
        u_im = s_im + shift * w_im - damped * w_re
        terms = (
            s_re * u_re + s_im * u_im,
            s_re * u_im - s_im * u_re,
            u_re * u_re + u_im * u_im,
        )
        return tuple(a + jnp.sum(b, axis=0) for a, b in zip(sums, terms))

    pairs, runs = rows // 2, length // group

    def both(y, sums):
        for n in range(pairs):
            for i in range(n * runs // pairs, (n + 1) * runs // pairs):
                sums = tally(y - 1, i, sums)
            transform(y, 2 * n)
        return sums

    for n in range(pairs):
        transform(0, 2 * n)
    sums = lax.fori_loop(1, bands, both, (jnp.zeros((rows, lanes), jnp.float32),) * 3)
    sums = lax.fori_loop(0, runs, functools.partial(tally, bands - 1), sums, unroll=2)
    sums = [jnp.sum(a, axis=0, keepdims=True) for a in (squares_ref[...],) + sums]
    lane = lax.broadcasted_iota(jnp.int32, (1, lanes), 1)
    packed = jnp.zeros((1, lanes), jnp.float32)
    for k, row in enumerate(sums):
        for shift in (lanes // 2, lanes // 4):
            row = row + pltpu.roll(row, shift, 1)
        packed = jnp.where(lax.div(lane, lanes // 4) == k, row, packed)
    own = len(everyone)
    heard[own : own + 1] = packed
    copies = [
        remote(heard.at[own : own + 1], heard.at[k : k + 1], sum_send, sum_recv, k, peer)
        for k, peer in enumerate(everyone)
    ]
    for copy in copies:
        copy.start()

    @pl.loop(0, groups)
    def _(k):
        send_edges(k).wait_send()
        send_inward(k).wait_send()
        for i in range(per):
            send_ends(k, i).wait_send()

        @pl.when(depth > 0)
        def _():
            send_outward(k).wait_send()

    @pl.loop(0, 2 * bands)
    def _(i):
        send_in(i).wait_send()

    @pl.loop(0, steps)
    def _(i):
        send_out(i).wait_send()

    for copy in copies:
        copy.wait()
    total_ref[...] = jnp.broadcast_to(jnp.sum(heard[...], axis=0, keepdims=True), total_ref.shape)


def scale(total_ref, w_ref, out_ref, scaled, sems):
    bands, _, length, _, _ = w_ref.shape
    pieces = sems.shape[0]
    depth = length // pieces
    row = total_ref[0:1]
    lane = lax.div(lax.broadcasted_iota(jnp.int32, row.shape, 1), lanes // 4)
    sums = [jnp.sum(jnp.where(lane == k, row, 0.0), axis=1, keepdims=True) for k in range(4)]
    size = sums[0] + epsilon
    one_re, one_im, squares = sums[1] / size, sums[2] / size, sums[3] / size
    one = one_re * one_re + one_im * one_im
    denominator = squares - one * (epsilon / size) + epsilon
    re = jnp.broadcast_to(one_re / denominator, (rows, lanes))
    im = jnp.broadcast_to(-one_im / denominator, (rows, lanes))

    def save(i):
        part = pl.ds(i * depth, depth)
        return pltpu.make_async_copy(scaled.at[:, part], out_ref.at[:, part], sems.at[i])

    @pl.loop(0, pieces)
    def _(i):
        @pl.loop(0, depth, unroll=4)
        def _(j):
            x = i * depth + j
            for y in range(bands):
                w_re, w_im = w_ref[y, 0, x], w_ref[y, 1, x]
                scaled[0, x, y * rows : (y + 1) * rows] = re * w_re - im * w_im
                scaled[1, x, y * rows : (y + 1) * rows] = re * w_im + im * w_re

        save(i).start()

    @pl.loop(0, pieces)
    def _(i):
        save(i).wait()


def on_device(blocks, parts, source, speed):
    _, length_x, number, width = source.shape
    length_z = width * parts
    part = length_x // parts
    tile = 2 * rows
    bands, tiles = number // rows, part // tile
    span = rows * blocks // 2
    groups, peers = part // span, blocks * parts - 1
    f32 = jnp.float32
    shape, dma = jax.ShapeDtypeStruct, pltpu.SemaphoreType.DMA

    def vmem(*size):
        return pltpu.VMEM(size, f32)

    anywhere, inside = pl.BlockSpec(memory_space=pl.ANY), pl.BlockSpec(memory_space=pltpu.VMEM)
    image, sums = pl.pallas_call(
        functools.partial(solve_all, blocks, parts),
        in_specs=[anywhere] * 7,
        out_specs=[inside, inside],
        out_shape=[vmem(bands, 2, length_x, rows, width), vmem(rows, width)],
        scratch_shapes=[
            vmem(2 * bands, length_x, rows, width),
            vmem(bands, length_x, rows, width),
            vmem(2, part, length_z),
            vmem(10, part, lanes),
            vmem(tiles, 3, 2, number, tile, width),
            vmem(tiles // 2, 2, number, tile, length_z),
            vmem(tiles // 2, 2, number, tile, length_z),
            vmem(2, number, tile, length_z),
            vmem(2, number, tile, length_z),
            vmem(groups, 3, 4, span, lanes),
            vmem(groups, 4, span, lanes),
            vmem(groups, 2, 2, span, lanes),
            vmem(groups, 2, 2, span, lanes),
            vmem(groups, 2, 4, span, lanes),
            vmem(groups, 2, 4, span, lanes),
            vmem(3, 2, number, part, width),
            pltpu.VMEM((2, length_x, length_x), jnp.bfloat16),
            pltpu.VMEM((2, length_z, length_z), jnp.bfloat16),
            vmem(rows, width),
            vmem(peers + 1, width),
            dma((2 * bands,)),
            dma((bands,)),
            dma((5,)),
            dma((2 * bands,)),
            dma((2 * bands,)),
        ]
        + [dma((tiles,))] * 2
        + [dma((2 * groups,))] * 2
        + [dma((groups,))] * 2
        + [dma((tiles,))] * 2
        + [dma((peers,))] * 2,
        compiler_params=pltpu.CompilerParams(
            vmem_limit_bytes=55 * 1024 * 1024, collective_id=0, has_side_effects=True
        ),
        name="solve_all",
    )(source, speed, root_table(length_x, length_z), *sine_table(length_x), *sine_table(length_z))
    pieces = 16
    return pl.pallas_call(
        scale,
        in_specs=[inside, inside],
        out_specs=anywhere,
        out_shape=shape(source.shape, f32),
        scratch_shapes=[vmem(*source.shape), dma((pieces,))],
        compiler_params=pltpu.CompilerParams(vmem_limit_bytes=20 * 1024 * 1024),
        name="scale",
    )(sums, image)


def solution(mesh):
    return jax.shard_map(
        functools.partial(on_device, mesh.shape["px"], mesh.shape["py"]),
        mesh=mesh,
        in_specs=(P(None, "samples", "px", "py"), P("samples", "px", "py")),
        out_specs=P(None, "samples", "px", "py"),
        check_vma=False,
    )
```

```python
import functools

import jax
import jax.numpy as jnp
import numpy as np
from jax import lax
from jax.experimental import pallas as pl
from jax.experimental.pallas import tpu as pltpu
from jax.sharding import PartitionSpec as P

wave_square = 0.25
damped = 0.125
epsilon = 1e-06
rows = 8
lanes = 128
MESH = pl.DeviceIdType.MESH


def sine_table(length):
    index = np.arange(length, dtype=np.int64) + 1
    turns = (index[:, None] * index[None, :]) % (2 * (length + 1))
    table = np.sqrt(2.0 / (length + 1.0)) * np.sin(np.pi * turns / (length + 1.0))
    high = table.astype(np.float32).astype(jnp.bfloat16)
    low = (table - high.astype(np.float64)).astype(np.float32).astype(jnp.bfloat16)
    return jnp.asarray(high), jnp.asarray(low)


def eigen_line(length):
    sine_half = np.sin(np.pi * (np.arange(length) + 1.0) / (2.0 * (length + 1.0)))
    return 4.0 * sine_half * sine_half


def root_table(length_x, length_z):
    half = eigen_line(length_x)[:, None] + eigen_line(length_z)[None, :]
    half = (half + 2.0 - wave_square + 1j * damped) / 2.0
    root = 1.0 / (half + np.sqrt(half * half - 1.0))
    return jnp.asarray(np.stack([root.real, root.imag]).astype(np.float32))


def halves(values):
    high = values.astype(jnp.bfloat16)
    low = (values - high.astype(jnp.float32)).astype(jnp.bfloat16)
    return high, low


def dot_three(left, right):
    dot = functools.partial(jnp.dot, preferred_element_type=jnp.float32)
    return dot(left[0], right[0]) + (dot(left[0], right[1]) + dot(left[1], right[0]))


def times(a, b):
    return a[0] * b[0] - a[1] * b[1], a[0] * b[1] + a[1] * b[0]


def plus(a, b):
    return a[0] + b[0], a[1] + b[1]


def inverse(a):
    scale = 1.0 / (a[0] * a[0] + a[1] * a[1])
    return a[0] * scale, -a[1] * scale


def minus(a, b):
    return a[0] - b[0], a[1] - b[1]


def power(a, number):
    result = None
    while number:
        if number & 1:
            result = a if result is None else times(result, a)
        number >>= 1
        if number:
            a = times(a, a)
    return result


def pair_of(ref, plane=0):
    return ref[plane], ref[plane + 1]


def greet(peers):
    barrier = pltpu.get_barrier_semaphore()
    for peer in peers:
        pl.semaphore_signal(barrier, inc=1, device_id=peer, device_id_type=MESH)
    pl.semaphore_wait(barrier, len(peers))


def remote(source, target, sends, receives, place, device):
    return pltpu.make_async_remote_copy(
        src_ref=source,
        dst_ref=target,
        send_sem=sends.at[place],
        recv_sem=receives.at[place],
        device_id=device,
        device_id_type=MESH,
    )


def solve_all(
    blocks,
    parts,
    source_ref,
    speed_ref,
    roots_ref,
    x_high_ref,
    x_low_ref,
    z_high_ref,
    z_low_ref,
    image,
    total_ref,
    source,
    speed,
    roots,
    rates,
    tiles,
    even_modes,
    odd_modes,
    even_work,
    odd_work,
    ends,
    pair,
    waves_out,
    waves,
    tops,
    outs,
    met,
    inner,
    edges,
    slots,
    x_halves,
    z_halves,
    squares_ref,
    heard,
    source_sem,
    speed_sem,
    table_sem,
    in_send,
    in_recv,
    ends_send,
    ends_recv,
    wave_send,
    wave_recv,
    top_send,
    top_recv,
    outs_send,
    outs_recv,
    edge_send,
    edge_recv,
    out_send,
    out_recv,
    sum_send,
    sum_recv,
):
    steps, _, _, number, tile, _ = tiles.shape
    _, length, _, _ = source.shape
    bands = number // rows
    part = length // parts
    length_z = even_modes.shape[-1]
    groups, _, _, span, _ = ends.shape
    per, places = span // tile, blocks // 2
    me = lax.axis_index("px")
    side, place = lax.rem(me, 2), lax.div(me, 2)
    other = me + 1 - 2 * side
    mine = lax.axis_index("py")
    beside = {"py": 1 - mine}
    depths = places // 2
    behind = lax.div(place, depths)
    depth = place + behind * (places - 1 - 2 * place)
    inmost = lax.div(depth + 1, depths)
    others = [lax.rem(place + k, places) for k in range(1, places)]
    toward = 1 - 2 * behind
    everyone = []
    for k in range(1, blocks * parts):
        peer = lax.rem(me * parts + mine + k, blocks * parts)
        everyone.append({"px": lax.div(peer, parts), "py": lax.rem(peer, parts)})

    def band(y):
        return pl.ds(pl.multiple_of(y * rows, rows), rows)

    def load_source(i):
        return pltpu.make_async_copy(
            source_ref.at[lax.div(i, bands), :, band(lax.rem(i, bands))], source.at[i], source_sem.at[i]
        )

    def load_speed(y):
        return pltpu.make_async_copy(speed_ref.at[:, band(y)], speed.at[y], speed_sem.at[y])

    root_rows = pl.ds(pl.multiple_of(mine * part, 8), part)
    tables = [
        (x_high_ref, x_halves.at[0]),
        (x_low_ref, x_halves.at[1]),
        (z_high_ref, z_halves.at[0]),
        (z_low_ref, z_halves.at[1]),
        (roots_ref.at[:, root_rows], roots),
    ]
    tables = [pltpu.make_async_copy(a, b, table_sem.at[k]) for k, (a, b) in enumerate(tables)]
    load_source(0).start()
    for copy in tables:
        copy.start()

    @pl.loop(1, 2 * bands)
    def _(i):
        load_source(i).start()

    @pl.loop(0, bands)
    def _(y):
        load_speed(y).start()

    greet(everyone)
    for copy in tables[:2]:
        copy.wait()
    x_table = (x_halves[0], x_halves[1])

    def slot_of(h, own):
        return own + lax.rem(h + own, 2) * (2 - own)

    def send_in(i):
        c, y = lax.div(i, bands), lax.rem(i, bands)
        return remote(
            tiles.at[:, 2, c, band(y)], tiles.at[:, mine, c, band(y)], in_send, in_recv, i, beside
        )

    @pl.loop(0, 2 * bands)
    def _(i):
        load_source(i).wait()
        c, y = lax.div(i, bands), lax.rem(i, bands)
        flat = source.at[i].reshape(length * rows, lanes)
        for j in range(0, rows, 2):
            pieces = [flat[pl.ds(j + k, length, stride=rows), :] for k in range(2)]
            result = dot_three(x_table, halves(jnp.concatenate(pieces, axis=1)))
            for k in range(2):
                for h in range(parts):
                    block = result[h * part : (h + 1) * part, k * lanes : (k + 1) * lanes]
                    tiles[:, slot_of(h, mine), c, y * rows + j + k] = block.reshape(steps, tile, lanes)
        send_in(i).start()

    for copy in tables[2:]:
        copy.wait()
    table = (z_halves[0], z_halves[1])
    zero = jnp.zeros((tile, length_z), jnp.float32)
    own_lanes = pl.ds(pl.multiple_of(side * lanes, lanes), lanes)
    root = (roots[0, :, own_lanes], roots[1, :, own_lanes])
    jump = power(root, number)
    rate = times(jump, jump)
    double = times(rate, rate)
    echo = (-root[0], -root[1])
    for n in range(1, depths):
        deeper = times(echo, double)
        echo = tuple(jnp.where(depth >= n, a, b) for a, b in zip(deeper, echo))
    whole = power(root, blocks * number + 1)
    square = times(whole, whole)
    spread = inverse((1.0 - square[0], -square[1]))
    for n, values in enumerate((jump, rate, echo, whole, spread)):
        rates[2 * n] = values[0]
        rates[2 * n + 1] = values[1]

    def send_ends(k, i):
        spot = pl.ds(pl.multiple_of(i * tile, tile), tile)
        return remote(
            ends.at[k, 2, :, spot],
            ends.at[k, side, :, spot],
            ends_send,
            ends_recv,
            k * per + i,
            {"px": other},
        )

    def wave(k, place):
        return remote(
            waves_out.at[k, 0], waves.at[k], wave_send, wave_recv, k, {"px": 2 * place + side}
        )

    def send_top(k, i, from_side):
        return pltpu.make_async_remote_copy(
            src_ref=tops.at[k, from_side],
            dst_ref=tops.at[k, from_side],
            send_sem=top_send.at[k, i],
            recv_sem=top_recv.at[k, from_side],
            device_id={"px": 2 * others[i] + side},
            device_id_type=MESH,
        )

    def send_outs(k, to_depth, from_depth):
        return pltpu.make_async_remote_copy(
            src_ref=waves_out.at[k, 1],
            dst_ref=outs.at[k, from_depth],
            send_sem=outs_send.at[k, to_depth],
            recv_sem=outs_recv.at[k, from_depth],
            device_id={"px": 2 * (to_depth + behind * (places - 1 - 2 * to_depth)) + side},
            device_id_type=MESH,
        )

    def send_edges(k, i):
        spot = pl.ds(pl.multiple_of(i * tile, tile), tile)
        return remote(
            inner.at[k, 1 - side, :, spot],
            edges.at[k, side, :, spot],
            edge_send,
            edge_recv,
            k * per + i,
            {"px": other},
        )

    def group_rates(k, *which):
        part = pl.ds(k * span, span) if isinstance(k, int) else pl.ds(pl.multiple_of(k * span, span), span)
        return [(rates[2 * n, part], rates[2 * n + 1, part]) for n in which]

    def tile_root(i):
        part = pl.ds(pl.multiple_of(i * tile, tile), tile)
        return roots[0, part], roots[1, part]

    modes, work = (even_modes, odd_modes), (even_work, odd_work)

    def transform_z(p, odd):
        for c in range(2):
            pieces = [tiles[2 * p + odd, h, c].reshape(number * tile, lanes) for h in range(parts)]
            result = dot_three(halves(jnp.concatenate(pieces, axis=1)), table)
            modes[odd][p, c] = result.reshape(number, tile, length_z)

    def sweep(p, odd):
        s = 2 * p + odd
        k, i = lax.div(s, per), lax.rem(s, per)
        root = tile_root(s)
        first, last = (zero, zero), (zero, zero)
        for j in range(number):
            back = number - 1 - j
            last = plus(times(root, last), (modes[odd][p, 0, j], modes[odd][p, 1, j]))
            first = plus(times(root, first), (modes[odd][p, 0, back], modes[odd][p, 1, back]))
        part = pl.ds(pl.multiple_of(i * tile, tile), tile)
        for h in range(2):
            slot = slot_of(h, side)
            for plane, value in enumerate(first + last):
                ends[k, slot, plane, part] = value[:, h * lanes : (h + 1) * lanes]
        return send_ends(k, i)

    def either(a, b):
        return tuple(jnp.where(behind == 0, x, y) for x, y in zip(a, b))

    def pass_inward(k, rate, echo, came):
        bounced = times(echo, pair_of(pair.at[k], 2))
        value = plus(pair_of(pair.at[k]), times(rate, plus(came, bounced)))

        @pl.when(inmost == 0)
        def _():
            for c in range(2):
                waves_out[k, 0, c] = value[c]
            wave(k, place + toward).start()

        @pl.when(inmost == 1)
        def _():
            for c in range(2):
                tops[k, behind, c] = value[c]
            for i in range(places - 1):
                send_top(k, i, behind).start()

    def merge(k):
        for i in range(per):
            send_ends(k, i).wait_recv()
        jump, rate, echo = group_rates(k, 0, 1, 2)
        first = plus(pair_of(ends.at[k, 0]), times(jump, pair_of(ends.at[k, 1])))
        last = plus(pair_of(ends.at[k, 1], 2), times(jump, pair_of(ends.at[k, 0], 2)))
        for plane, value in enumerate(either(last, first) + either(first, last)):
            pair[k, plane] = value

        @pl.when(depth > 0)
        def _():
            for c in range(2):
                waves_out[k, 1, c] = pair[k, 2 + c]

        for n in range(depths - 1):

            @pl.when(depth > n)
            def _():
                send_outs(k, n, depth).start()

        @pl.when(depth == 0)
        def _():
            none = jnp.zeros((span, lanes), jnp.float32)
            for c in range(2):
                waves[k, c] = none
            pass_inward(k, rate, echo, (none, none))

    def relay(k):
        @pl.when(depth > 0)
        def _():
            wave(k, place - toward).wait_recv()
            rate, echo = group_rates(k, 1, 2)
            pass_inward(k, rate, echo, pair_of(waves.at[k]))

    def expand(k):
        @pl.when(inmost == 0)
        def _():
            send_top(k, 0, behind).wait_recv()

        send_top(k, 0, 1 - behind).wait_recv()
        jump, rate, echo, whole, spread = group_rates(k, 0, 1, 2, 3, 4)
        ours, theirs = pair_of(tops.at[k, behind]), pair_of(tops.at[k, 1 - behind])
        value = times(spread, minus(theirs, times(whole, ours)))
        for c in range(2):
            met[k, c] = value[c]
        for n in range(depths - 1, 0, -1):

            @pl.when(depth < n)
            def _():
                send_outs(k, 0, n).wait_recv()
                value = plus(pair_of(outs.at[k, n]), times(rate, pair_of(met.at[k])))
                for c in range(2):
                    met[k, c] = value[c]

        came = pair_of(met.at[k])
        out = plus(pair_of(pair.at[k], 2), times(rate, came))
        back = plus(pair_of(waves.at[k]), times(echo, out))
        before, after = either(back, came), either(came, back)
        left = before + plus(pair_of(ends.at[k, 1]), times(jump, after))
        right = plus(pair_of(ends.at[k, 0], 2), times(jump, before)) + after
        for q, values in enumerate((left, right)):
            for plane, value in enumerate(values):
                inner[k, q, plane] = value
        for i in range(per):
            send_edges(k, i).start()
        edges[k, side] = inner[k, side]

    def send_out(i):
        spot = pl.ds(pl.multiple_of(i * tile, tile), tile)
        return remote(slots.at[2, :, :, spot], slots.at[mine, :, :, spot], out_send, out_recv, i, beside)

    def solve_y(p, odd):
        s = 2 * p + odd
        k, i = lax.div(s, per), lax.rem(s, per)
        root = tile_root(s)
        part = pl.ds(pl.multiple_of(i * tile, tile), tile)
        carried = [
            jnp.concatenate([edges[k, h, plane, part] for h in range(2)], axis=1) for plane in range(4)
        ]
        state, after = tuple(carried[:2]), tuple(carried[2:])
        for j in range(number):
            state = plus(times(root, state), (modes[odd][p, 0, j], modes[odd][p, 1, j]))
            work[odd][0, j] = state[0]
            work[odd][1, j] = state[1]
        square = times(root, root)
        scaled = times(root, inverse((1.0 - square[0], -square[1])))
        value = times(scaled, plus(times(root, state), after))
        for j in range(number - 1, -1, -1):
            value = times(root, plus(value, (work[odd][0, j], work[odd][1, j])))
            work[odd][0, j] = value[0]
            work[odd][1, j] = value[1]

    def emit(p, odd):
        s = 2 * p + odd
        spot = pl.ds(pl.multiple_of(s * tile, tile), tile)
        for c in range(2):
            result = dot_three(halves(work[odd][c].reshape(number * tile, length_z)), table)
            for h in range(parts):
                block = result[:, h * lanes : (h + 1) * lanes]
                slots[slot_of(h, mine), c, :, spot] = block.reshape(number, tile, lanes)
        return send_out(s)

    @pl.loop(0, 2 * bands)
    def _(i):
        send_in(i).wait_recv()

    group = 8
    squares_ref[...] = jnp.zeros_like(squares_ref)

    def prepare(y):
        load_speed(y).wait()

        def step(i, square):
            some = pl.ds(i * group, group)
            v = speed[y, some]
            speed[y, some] = wave_square - wave_square / (v * v)
            s_re, s_im = source[y, some], source[bands + y, some]
            return square + jnp.sum(s_re * s_re + s_im * s_im, axis=0)

        squares_ref[...] += lax.fori_loop(
            0, length // group, step, jnp.zeros((rows, lanes), jnp.float32), unroll=2
        )

    lag = 2

    duos = steps // 2
    duos_of = per // 2

    def ready(p):
        @pl.when(jnp.logical_and(lax.rem(p + 1, duos_of) == 0, lax.div(p, duos_of) >= lag))
        def _():
            merge(lax.div(p, duos_of) - lag)

    transform_z(0, 0)

    @pl.loop(0, duos - 1)
    def _(p):
        copy = sweep(p, 0)
        transform_z(p, 1)
        copy.start()
        copy = sweep(p, 1)
        transform_z(p + 1, 0)
        copy.start()
        ready(p)

    copy = sweep(duos - 1, 0)
    transform_z(duos - 1, 1)
    copy.start()
    sweep(duos - 1, 1).start()
    if groups > lag:
        merge(groups - 1 - lag)
    early = 3
    stages = [(2.7, merge, k) for k in range(max(groups - lag, 0), groups)]
    stages += [(5.7, relay, k) for k in range(groups)]
    stages += [(10.4, expand, k) for k in range(min(early, groups))]
    stages += [(4.2, prepare, k) for k in range(bands)]
    for _, stage, k in sorted(stages, key=lambda item: 1.55 * item[2] + item[0]):
        stage(k)

    def await_edges(p, odd):
        s = 2 * p + odd
        send_edges(lax.div(s, per), lax.rem(s, per)).wait_recv()

    await_edges(0, 0)
    solve_y(0, 0)
    await_edges(0, 1)
    copy = emit(0, 0)
    solve_y(0, 1)
    copy.start()

    @pl.loop(1, duos)
    def _(p):
        k = lax.div(p, duos_of)

        @pl.when(lax.rem(p, duos_of) == 0)
        def _():
            @pl.when(k - 1 + early < groups)
            def _():
                expand(k - 1 + early)

        await_edges(p, 0)
        copy = emit(p - 1, 1)
        solve_y(p, 0)
        copy.start()
        await_edges(p, 1)
        copy = emit(p, 0)
        solve_y(p, 1)
        copy.start()

    emit(duos - 1, 1).start()

    @pl.loop(0, steps)
    def _(i):
        send_out(i).wait_recv()

    def transform(y, j):
        flat = image.at[y].reshape(2 * length * rows, lanes)
        for c in range(2):
            pieces = [
                jnp.concatenate([slots[h, c, y * rows + j + k] for h in range(parts)], axis=0)
                for k in range(2)
            ]
            result = dot_three(x_table, halves(jnp.concatenate(pieces, axis=1)))
            for k in range(2):
                flat[pl.ds(c * length * rows + j + k, length, stride=rows), :] = result[
                    :, k * lanes : (k + 1) * lanes
                ]

    def tally(y, i, sums):
        some = pl.ds(i * group, group)
        shift = speed[y, some]
        s_re, s_im = source[y, some], source[bands + y, some]
        w_re, w_im = image[y, 0, some], image[y, 1, some]
        u_re = s_re + shift * w_re + damped * w_im
        u_im = s_im + shift * w_im - damped * w_re
        terms = (
            s_re * u_re + s_im * u_im,
            s_re * u_im - s_im * u_re,
            u_re * u_re + u_im * u_im,
        )
        return tuple(a + jnp.sum(b, axis=0) for a, b in zip(sums, terms))

    pairs, runs = rows // 2, length // group

    def both(y, sums):
        for n in range(pairs):
            for i in range(n * runs // pairs, (n + 1) * runs // pairs):
                sums = tally(y - 1, i, sums)
            transform(y, 2 * n)
        return sums

    for n in range(pairs):
        transform(0, 2 * n)
    sums = lax.fori_loop(1, bands, both, (jnp.zeros((rows, lanes), jnp.float32),) * 3)
    sums = lax.fori_loop(0, runs, functools.partial(tally, bands - 1), sums, unroll=2)
    sums = [jnp.sum(a, axis=0, keepdims=True) for a in (squares_ref[...],) + sums]
    lane = lax.broadcasted_iota(jnp.int32, (1, lanes), 1)
    packed = jnp.zeros((1, lanes), jnp.float32)
    for k, row in enumerate(sums):
        for shift in (lanes // 2, lanes // 4):
            row = row + pltpu.roll(row, shift, 1)
        packed = jnp.where(lax.div(lane, lanes // 4) == k, row, packed)
    own = len(everyone)
    heard[own : own + 1] = packed
    copies = [
        remote(heard.at[own : own + 1], heard.at[k : k + 1], sum_send, sum_recv, k, peer)
        for k, peer in enumerate(everyone)
    ]
    for copy in copies:
        copy.start()

    @pl.loop(0, groups)
    def _(k):
        for i in range(per):
            send_ends(k, i).wait_send()
            send_edges(k, i).wait_send()

        @pl.when(inmost == 0)
        def _():
            wave(k, place + toward).wait_send()

        @pl.when(inmost == 1)
        def _():
            for i in range(places - 1):
                send_top(k, i, behind).wait_send()

        for n in range(depths - 1):

            @pl.when(depth > n)
            def _():
                send_outs(k, n, depth).wait_send()

    @pl.loop(0, 2 * bands)
    def _(i):
        send_in(i).wait_send()

    @pl.loop(0, steps)
    def _(i):
        send_out(i).wait_send()

    for copy in copies:
        copy.wait()
    total_ref[...] = jnp.broadcast_to(jnp.sum(heard[...], axis=0, keepdims=True), total_ref.shape)


def scale(total_ref, w_ref, out_ref, scaled, sems):
    bands, _, length, _, _ = w_ref.shape
    pieces = sems.shape[0]
    depth = length // pieces
    row = total_ref[0:1]
    lane = lax.div(lax.broadcasted_iota(jnp.int32, row.shape, 1), lanes // 4)
    sums = [jnp.sum(jnp.where(lane == k, row, 0.0), axis=1, keepdims=True) for k in range(4)]
    size = sums[0] + epsilon
    one_re, one_im, squares = sums[1] / size, sums[2] / size, sums[3] / size
    one = one_re * one_re + one_im * one_im
    denominator = squares - one * (epsilon / size) + epsilon
    re = jnp.broadcast_to(one_re / denominator, (rows, lanes))
    im = jnp.broadcast_to(-one_im / denominator, (rows, lanes))

    def save(i):
        part = pl.ds(i * depth, depth)
        return pltpu.make_async_copy(scaled.at[:, part], out_ref.at[:, part], sems.at[i])

    @pl.loop(0, pieces)
    def _(i):
        @pl.loop(0, depth, unroll=4)
        def _(j):
            x = i * depth + j
            for y in range(bands):
                w_re, w_im = w_ref[y, 0, x], w_ref[y, 1, x]
                scaled[0, x, y * rows : (y + 1) * rows] = re * w_re - im * w_im
                scaled[1, x, y * rows : (y + 1) * rows] = re * w_im + im * w_re

        save(i).start()

    @pl.loop(0, pieces)
    def _(i):
        save(i).wait()


def on_device(blocks, parts, source, speed):
    _, length_x, number, width = source.shape
    length_z = width * parts
    part = length_x // parts
    tile = 2 * rows
    bands, tiles = number // rows, part // tile
    span = rows * blocks // 2
    groups, places, peers = part // span, blocks // 2, blocks * parts - 1
    f32 = jnp.float32
    shape, dma = jax.ShapeDtypeStruct, pltpu.SemaphoreType.DMA

    def vmem(*size):
        return pltpu.VMEM(size, f32)

    anywhere, inside = pl.BlockSpec(memory_space=pl.ANY), pl.BlockSpec(memory_space=pltpu.VMEM)
    image, sums = pl.pallas_call(
        functools.partial(solve_all, blocks, parts),
        in_specs=[anywhere] * 7,
        out_specs=[inside, inside],
        out_shape=[vmem(bands, 2, length_x, rows, width), vmem(rows, width)],
        scratch_shapes=[
            vmem(2 * bands, length_x, rows, width),
            vmem(bands, length_x, rows, width),
            vmem(2, part, length_z),
            vmem(10, part, lanes),
            vmem(tiles, 3, 2, number, tile, width),
            vmem(tiles // 2, 2, number, tile, length_z),
            vmem(tiles // 2, 2, number, tile, length_z),
            vmem(2, number, tile, length_z),
            vmem(2, number, tile, length_z),
            vmem(groups, 3, 4, span, lanes),
            vmem(groups, 4, span, lanes),
            vmem(groups, 2, 2, span, lanes),
            vmem(groups, 2, span, lanes),
            vmem(groups, 2, 2, span, lanes),
            vmem(groups, places // 2, 2, span, lanes),
            vmem(groups, 2, span, lanes),
            vmem(groups, 2, 4, span, lanes),
            vmem(groups, 2, 4, span, lanes),
            vmem(3, 2, number, part, width),
            pltpu.VMEM((2, length_x, length_x), jnp.bfloat16),
            pltpu.VMEM((2, length_z, length_z), jnp.bfloat16),
            vmem(rows, width),
            vmem(peers + 1, width),
            dma((2 * bands,)),
            dma((bands,)),
            dma((5,)),
            dma((2 * bands,)),
            dma((2 * bands,)),
        ]
        + [dma((tiles,))] * 2
        + [dma((groups,))] * 2
        + [dma((groups, places - 1)), dma((groups, 2))]
        + [dma((groups, places // 2))] * 2
        + [dma((tiles,))] * 2
        + [dma((tiles,))] * 2
        + [dma((peers,))] * 2,
        compiler_params=pltpu.CompilerParams(
            vmem_limit_bytes=55 * 1024 * 1024, collective_id=0, has_side_effects=True
        ),
        name="solve_all",
    )(source, speed, root_table(length_x, length_z), *sine_table(length_x), *sine_table(length_z))
    pieces = 16
    return pl.pallas_call(
        scale,
        in_specs=[inside, inside],
        out_specs=anywhere,
        out_shape=shape(source.shape, f32),
        scratch_shapes=[vmem(*source.shape), dma((pieces,))],
        compiler_params=pltpu.CompilerParams(vmem_limit_bytes=20 * 1024 * 1024),
        name="scale",
    )(sums, image)


def solution(mesh):
    return jax.shard_map(
        functools.partial(on_device, mesh.shape["px"], mesh.shape["py"]),
        mesh=mesh,
        in_specs=(P(None, "samples", "px", "py"), P("samples", "px", "py")),
        out_specs=P(None, "samples", "px", "py"),
        check_vma=False,
    )
```

```python
import functools

import jax
import jax.numpy as jnp
import numpy as np
from jax import lax
from jax.experimental import pallas as pl
from jax.experimental.pallas import tpu as pltpu
from jax.sharding import PartitionSpec as P

wave_square = 0.25
damped = 0.125
epsilon = 1e-06
rows = 8
lanes = 128
MESH = pl.DeviceIdType.MESH


def sine_table(length):
    index = np.arange(length, dtype=np.int64) + 1
    turns = (index[:, None] * index[None, :]) % (2 * (length + 1))
    table = np.sqrt(2.0 / (length + 1.0)) * np.sin(np.pi * turns / (length + 1.0))
    high = table.astype(np.float32).astype(jnp.bfloat16)
    low = (table - high.astype(np.float64)).astype(np.float32).astype(jnp.bfloat16)
    return jnp.asarray(high), jnp.asarray(low)


def eigen_line(length):
    sine_half = np.sin(np.pi * (np.arange(length) + 1.0) / (2.0 * (length + 1.0)))
    return 4.0 * sine_half * sine_half


def root_table(length_x, length_z):
    half = eigen_line(length_x)[:, None] + eigen_line(length_z)[None, :]
    half = (half + 2.0 - wave_square + 1j * damped) / 2.0
    root = 1.0 / (half + np.sqrt(half * half - 1.0))
    return jnp.asarray(np.stack([root.real, root.imag]).astype(np.float32))


def halves(values):
    high = values.astype(jnp.bfloat16)
    low = (values - high.astype(jnp.float32)).astype(jnp.bfloat16)
    return high, low


def dot_three(left, right):
    dot = functools.partial(jnp.dot, preferred_element_type=jnp.float32)
    return dot(left[0], right[0]) + (dot(left[0], right[1]) + dot(left[1], right[0]))


def times(a, b):
    return a[0] * b[0] - a[1] * b[1], a[0] * b[1] + a[1] * b[0]


def plus(a, b):
    return a[0] + b[0], a[1] + b[1]


def inverse(a):
    scale = 1.0 / (a[0] * a[0] + a[1] * a[1])
    return a[0] * scale, -a[1] * scale


def minus(a, b):
    return a[0] - b[0], a[1] - b[1]


def power(a, number):
    result = None
    while number:
        if number & 1:
            result = a if result is None else times(result, a)
        number >>= 1
        if number:
            a = times(a, a)
    return result


def pair_of(ref, plane=0):
    return ref[plane], ref[plane + 1]


def greet(peers):
    barrier = pltpu.get_barrier_semaphore()
    for peer in peers:
        pl.semaphore_signal(barrier, inc=1, device_id=peer, device_id_type=MESH)


def await_greetings(peers):
    pl.semaphore_wait(pltpu.get_barrier_semaphore(), len(peers))


def between(source, target, sent, received, device):
    return pltpu.make_async_remote_copy(
        src_ref=source,
        dst_ref=target,
        send_sem=sent,
        recv_sem=received,
        device_id=device,
        device_id_type=MESH,
    )


def remote(source, target, sends, receives, place, device):
    return between(source, target, sends.at[place], receives.at[place], device)


def solve_all(
    blocks,
    parts,
    source_ref,
    speed_ref,
    roots_ref,
    x_high_ref,
    x_low_ref,
    z_high_ref,
    z_low_ref,
    image,
    total_ref,
    source,
    speed,
    roots,
    rates,
    tiles,
    even_modes,
    odd_modes,
    even_work,
    odd_work,
    ends,
    pair,
    waves_out,
    waves,
    tops,
    outs,
    met,
    inner,
    edges,
    slots,
    x_halves,
    z_halves,
    squares_ref,
    heard,
    source_sem,
    speed_sem,
    table_sem,
    in_send,
    in_recv,
    ends_send,
    ends_recv,
    wave_send,
    wave_recv,
    top_send,
    top_recv,
    outs_send,
    outs_recv,
    edge_send,
    edge_recv,
    out_send,
    out_recv,
    sum_send,
    sum_recv,
):
    steps, _, _, number, tile, _ = tiles.shape
    _, length, _, _ = source.shape
    bands = number // rows
    part = length // parts
    length_z = even_modes.shape[-1]
    groups, _, _, span, _ = ends.shape
    per, places = span // tile, blocks // 2
    me = lax.axis_index("px")
    side, place = lax.rem(me, 2), lax.div(me, 2)
    other = me + 1 - 2 * side
    mine = lax.axis_index("py")
    beside = {"py": 1 - mine}
    depths = places // 2
    behind = lax.div(place, depths)
    depth = place + behind * (places - 1 - 2 * place)
    inmost = lax.div(depth + 1, depths)
    others = [lax.rem(place + k, places) for k in range(1, places)]
    toward = 1 - 2 * behind
    everyone = []
    for k in range(1, blocks * parts):
        peer = lax.rem(me * parts + mine + k, blocks * parts)
        everyone.append({"px": lax.div(peer, parts), "py": lax.rem(peer, parts)})

    def band(y):
        return pl.ds(pl.multiple_of(y * rows, rows), rows)

    def load_source(i):
        return pltpu.make_async_copy(
            source_ref.at[lax.div(i, bands), :, band(lax.rem(i, bands))], source.at[i], source_sem.at[i]
        )

    def load_speed(y):
        return pltpu.make_async_copy(speed_ref.at[:, band(y)], speed.at[y], speed_sem.at[y])

    root_rows = pl.ds(pl.multiple_of(mine * part, 8), part)
    tables = [
        (x_high_ref, x_halves.at[0]),
        (x_low_ref, x_halves.at[1]),
        (z_high_ref, z_halves.at[0]),
        (z_low_ref, z_halves.at[1]),
        (roots_ref.at[:, root_rows], roots),
    ]
    tables = [pltpu.make_async_copy(a, b, table_sem.at[k]) for k, (a, b) in enumerate(tables)]
    load_source(0).start()
    for copy in tables:
        copy.start()

    @pl.loop(1, 2 * bands)
    def _(i):
        load_source(i).start()

    @pl.loop(0, bands)
    def _(y):
        load_speed(y).start()

    greet(everyone)
    for copy in tables[:2]:
        copy.wait()
    x_table = (x_halves[0], x_halves[1])

    def slot_of(h, own):
        return own + lax.rem(h + own, 2) * (2 - own)

    def send_in(i):
        c, y = lax.div(i, bands), lax.rem(i, bands)
        return remote(
            tiles.at[:, 2, c, band(y)], tiles.at[:, mine, c, band(y)], in_send, in_recv, 0, beside
        )

    @pl.loop(0, 2 * bands)
    def _(i):
        load_source(i).wait()
        c, y = lax.div(i, bands), lax.rem(i, bands)
        flat = source.at[i].reshape(length * rows, lanes)
        for j in range(0, rows, 2):
            pieces = [flat[pl.ds(j + k, length, stride=rows), :] for k in range(2)]
            result = dot_three(x_table, halves(jnp.concatenate(pieces, axis=1)))
            for k in range(2):
                for h in range(parts):
                    block = result[h * part : (h + 1) * part, k * lanes : (k + 1) * lanes]
                    tiles[:, slot_of(h, mine), c, y * rows + j + k] = block.reshape(steps, tile, lanes)

        @pl.when(i == 0)
        def _():
            await_greetings(everyone)

        send_in(i).start()

    for copy in tables[2:]:
        copy.wait()
    table = (z_halves[0], z_halves[1])
    zero = jnp.zeros((tile, length_z), jnp.float32)
    own_lanes = pl.ds(pl.multiple_of(side * lanes, lanes), lanes)
    root = (roots[0, :, own_lanes], roots[1, :, own_lanes])
    jump = power(root, number)
    rate = times(jump, jump)
    double = times(rate, rate)
    echo = (-root[0], -root[1])
    for n in range(1, depths):
        deeper = times(echo, double)
        echo = tuple(jnp.where(depth >= n, a, b) for a, b in zip(deeper, echo))
    whole = power(root, blocks * number + 1)
    square = times(whole, whole)
    spread = inverse((1.0 - square[0], -square[1]))
    for n, values in enumerate((jump, rate, echo, whole, spread)):
        rates[2 * n] = values[0]
        rates[2 * n + 1] = values[1]

    def send_ends(k, i):
        spot = pl.ds(pl.multiple_of(i * tile, tile), tile)
        return between(
            ends.at[k, 2, :, spot],
            ends.at[k, side, :, spot],
            ends_send.at[0],
            ends_recv.at[k],
            {"px": other},
        )

    def wave(k, place):
        return between(
            waves_out.at[k, 0], waves.at[k], wave_send.at[0], wave_recv.at[k], {"px": 2 * place + side}
        )

    def send_top(k, i, from_side):
        return pltpu.make_async_remote_copy(
            src_ref=tops.at[k, from_side],
            dst_ref=tops.at[k, from_side],
            send_sem=top_send.at[i],
            recv_sem=top_recv.at[k, from_side],
            device_id={"px": 2 * others[i] + side},
            device_id_type=MESH,
        )

    def send_outs(k, to_depth, from_depth):
        return pltpu.make_async_remote_copy(
            src_ref=waves_out.at[k, 1],
            dst_ref=outs.at[k, from_depth],
            send_sem=outs_send.at[to_depth],
            recv_sem=outs_recv.at[k, from_depth - 1],
            device_id={"px": 2 * (to_depth + behind * (places - 1 - 2 * to_depth)) + side},
            device_id_type=MESH,
        )

    def send_edges(k, i):
        spot = pl.ds(pl.multiple_of(i * tile, tile), tile)
        return between(
            inner.at[k, 1 - side, :, spot],
            edges.at[k, side, :, spot],
            edge_send.at[0],
            edge_recv.at[k * per + i],
            {"px": other},
        )

    def group_rates(k, *which):
        part = pl.ds(k * span, span) if isinstance(k, int) else pl.ds(pl.multiple_of(k * span, span), span)
        return [(rates[2 * n, part], rates[2 * n + 1, part]) for n in which]

    def tile_root(i):
        part = pl.ds(pl.multiple_of(i * tile, tile), tile)
        return roots[0, part], roots[1, part]

    modes, work = (even_modes, odd_modes), (even_work, odd_work)

    def transform_z(p, odd):
        for c in range(2):
            pieces = [tiles[2 * p + odd, h, c].reshape(number * tile, lanes) for h in range(parts)]
            result = dot_three(halves(jnp.concatenate(pieces, axis=1)), table)
            modes[odd][p, c] = result.reshape(number, tile, length_z)

    def sweep(p, odd):
        s = 2 * p + odd
        k, i = lax.div(s, per), lax.rem(s, per)
        root = tile_root(s)
        first, last = (zero, zero), (zero, zero)
        for j in range(number):
            back = number - 1 - j
            last = plus(times(root, last), (modes[odd][p, 0, j], modes[odd][p, 1, j]))
            first = plus(times(root, first), (modes[odd][p, 0, back], modes[odd][p, 1, back]))
        part = pl.ds(pl.multiple_of(i * tile, tile), tile)
        for h in range(2):
            slot = slot_of(h, side)
            for plane, value in enumerate(first + last):
                ends[k, slot, plane, part] = value[:, h * lanes : (h + 1) * lanes]
        return send_ends(k, i)

    def either(a, b):
        return tuple(jnp.where(behind == 0, x, y) for x, y in zip(a, b))

    def pass_inward(k, rate, echo, came):
        bounced = times(echo, pair_of(pair.at[k], 2))
        value = plus(pair_of(pair.at[k]), times(rate, plus(came, bounced)))

        @pl.when(inmost == 0)
        def _():
            for c in range(2):
                waves_out[k, 0, c] = value[c]
            wave(k, place + toward).start()

        @pl.when(inmost == 1)
        def _():
            for c in range(2):
                tops[k, behind, c] = value[c]
            for i in range(places - 1):
                send_top(k, i, behind).start()

    def merge(k):
        between(
            ends.at[k, 2], ends.at[k, 1 - side], ends_send.at[0], ends_recv.at[k], {"px": other}
        ).wait_recv()
        jump, rate, echo = group_rates(k, 0, 1, 2)
        first = plus(pair_of(ends.at[k, 0]), times(jump, pair_of(ends.at[k, 1])))
        last = plus(pair_of(ends.at[k, 1], 2), times(jump, pair_of(ends.at[k, 0], 2)))
        for plane, value in enumerate(either(last, first) + either(first, last)):
            pair[k, plane] = value

        @pl.when(depth > 0)
        def _():
            for c in range(2):
                waves_out[k, 1, c] = pair[k, 2 + c]

        for n in range(depths - 1):

            @pl.when(depth > n)
            def _():
                send_outs(k, n, depth).start()

        @pl.when(depth == 0)
        def _():
            none = jnp.zeros((span, lanes), jnp.float32)
            for c in range(2):
                waves[k, c] = none
            pass_inward(k, rate, echo, (none, none))

    def relay(k):
        @pl.when(depth > 0)
        def _():
            wave(k, place - toward).wait_recv()
            rate, echo = group_rates(k, 1, 2)
            pass_inward(k, rate, echo, pair_of(waves.at[k]))

    def expand(k):
        @pl.when(inmost == 0)
        def _():
            send_top(k, 0, behind).wait_recv()

        send_top(k, 0, 1 - behind).wait_recv()
        jump, rate, echo, whole, spread = group_rates(k, 0, 1, 2, 3, 4)
        ours, theirs = pair_of(tops.at[k, behind]), pair_of(tops.at[k, 1 - behind])
        value = times(spread, minus(theirs, times(whole, ours)))
        for c in range(2):
            met[k, c] = value[c]
        for n in range(depths - 1, 0, -1):

            @pl.when(depth < n)
            def _():
                send_outs(k, 0, n).wait_recv()
                value = plus(pair_of(outs.at[k, n]), times(rate, pair_of(met.at[k])))
                for c in range(2):
                    met[k, c] = value[c]

        came = pair_of(met.at[k])
        out = plus(pair_of(pair.at[k], 2), times(rate, came))
        back = plus(pair_of(waves.at[k]), times(echo, out))
        before, after = either(back, came), either(came, back)
        left = before + plus(pair_of(ends.at[k, 1]), times(jump, after))
        right = plus(pair_of(ends.at[k, 0], 2), times(jump, before)) + after
        for q, values in enumerate((left, right)):
            for plane, value in enumerate(values):
                inner[k, q, plane] = value
        for i in range(per):
            send_edges(k, i).start()
        edges[k, side] = inner[k, side]

    def send_out(i, c):
        spot = pl.ds(pl.multiple_of(i * tile, tile), tile)
        return remote(slots.at[2, c, :, spot], slots.at[mine, c, :, spot], out_send, out_recv, 0, beside)

    def solve_y(p, odd):
        s = 2 * p + odd
        k, i = lax.div(s, per), lax.rem(s, per)
        root = tile_root(s)
        part = pl.ds(pl.multiple_of(i * tile, tile), tile)
        carried = [
            jnp.concatenate([edges[k, h, plane, part] for h in range(2)], axis=1) for plane in range(4)
        ]
        state, after = tuple(carried[:2]), tuple(carried[2:])
        for j in range(number):
            state = plus(times(root, state), (modes[odd][p, 0, j], modes[odd][p, 1, j]))
            work[odd][0, j] = state[0]
            work[odd][1, j] = state[1]
        square = times(root, root)
        scaled = times(root, inverse((1.0 - square[0], -square[1])))
        value = times(scaled, plus(times(root, state), after))
        for j in range(number - 1, -1, -1):
            value = times(root, plus(value, (work[odd][0, j], work[odd][1, j])))
            work[odd][0, j] = value[0]
            work[odd][1, j] = value[1]

    def emit(p, odd, parts_of=range(2)):
        s = 2 * p + odd
        spot = pl.ds(pl.multiple_of(s * tile, tile), tile)
        for c in parts_of:
            result = dot_three(halves(work[odd][c].reshape(number * tile, length_z)), table)
            for h in range(parts):
                block = result[:, h * lanes : (h + 1) * lanes]
                slots[slot_of(h, mine), c, :, spot] = block.reshape(number, tile, lanes)
        return [send_out(s, c) for c in parts_of]

    all_in = remote(tiles.at[:, 2], tiles.at[:, mine], in_send, in_recv, 0, beside)
    all_in.wait_recv()

    group = 8
    squares_ref[...] = jnp.zeros_like(squares_ref)

    def prepare(y):
        load_speed(y).wait()

        def step(i, square):
            some = pl.ds(i * group, group)
            v = speed[y, some]
            speed[y, some] = wave_square - wave_square / (v * v)
            s_re, s_im = source[y, some], source[bands + y, some]
            return square + jnp.sum(s_re * s_re + s_im * s_im, axis=0)

        squares_ref[...] += lax.fori_loop(
            0, length // group, step, jnp.zeros((rows, lanes), jnp.float32), unroll=2
        )

    lag = 2

    duos = steps // 2
    duos_of = per // 2

    def ready(p):
        @pl.when(jnp.logical_and(lax.rem(p + 1, duos_of) == 0, lax.div(p, duos_of) >= lag))
        def _():
            merge(lax.div(p, duos_of) - lag)

    transform_z(0, 0)

    @pl.loop(0, duos - 1)
    def _(p):
        copy = sweep(p, 0)
        transform_z(p, 1)
        copy.start()
        copy = sweep(p, 1)
        transform_z(p + 1, 0)
        copy.start()
        ready(p)

    copy = sweep(duos - 1, 0)
    transform_z(duos - 1, 1)
    copy.start()
    sweep(duos - 1, 1).start()
    if groups > lag:
        merge(groups - 1 - lag)
    early = 3
    stages = [(2.7, merge, k) for k in range(max(groups - lag, 0), groups)]
    stages += [(5.7, relay, k) for k in range(groups)]
    stages += [(10.4, expand, k) for k in range(min(early, groups))]
    stages += [(4.2, prepare, k) for k in range(bands)]
    for _, stage, k in sorted(stages, key=lambda item: 1.55 * item[2] + item[0]):
        stage(k)

    def await_edges(p, odd):
        s = 2 * p + odd
        send_edges(lax.div(s, per), lax.rem(s, per)).wait_recv()

    await_edges(0, 0)
    solve_y(0, 0)
    await_edges(0, 1)
    copies = emit(0, 0)
    solve_y(0, 1)
    for copy in copies:
        copy.start()

    @pl.loop(1, duos)
    def _(p):
        k = lax.div(p, duos_of)

        @pl.when(lax.rem(p, duos_of) == 0)
        def _():
            @pl.when(k - 1 + early < groups)
            def _():
                expand(k - 1 + early)

        await_edges(p, 0)
        copies = emit(p - 1, 1)
        solve_y(p, 0)
        for copy in copies:
            copy.start()

        await_edges(p, 1)
        copies = emit(p, 0)
        solve_y(p, 1)
        for copy in copies:
            copy.start()

    for c in range(2):
        emit(duos - 1, 1, [c])[0].start()

    all_out = remote(slots.at[2], slots.at[mine], out_send, out_recv, 0, beside)
    all_out.wait_recv()

    def transform(y, j):
        flat = image.at[y].reshape(2 * length * rows, lanes)
        for c in range(2):
            pieces = [
                jnp.concatenate([slots[h, c, y * rows + j + k] for h in range(parts)], axis=0)
                for k in range(2)
            ]
            result = dot_three(x_table, halves(jnp.concatenate(pieces, axis=1)))
            for k in range(2):
                flat[pl.ds(c * length * rows + j + k, length, stride=rows), :] = result[
                    :, k * lanes : (k + 1) * lanes
                ]

    def tally(y, i, sums):
        some = pl.ds(i * group, group)
        shift = speed[y, some]
        s_re, s_im = source[y, some], source[bands + y, some]
        w_re, w_im = image[y, 0, some], image[y, 1, some]
        u_re = s_re + shift * w_re + damped * w_im
        u_im = s_im + shift * w_im - damped * w_re
        terms = (
            s_re * u_re + s_im * u_im,
            s_re * u_im - s_im * u_re,
            u_re * u_re + u_im * u_im,
        )
        return tuple(a + jnp.sum(b, axis=0) for a, b in zip(sums, terms))

    pairs, runs = rows // 2, length // group

    def both(y, sums):
        for n in range(pairs):
            for i in range(n * runs // pairs, (n + 1) * runs // pairs):
                sums = tally(y - 1, i, sums)
            transform(y, 2 * n)
        return sums

    for n in range(pairs):
        transform(0, 2 * n)
    sums = lax.fori_loop(1, bands, both, (jnp.zeros((rows, lanes), jnp.float32),) * 3)
    sums = lax.fori_loop(0, runs, functools.partial(tally, bands - 1), sums, unroll=2)
    sums = [jnp.sum(a, axis=0, keepdims=True) for a in (squares_ref[...],) + sums]
    lane = lax.broadcasted_iota(jnp.int32, (1, lanes), 1)
    packed = jnp.zeros((1, lanes), jnp.float32)
    for k, row in enumerate(sums):
        for shift in (lanes // 2, lanes // 4):
            row = row + pltpu.roll(row, shift, 1)
        packed = jnp.where(lax.div(lane, lanes // 4) == k, row, packed)
    own = len(everyone)
    heard[own] = packed
    copies = [
        remote(heard.at[own], heard.at[k], sum_send, sum_recv, 0, peer)
        for k, peer in enumerate(everyone)
    ]
    for copy in copies:
        copy.start()

    between(ends.at[:, 2], ends.at[:, side], ends_send.at[0], ends_recv.at[0], {"px": other}).wait_send()
    between(inner.at[:, 1 - side], edges.at[:, side], edge_send.at[0], edge_recv.at[0], {"px": other}).wait_send()

    @pl.when(inmost == 0)
    def _():
        between(waves_out.at[:, 0], waves, wave_send.at[0], wave_recv.at[0], {"px": other}).wait_send()

    @pl.when(inmost == 1)
    def _():
        for i in range(places - 1):
            ours = tops.at[:, behind]
            between(ours, ours, top_send.at[i], top_recv.at[0, 0], {"px": other}).wait_send()

    for n in range(depths - 1):

        @pl.when(depth > n)
        def _():
            sent = waves_out.at[:, 1]
            between(sent, outs.at[:, 0], outs_send.at[n], outs_recv.at[0, 0], {"px": other}).wait_send()

    all_in.wait_send()
    all_out.wait_send()
    rest = heard.at[0:own]
    remote(rest, rest, sum_send, sum_recv, 0, everyone[0]).wait()
    total_ref[...] = jnp.broadcast_to(jnp.sum(heard[...], axis=0), total_ref.shape)


def scale(total_ref, w_ref, out_ref, scaled, sems):
    bands, _, length, _, _ = w_ref.shape
    pieces = sems.shape[0]
    depth = length // pieces
    row = total_ref[0:1]
    lane = lax.div(lax.broadcasted_iota(jnp.int32, row.shape, 1), lanes // 4)
    sums = [jnp.sum(jnp.where(lane == k, row, 0.0), axis=1, keepdims=True) for k in range(4)]
    size = sums[0] + epsilon
    one_re, one_im, squares = sums[1] / size, sums[2] / size, sums[3] / size
    one = one_re * one_re + one_im * one_im
    denominator = squares - one * (epsilon / size) + epsilon
    re = jnp.broadcast_to(one_re / denominator, (rows, lanes))
    im = jnp.broadcast_to(-one_im / denominator, (rows, lanes))

    def save(i):
        part = pl.ds(i * depth, depth)
        return pltpu.make_async_copy(scaled.at[:, part], out_ref.at[:, part], sems.at[i])

    @pl.loop(0, pieces)
    def _(i):
        @pl.loop(0, depth, unroll=4)
        def _(j):
            x = i * depth + j
            for y in range(bands):
                w_re, w_im = w_ref[y, 0, x], w_ref[y, 1, x]
                scaled[0, x, y * rows : (y + 1) * rows] = re * w_re - im * w_im
                scaled[1, x, y * rows : (y + 1) * rows] = re * w_im + im * w_re

        save(i).start()

    @pl.loop(0, pieces)
    def _(i):
        save(i).wait()


def on_device(blocks, parts, source, speed):
    _, length_x, number, width = source.shape
    length_z = width * parts
    part = length_x // parts
    tile = 2 * rows
    bands, tiles = number // rows, part // tile
    span = rows * blocks // 2
    groups, places, peers = part // span, blocks // 2, blocks * parts - 1
    f32 = jnp.float32
    shape, dma = jax.ShapeDtypeStruct, pltpu.SemaphoreType.DMA

    def vmem(*size):
        return pltpu.VMEM(size, f32)

    anywhere, inside = pl.BlockSpec(memory_space=pl.ANY), pl.BlockSpec(memory_space=pltpu.VMEM)
    image, sums = pl.pallas_call(
        functools.partial(solve_all, blocks, parts),
        in_specs=[anywhere] * 7,
        out_specs=[inside, inside],
        out_shape=[vmem(bands, 2, length_x, rows, width), vmem(rows, width)],
        scratch_shapes=[
            vmem(2 * bands, length_x, rows, width),
            vmem(bands, length_x, rows, width),
            vmem(2, part, length_z),
            vmem(10, part, lanes),
            vmem(tiles, 3, 2, number, tile, width),
            vmem(tiles // 2, 2, number, tile, length_z),
            vmem(tiles // 2, 2, number, tile, length_z),
            vmem(2, number, tile, length_z),
            vmem(2, number, tile, length_z),
            vmem(groups, 3, 4, span, lanes),
            vmem(groups, 4, span, lanes),
            vmem(groups, 2, 2, span, lanes),
            vmem(groups, 2, span, lanes),
            vmem(groups, 2, 2, span, lanes),
            vmem(groups, places // 2, 2, span, lanes),
            vmem(groups, 2, span, lanes),
            vmem(groups, 2, 4, span, lanes),
            vmem(groups, 2, 4, span, lanes),
            vmem(3, 2, number, part, width),
            pltpu.VMEM((2, length_x, length_x), jnp.bfloat16),
            pltpu.VMEM((2, length_z, length_z), jnp.bfloat16),
            vmem(rows, width),
            vmem(peers + 1, 1, width),
            dma((2 * bands,)),
            dma((bands,)),
            dma((5,)),
            dma((1,)),
            dma((1,)),
            dma((1,)),
            dma((groups,)),
            dma((1,)),
            dma((groups,)),
            dma((places - 1,)),
            dma((groups, 2)),
            dma((places // 2,)),
            dma((groups, places // 2 - 1)),
            dma((1,)),
            dma((tiles,)),
            dma((1,)),
            dma((1,)),
            dma((1,)),
            dma((1,)),
        ],
        compiler_params=pltpu.CompilerParams(
            vmem_limit_bytes=55 * 1024 * 1024, collective_id=0, has_side_effects=True
        ),
        name="solve_all",
    )(source, speed, root_table(length_x, length_z), *sine_table(length_x), *sine_table(length_z))
    pieces = 16
    return pl.pallas_call(
        scale,
        in_specs=[inside, inside],
        out_specs=anywhere,
        out_shape=shape(source.shape, f32),
        scratch_shapes=[vmem(*source.shape), dma((pieces,))],
        compiler_params=pltpu.CompilerParams(vmem_limit_bytes=20 * 1024 * 1024),
        name="scale",
    )(sums, image)


def solution(mesh):
    return jax.shard_map(
        functools.partial(on_device, mesh.shape["px"], mesh.shape["py"]),
        mesh=mesh,
        in_specs=(P(None, "samples", "px", "py"), P("samples", "px", "py")),
        out_specs=P(None, "samples", "px", "py"),
        check_vma=False,
    )
```

```python
import functools

import jax
import jax.numpy as jnp
import numpy as np
from jax import lax
from jax.experimental import pallas as pl
from jax.experimental.pallas import tpu as pltpu
from jax.sharding import PartitionSpec as P

wave_square = 0.25
damped = 0.125
epsilon = 1e-06
rows = 8
lanes = 128
MESH = pl.DeviceIdType.MESH


def sine_table(length):
    index = np.arange(length, dtype=np.int64) + 1
    turns = (index[:, None] * index[None, :]) % (2 * (length + 1))
    table = np.sqrt(2.0 / (length + 1.0)) * np.sin(np.pi * turns / (length + 1.0))
    high = table.astype(np.float32).astype(jnp.bfloat16)
    low = (table - high.astype(np.float64)).astype(np.float32).astype(jnp.bfloat16)
    return jnp.asarray(high), jnp.asarray(low)


def eigen_line(length):
    sine_half = np.sin(np.pi * (np.arange(length) + 1.0) / (2.0 * (length + 1.0)))
    return 4.0 * sine_half * sine_half


def root_table(length_x, length_z):
    half = eigen_line(length_x)[:, None] + eigen_line(length_z)[None, :]
    half = (half + 2.0 - wave_square + 1j * damped) / 2.0
    root = 1.0 / (half + np.sqrt(half * half - 1.0))
    return jnp.asarray(np.stack([root.real, root.imag]).astype(np.float32))


def halves(values):
    high = values.astype(jnp.bfloat16)
    low = (values - high.astype(jnp.float32)).astype(jnp.bfloat16)
    return high, low


def dot_three(left, right):
    dot = functools.partial(jnp.dot, preferred_element_type=jnp.float32)
    return dot(left[0], right[0]) + (dot(left[0], right[1]) + dot(left[1], right[0]))


def times(a, b):
    return a[0] * b[0] - a[1] * b[1], a[0] * b[1] + a[1] * b[0]


def plus(a, b):
    return a[0] + b[0], a[1] + b[1]


def inverse(a):
    scale = 1.0 / (a[0] * a[0] + a[1] * a[1])
    return a[0] * scale, -a[1] * scale


def minus(a, b):
    return a[0] - b[0], a[1] - b[1]


def power(a, number):
    result = None
    while number:
        if number & 1:
            result = a if result is None else times(result, a)
        number >>= 1
        if number:
            a = times(a, a)
    return result


def pair_of(ref, plane=0):
    return ref[plane], ref[plane + 1]


def greet(peers):
    barrier = pltpu.get_barrier_semaphore()
    for peer in peers:
        pl.semaphore_signal(barrier, inc=1, device_id=peer, device_id_type=MESH)


def await_greetings(peers):
    pl.semaphore_wait(pltpu.get_barrier_semaphore(), len(peers))


def between(source, target, sent, received, device):
    return pltpu.make_async_remote_copy(
        src_ref=source,
        dst_ref=target,
        send_sem=sent,
        recv_sem=received,
        device_id=device,
        device_id_type=MESH,
    )


def remote(source, target, sends, receives, place, device):
    return between(source, target, sends.at[place], receives.at[place], device)


def solve_all(
    blocks,
    parts,
    source_ref,
    speed_ref,
    roots_ref,
    x_high_ref,
    x_low_ref,
    z_high_ref,
    z_low_ref,
    image,
    total_ref,
    source,
    speed,
    roots,
    rates,
    tiles,
    even_modes,
    odd_modes,
    even_work,
    odd_work,
    ends,
    pair,
    waves_out,
    waves,
    tops,
    outs,
    met,
    inner,
    edges,
    slots,
    x_halves,
    z_halves,
    squares_ref,
    heard,
    source_sem,
    speed_sem,
    table_sem,
    in_send,
    in_recv,
    ends_send,
    ends_recv,
    wave_send,
    wave_recv,
    top_send,
    top_recv,
    outs_send,
    outs_recv,
    edge_send,
    edge_recv,
    out_send,
    out_recv,
    sum_send,
    sum_recv,
):
    steps, _, _, number, tile, _ = tiles.shape
    _, length, _, _ = source.shape
    bands = number // rows
    part = length // parts
    length_z = even_modes.shape[-1]
    groups, _, _, span, _ = ends.shape
    per, places = span // tile, blocks // 2
    me = lax.axis_index("px")
    side, place = lax.rem(me, 2), lax.div(me, 2)
    other = me + 1 - 2 * side
    mine = lax.axis_index("py")
    beside = {"py": 1 - mine}
    depths = places // 2
    behind = lax.div(place, depths)
    depth = place + behind * (places - 1 - 2 * place)
    inmost = lax.div(depth + 1, depths)
    others = [lax.rem(place + k, places) for k in range(1, places)]
    toward = 1 - 2 * behind
    everyone = []
    for k in range(1, blocks * parts):
        peer = lax.rem(me * parts + mine + k, blocks * parts)
        everyone.append({"px": lax.div(peer, parts), "py": lax.rem(peer, parts)})

    def band(y):
        return pl.ds(pl.multiple_of(y * rows, rows), rows)

    def load_source(i):
        return pltpu.make_async_copy(
            source_ref.at[lax.div(i, bands), :, band(lax.rem(i, bands))], source.at[i], source_sem.at[i]
        )

    def load_speed(y):
        return pltpu.make_async_copy(speed_ref.at[:, band(y)], speed.at[y], speed_sem.at[y])

    root_rows = pl.ds(pl.multiple_of(mine * part, 8), part)
    tables = [
        (x_high_ref, x_halves.at[0]),
        (x_low_ref, x_halves.at[1]),
        (z_high_ref, z_halves.at[0]),
        (z_low_ref, z_halves.at[1]),
        (roots_ref.at[:, root_rows], roots),
    ]
    tables = [pltpu.make_async_copy(a, b, table_sem.at[k]) for k, (a, b) in enumerate(tables)]
    load_source(0).start()
    for copy in tables:
        copy.start()

    @pl.loop(1, 2 * bands)
    def _(i):
        load_source(i).start()

    @pl.loop(0, bands)
    def _(y):
        load_speed(y).start()

    greet(everyone)
    for copy in tables[:2]:
        copy.wait()
    x_table = (x_halves[0], x_halves[1])

    def slot_of(h, own):
        return own + lax.rem(h + own, 2) * (2 - own)

    def send_in(i):
        c, y = lax.div(i, bands), lax.rem(i, bands)
        return remote(
            tiles.at[:, 2, c, band(y)], tiles.at[:, mine, c, band(y)], in_send, in_recv, 0, beside
        )

    @pl.loop(0, 2 * bands)
    def _(i):
        load_source(i).wait()
        c, y = lax.div(i, bands), lax.rem(i, bands)
        flat = source.at[i].reshape(length * rows, lanes)
        for j in range(0, rows, 2):
            pieces = [flat[pl.ds(j + k, length, stride=rows), :] for k in range(2)]
            result = dot_three(x_table, halves(jnp.concatenate(pieces, axis=1)))
            for k in range(2):
                for h in range(parts):
                    block = result[h * part : (h + 1) * part, k * lanes : (k + 1) * lanes]
                    tiles[:, slot_of(h, mine), c, y * rows + j + k] = block.reshape(steps, tile, lanes)

        @pl.when(i == 0)
        def _():
            await_greetings(everyone)

        send_in(i).start()

    for copy in tables[2:]:
        copy.wait()
    table = (z_halves[0], z_halves[1])
    zero = jnp.zeros((tile, length_z), jnp.float32)
    own_lanes = pl.ds(pl.multiple_of(side * lanes, lanes), lanes)
    root = (roots[0, :, own_lanes], roots[1, :, own_lanes])
    jump = power(root, number)
    rate = times(jump, jump)
    double = times(rate, rate)
    echo = (-root[0], -root[1])
    for n in range(1, depths):
        deeper = times(echo, double)
        echo = tuple(jnp.where(depth >= n, a, b) for a, b in zip(deeper, echo))
    whole = power(root, blocks * number + 1)
    square = times(whole, whole)
    spread = inverse((1.0 - square[0], -square[1]))
    for n, values in enumerate((jump, rate, echo, whole, spread)):
        rates[2 * n] = values[0]
        rates[2 * n + 1] = values[1]

    def send_ends(k, i):
        spot = pl.ds(pl.multiple_of(i * tile, tile), tile)
        return between(
            ends.at[k, 2, :, spot],
            ends.at[k, side, :, spot],
            ends_send.at[0],
            ends_recv.at[k],
            {"px": other},
        )

    def wave(k, place):
        return between(
            waves_out.at[k, 0], waves.at[k], wave_send.at[0], wave_recv.at[k], {"px": 2 * place + side}
        )

    def send_top(k, i, from_side):
        return pltpu.make_async_remote_copy(
            src_ref=tops.at[k, from_side],
            dst_ref=tops.at[k, from_side],
            send_sem=top_send.at[i],
            recv_sem=top_recv.at[k, from_side],
            device_id={"px": 2 * others[i] + side},
            device_id_type=MESH,
        )

    def send_outs(k, to_depth, from_depth):
        return pltpu.make_async_remote_copy(
            src_ref=waves_out.at[k, 1],
            dst_ref=outs.at[k, from_depth],
            send_sem=outs_send.at[to_depth],
            recv_sem=outs_recv.at[k, from_depth - 1],
            device_id={"px": 2 * (to_depth + behind * (places - 1 - 2 * to_depth)) + side},
            device_id_type=MESH,
        )

    def send_edges(k, i):
        spot = pl.ds(pl.multiple_of(i * tile, tile), tile)
        return between(
            inner.at[k, 1 - side, :, spot],
            edges.at[k, side, :, spot],
            edge_send.at[0],
            edge_recv.at[k * per + i],
            {"px": other},
        )

    def group_rates(k, *which):
        part = pl.ds(k * span, span) if isinstance(k, int) else pl.ds(pl.multiple_of(k * span, span), span)
        return [(rates[2 * n, part], rates[2 * n + 1, part]) for n in which]

    def tile_root(i):
        part = pl.ds(pl.multiple_of(i * tile, tile), tile)
        return roots[0, part], roots[1, part]

    modes, work = (even_modes, odd_modes), (even_work, odd_work)

    def transform_z(p, odd):
        for c in range(2):
            pieces = [tiles[2 * p + odd, h, c].reshape(number * tile, lanes) for h in range(parts)]
            result = dot_three(halves(jnp.concatenate(pieces, axis=1)), table)
            modes[odd][p, c] = result.reshape(number, tile, length_z)

    def sweep(p, odd):
        s = 2 * p + odd
        k, i = lax.div(s, per), lax.rem(s, per)
        root = tile_root(s)
        first, last = (zero, zero), (zero, zero)
        for j in range(number):
            back = number - 1 - j
            last = plus(times(root, last), (modes[odd][p, 0, j], modes[odd][p, 1, j]))
            first = plus(times(root, first), (modes[odd][p, 0, back], modes[odd][p, 1, back]))
        part = pl.ds(pl.multiple_of(i * tile, tile), tile)
        for h in range(2):
            slot = slot_of(h, side)
            for plane, value in enumerate(first + last):
                ends[k, slot, plane, part] = value[:, h * lanes : (h + 1) * lanes]
        return send_ends(k, i)

    def either(a, b):
        return tuple(jnp.where(behind == 0, x, y) for x, y in zip(a, b))

    def pass_inward(k, rate, echo, came):
        bounced = times(echo, pair_of(pair.at[k], 2))
        value = plus(pair_of(pair.at[k]), times(rate, plus(came, bounced)))

        @pl.when(inmost == 0)
        def _():
            for c in range(2):
                waves_out[k, 0, c] = value[c]
            wave(k, place + toward).start()

        @pl.when(inmost == 1)
        def _():
            for c in range(2):
                tops[k, behind, c] = value[c]
            for i in range(places - 1):
                send_top(k, i, behind).start()

    def merge(k):
        between(
            ends.at[k, 2], ends.at[k, 1 - side], ends_send.at[0], ends_recv.at[k], {"px": other}
        ).wait_recv()
        jump, rate, echo = group_rates(k, 0, 1, 2)
        first = plus(pair_of(ends.at[k, 0]), times(jump, pair_of(ends.at[k, 1])))
        last = plus(pair_of(ends.at[k, 1], 2), times(jump, pair_of(ends.at[k, 0], 2)))
        for plane, value in enumerate(either(last, first) + either(first, last)):
            pair[k, plane] = value

        @pl.when(depth > 0)
        def _():
            for c in range(2):
                waves_out[k, 1, c] = pair[k, 2 + c]

        for n in range(depths - 1):

            @pl.when(depth > n)
            def _():
                send_outs(k, n, depth).start()

        @pl.when(depth == 0)
        def _():
            none = jnp.zeros((span, lanes), jnp.float32)
            for c in range(2):
                waves[k, c] = none
            pass_inward(k, rate, echo, (none, none))

    def relay(k):
        @pl.when(depth > 0)
        def _():
            wave(k, place - toward).wait_recv()
            rate, echo = group_rates(k, 1, 2)
            pass_inward(k, rate, echo, pair_of(waves.at[k]))

    def expand(k):
        @pl.when(inmost == 0)
        def _():
            send_top(k, 0, behind).wait_recv()

        send_top(k, 0, 1 - behind).wait_recv()
        jump, rate, echo, whole, spread = group_rates(k, 0, 1, 2, 3, 4)
        ours, theirs = pair_of(tops.at[k, behind]), pair_of(tops.at[k, 1 - behind])
        value = times(spread, minus(theirs, times(whole, ours)))
        for c in range(2):
            met[k, c] = value[c]
        for n in range(depths - 1, 0, -1):

            @pl.when(depth < n)
            def _():
                send_outs(k, 0, n).wait_recv()
                value = plus(pair_of(outs.at[k, n]), times(rate, pair_of(met.at[k])))
                for c in range(2):
                    met[k, c] = value[c]

        came = pair_of(met.at[k])
        out = plus(pair_of(pair.at[k], 2), times(rate, came))
        back = plus(pair_of(waves.at[k]), times(echo, out))
        before, after = either(back, came), either(came, back)
        left = before + plus(pair_of(ends.at[k, 1]), times(jump, after))
        right = plus(pair_of(ends.at[k, 0], 2), times(jump, before)) + after
        for q, values in enumerate((left, right)):
            for plane, value in enumerate(values):
                inner[k, q, plane] = value
        for i in range(per):
            send_edges(k, i).start()
        edges[k, side] = inner[k, side]

    def send_out(i, c):
        spot = pl.ds(pl.multiple_of(i * tile, tile), tile)
        return remote(slots.at[2, c, :, spot], slots.at[mine, c, :, spot], out_send, out_recv, 0, beside)

    def solve_y(p, odd):
        s = 2 * p + odd
        k, i = lax.div(s, per), lax.rem(s, per)
        root = tile_root(s)
        part = pl.ds(pl.multiple_of(i * tile, tile), tile)
        carried = [
            jnp.concatenate([edges[k, h, plane, part] for h in range(2)], axis=1) for plane in range(4)
        ]
        state, after = tuple(carried[:2]), tuple(carried[2:])
        for j in range(number):
            state = plus(times(root, state), (modes[odd][p, 0, j], modes[odd][p, 1, j]))
            work[odd][0, j] = state[0]
            work[odd][1, j] = state[1]
        square = times(root, root)
        scaled = times(root, inverse((1.0 - square[0], -square[1])))
        value = times(scaled, plus(times(root, state), after))
        for j in range(number - 1, -1, -1):
            value = times(root, plus(value, (work[odd][0, j], work[odd][1, j])))
            work[odd][0, j] = value[0]
            work[odd][1, j] = value[1]

    def emit(p, odd, parts_of=range(2)):
        s = 2 * p + odd
        spot = pl.ds(pl.multiple_of(s * tile, tile), tile)
        for c in parts_of:
            result = dot_three(halves(work[odd][c].reshape(number * tile, length_z)), table)
            for h in range(parts):
                block = result[:, h * lanes : (h + 1) * lanes]
                slots[slot_of(h, mine), c, :, spot] = block.reshape(number, tile, lanes)
        return [send_out(s, c) for c in parts_of]

    all_in = remote(tiles.at[:, 2], tiles.at[:, mine], in_send, in_recv, 0, beside)
    all_in.wait_recv()

    group = 8
    squares_ref[...] = jnp.zeros_like(squares_ref)

    def prepare(y):
        load_speed(y).wait()

        def step(i, square):
            some = pl.ds(i * group, group)
            v = speed[y, some]
            speed[y, some] = wave_square - wave_square / (v * v)
            s_re, s_im = source[y, some], source[bands + y, some]
            return square + jnp.sum(s_re * s_re + s_im * s_im, axis=0)

        squares_ref[...] += lax.fori_loop(
            0, length // group, step, jnp.zeros((rows, lanes), jnp.float32), unroll=2
        )

    lag = 2

    duos = steps // 2
    duos_of = per // 2

    def ready(p):
        @pl.when(jnp.logical_and(lax.rem(p + 1, duos_of) == 0, lax.div(p, duos_of) >= lag))
        def _():
            merge(lax.div(p, duos_of) - lag)

    transform_z(0, 0)

    @pl.loop(0, duos - 1)
    def _(p):
        copy = sweep(p, 0)
        transform_z(p, 1)
        copy.start()
        copy = sweep(p, 1)
        transform_z(p + 1, 0)
        copy.start()
        ready(p)

    copy = sweep(duos - 1, 0)
    transform_z(duos - 1, 1)
    copy.start()
    sweep(duos - 1, 1).start()
    if groups > lag:
        merge(groups - 1 - lag)
    early = 3
    stages = [(2.7, merge, k) for k in range(max(groups - lag, 0), groups)]
    stages += [(5.7, relay, k) for k in range(groups)]
    stages += [(10.4, expand, k) for k in range(min(early, groups))]
    stages += [(4.2, prepare, k) for k in range(bands)]
    for _, stage, k in sorted(stages, key=lambda item: 1.55 * item[2] + item[0]):
        stage(k)

    def await_edges(p, odd):
        s = 2 * p + odd
        send_edges(lax.div(s, per), lax.rem(s, per)).wait_recv()

    await_edges(0, 0)
    solve_y(0, 0)
    await_edges(0, 1)
    copies = emit(0, 0)
    solve_y(0, 1)
    for copy in copies:
        copy.start()

    @pl.loop(1, duos)
    def _(p):
        k = lax.div(p, duos_of)

        @pl.when(lax.rem(p, duos_of) == 0)
        def _():
            @pl.when(k - 1 + early < groups)
            def _():
                expand(k - 1 + early)

        await_edges(p, 0)
        copies = emit(p - 1, 1)
        solve_y(p, 0)
        for copy in copies:
            copy.start()

        await_edges(p, 1)
        copies = emit(p, 0)
        solve_y(p, 1)
        for copy in copies:
            copy.start()

    for c in range(2):
        emit(duos - 1, 1, [c])[0].start()

    all_out = remote(slots.at[2], slots.at[mine], out_send, out_recv, 0, beside)
    all_out.wait_recv()

    def transform(y, j):
        flat = image.at[y].reshape(2 * length * rows, lanes)
        for c in range(2):
            pieces = [
                jnp.concatenate([slots[h, c, y * rows + j + k] for h in range(parts)], axis=0)
                for k in range(2)
            ]
            result = dot_three(x_table, halves(jnp.concatenate(pieces, axis=1)))
            for k in range(2):
                flat[pl.ds(c * length * rows + j + k, length, stride=rows), :] = result[
                    :, k * lanes : (k + 1) * lanes
                ]

    def tally(y, i, sums):
        some = pl.ds(i * group, group)
        shift = speed[y, some]
        s_re, s_im = source[y, some], source[bands + y, some]
        w_re, w_im = image[y, 0, some], image[y, 1, some]
        u_re = s_re + shift * w_re + damped * w_im
        u_im = s_im + shift * w_im - damped * w_re
        terms = (
            s_re * u_re + s_im * u_im,
            s_re * u_im - s_im * u_re,
            u_re * u_re + u_im * u_im,
        )
        return tuple(a + jnp.sum(b, axis=0) for a, b in zip(sums, terms))

    pairs, runs = rows // 2, length // group

    def both(y, sums):
        for n in range(pairs):
            for i in range(n * runs // pairs, (n + 1) * runs // pairs):
                sums = tally(y - 1, i, sums)
            transform(y, 2 * n)
        return sums

    for n in range(pairs):
        transform(0, 2 * n)
    sums = lax.fori_loop(1, bands, both, (jnp.zeros((rows, lanes), jnp.float32),) * 3)
    sums = lax.fori_loop(0, runs, functools.partial(tally, bands - 1), sums, unroll=2)
    sums = [jnp.sum(a, axis=0, keepdims=True) for a in (squares_ref[...],) + sums]
    lane = lax.broadcasted_iota(jnp.int32, (1, lanes), 1)
    packed = jnp.zeros((1, lanes), jnp.float32)
    for k, row in enumerate(sums):
        for shift in (lanes // 2, lanes // 4):
            row = row + pltpu.roll(row, shift, 1)
        packed = jnp.where(lax.div(lane, lanes // 4) == k, row, packed)
    own = len(everyone)
    heard[own] = packed
    copies = [
        remote(heard.at[own], heard.at[k], sum_send, sum_recv, 0, peer)
        for k, peer in enumerate(everyone)
    ]
    for copy in copies:
        copy.start()

    between(ends.at[:, 2], ends.at[:, side], ends_send.at[0], ends_recv.at[0], {"px": other}).wait_send()
    between(inner.at[:, 1 - side], edges.at[:, side], edge_send.at[0], edge_recv.at[0], {"px": other}).wait_send()

    @pl.when(inmost == 0)
    def _():
        between(waves_out.at[:, 0], waves, wave_send.at[0], wave_recv.at[0], {"px": other}).wait_send()

    @pl.when(inmost == 1)
    def _():
        for i in range(places - 1):
            ours = tops.at[:, behind]
            between(ours, ours, top_send.at[i], top_recv.at[0, 0], {"px": other}).wait_send()

    for n in range(depths - 1):

        @pl.when(depth > n)
        def _():
            sent = waves_out.at[:, 1]
            between(sent, outs.at[:, 0], outs_send.at[n], outs_recv.at[0, 0], {"px": other}).wait_send()

    all_in.wait_send()
    all_out.wait_send()
    rest = heard.at[0:own]
    remote(rest, rest, sum_send, sum_recv, 0, everyone[0]).wait()
    total_ref[...] = jnp.broadcast_to(jnp.sum(heard[...], axis=0), total_ref.shape)


def scale(total_ref, w_ref, out_ref, scaled, sems):
    bands, _, length, _, _ = w_ref.shape
    pieces = sems.shape[0]
    depth = length // pieces
    row = total_ref[0:1]
    lane = lax.div(lax.broadcasted_iota(jnp.int32, row.shape, 1), lanes // 4)
    sums = [jnp.sum(jnp.where(lane == k, row, 0.0), axis=1, keepdims=True) for k in range(4)]
    size = sums[0] + epsilon
    one_re, one_im, squares = sums[1] / size, sums[2] / size, sums[3] / size
    one = one_re * one_re + one_im * one_im
    denominator = squares - one * (epsilon / size) + epsilon
    re = jnp.broadcast_to(one_re / denominator, (rows, lanes))
    im = jnp.broadcast_to(-one_im / denominator, (rows, lanes))

    def save(i):
        part = pl.ds(i * depth, depth)
        return pltpu.make_async_copy(scaled.at[:, part], out_ref.at[:, part], sems.at[i])

    @pl.loop(0, pieces)
    def _(i):
        @pl.loop(0, depth, unroll=4)
        def _(j):
            x = i * depth + j
            for y in range(bands):
                w_re, w_im = w_ref[y, 0, x], w_ref[y, 1, x]
                scaled[0, x, y * rows : (y + 1) * rows] = re * w_re - im * w_im
                scaled[1, x, y * rows : (y + 1) * rows] = re * w_im + im * w_re

        save(i).start()

    @pl.loop(0, pieces)
    def _(i):
        save(i).wait()


def on_device(blocks, parts, source, speed):
    _, length_x, number, width = source.shape
    length_z = width * parts
    part = length_x // parts
    tile = 2 * rows
    bands, tiles = number // rows, part // tile
    span = rows * blocks // 2
    groups, places, peers = part // span, blocks // 2, blocks * parts - 1
    f32 = jnp.float32
    shape, dma = jax.ShapeDtypeStruct, pltpu.SemaphoreType.DMA

    def vmem(*size):
        return pltpu.VMEM(size, f32)

    anywhere, inside = pl.BlockSpec(memory_space=pl.ANY), pl.BlockSpec(memory_space=pltpu.VMEM)
    image, sums = pl.pallas_call(
        functools.partial(solve_all, blocks, parts),
        in_specs=[anywhere] * 7,
        out_specs=[inside, inside],
        out_shape=[vmem(bands, 2, length_x, rows, width), vmem(rows, width)],
        scratch_shapes=[
            vmem(2 * bands, length_x, rows, width),
            vmem(bands, length_x, rows, width),
            vmem(2, part, length_z),
            vmem(10, part, lanes),
            vmem(tiles, 3, 2, number, tile, width),
            vmem(tiles // 2, 2, number, tile, length_z),
            vmem(tiles // 2, 2, number, tile, length_z),
            vmem(2, number, tile, length_z),
            vmem(2, number, tile, length_z),
            vmem(groups, 3, 4, span, lanes),
            vmem(groups, 4, span, lanes),
            vmem(groups, 2, 2, span, lanes),
            vmem(groups, 2, span, lanes),
            vmem(groups, 2, 2, span, lanes),
            vmem(groups, places // 2, 2, span, lanes),
            vmem(groups, 2, span, lanes),
            vmem(groups, 2, 4, span, lanes),
            vmem(groups, 2, 4, span, lanes),
            vmem(3, 2, number, part, width),
            pltpu.VMEM((2, length_x, length_x), jnp.bfloat16),
            pltpu.VMEM((2, length_z, length_z), jnp.bfloat16),
            vmem(rows, width),
            vmem(peers + 1, 1, width),
            dma((2 * bands,)),
            dma((bands,)),
            dma((5,)),
            dma((1,)),
            dma((1,)),
            dma((1,)),
            dma((groups,)),
            dma((1,)),
            dma((groups,)),
            dma((places - 1,)),
            dma((groups, 2)),
            dma((places // 2,)),
            dma((groups, places // 2 - 1)),
            dma((1,)),
            dma((tiles,)),
            dma((1,)),
            dma((1,)),
            dma((1,)),
            dma((1,)),
        ],
        compiler_params=pltpu.CompilerParams(
            vmem_limit_bytes=55 * 1024 * 1024, collective_id=0, has_side_effects=True
        ),
        name="solve_all",
    )(source, speed, root_table(length_x, length_z), *sine_table(length_x), *sine_table(length_z))
    pieces = 32
    return pl.pallas_call(
        scale,
        in_specs=[inside, inside],
        out_specs=anywhere,
        out_shape=shape(source.shape, f32),
        scratch_shapes=[vmem(*source.shape), dma((pieces,))],
        compiler_params=pltpu.CompilerParams(vmem_limit_bytes=20 * 1024 * 1024),
        name="scale",
    )(sums, image)


def solution(mesh):
    return jax.shard_map(
        functools.partial(on_device, mesh.shape["px"], mesh.shape["py"]),
        mesh=mesh,
        in_specs=(P(None, "samples", "px", "py"), P("samples", "px", "py")),
        out_specs=P(None, "samples", "px", "py"),
        check_vma=False,
    )
```
